32 devices in a mesh: batch: 4 (over y, core), order: 8 (over z, x).
Axes of the slice: x: 2, y: 2, z: 4, core: 2. Of those that a mesh axis runs over, the one named last changes fastest.
Arguments:
- series: float32 [512, 23040], P('order', 'batch'), may hold values from -6 to 6
- norm_gain: float32 [512], P('order'), may hold values from 0.1 to 1.9
- mode_in: float32 [2, 32, 4, 512], P(None, None, None, 'order'), may hold values from -0.25 to 0.25
- mode_out: float32 [2, 32, 4, 512], P(None, None, None, 'order'), may hold values from -9 to 9
- lengths: int32 [32], P('batch'), may hold values from 96 to 720, as said below
- grad_out: float32 [512, 23040], P('order', 'batch'), may hold values from -6 to 6
Outputs:
- layer_out: float32 [512, 23040], P('order', 'batch')
- grad_series: float32 [512, 23040], P('order', 'batch')
- grad_gain: float32 [512], P('order')
- grad_mode_in: float32 [2, 32, 4, 512], P(None, None, None, 'order')
- grad_mode_out: float32 [2, 32, 4, 512], P(None, None, None, 'order')
- stream_rms: float32 [3], replicated
The draws below stay inside these ranges and needn't reach their ends.
Inputs may be any that keep to these rules, and one draw needn't show every extreme that they name: `lengths`: A window's valid steps are its first steps; each length is one of 96, 336 and 720.
All inputs are finite; a program needn't handle non-finite values.
Results may differ from the reference program's by a relative error of at most 0.0003.
Values sent between devices are 32-bit elements; how exact they have to be, the bound alone decides.
No kernel may reach another device: no remote copies, remote signals or barrier semaphores. Data moves between devices by JAX's collectives and lax.ppermute only.
A program may use at most 256 MiB of HBM per device.

```python
import math
import jax
import jax.numpy as jnp
from jax import lax

D = 512
ORDER = 256
MODES = 32
RANK = 4
LEN = 720
WINDOWS = 32


def draw_lengths(key, part):
    picked = jax.random.randint(key, (WINDOWS,), 0, 3)
    picked = picked.at[0].set(2).at[1].set(0)
    length_set = jnp.array([LEN * 2 // 15, LEN * 7 // 15, LEN], dtype=jnp.int32)
    return length_set[picked]


def levels(key, dims, split, smallest, top_value):
    gain = 1.0
    for axis_at, shards_of in split:
        steps = jax.random.uniform(jax.random.fold_in(jax.random.fold_in(key, 6), axis_at), (shards_of,), jnp.float32, smallest / len(split), top_value / len(split))
        gain = gain * jnp.repeat(jnp.exp(steps), dims[axis_at] // shards_of).reshape((-1,) + (1,) * (len(dims) - 1 - axis_at))
    return gain


def gaussian(rng, extent, deviation, most, pieces=(), held_as=jnp.bfloat16):
    entries = deviation * jax.random.normal(rng, extent, jnp.float32)
    if pieces:
        entries = entries * levels(rng, extent, pieces, -0.22, 0.18)
    return jnp.clip(entries, -most, most).astype(held_as)


def setup_inputs(seed: int = 0) -> dict:
    streams_of = jax.random.split(jax.random.key(seed), 7)
    return {
        "series": gaussian(streams_of[0], (D, WINDOWS * LEN), 1.0, 6.0, ((0, 8), (1, 4)), jnp.float32),
        "norm_gain": jnp.clip(1.0 + 0.18 * jax.random.normal(streams_of[1], (D,), jnp.float32), 0.1, 1.9),
        "mode_in": gaussian(streams_of[2], (2, MODES, RANK, D), D ** -0.5, 0.25, ((3, 8),), jnp.float32),
        "mode_out": gaussian(streams_of[3], (2, MODES, RANK, D), 1.5, 9.0, ((3, 8),), jnp.float32),
        "lengths": draw_lengths(jax.random.fold_in(streams_of[6], 71), 0),
        "grad_out": gaussian(streams_of[5], (D, WINDOWS * LEN), 1.0, 6.0, ((0, 8), (1, 4)), jnp.float32),
    }


precise_mode = lax.Precision.HIGHEST
epsilon = 1e-06

@jax.custom_vjp
def low(v):
    return lax.optimization_barrier(v.astype(jnp.bfloat16)).astype(jnp.float32)

@jax.custom_vjp
def low_back(v):
    return v

def low_keep(v):
    return (low(v), None)

def low_pass(kept, grad):
    return (grad,)

def back_keep(v):
    return (v, None)

def back_low(kept, grad):
    return (low(grad),)
low.defvjp(low_keep, low_pass)
low_back.defvjp(back_keep, back_low)

def legendre_rows(order_count, steps_count):
    positions = jnp.arange(steps_count, dtype=jnp.float32)
    coords = 1.0 - (2.0 * positions + 1.0) / steps_count
    first_row = jnp.ones((steps_count,), jnp.float32)

    def advance(carry, degree):
        earlier, current = carry
        following = ((2.0 * degree + 1.0) * coords * current - degree * earlier) / (degree + 1.0)
        return ((current, following), following)
    degrees = jnp.arange(1, order_count - 1, dtype=jnp.float32)
    final_pair, higher = lax.scan(advance, (first_row, coords), degrees)
    stacked = jnp.concatenate([first_row[None], coords[None], higher], axis=0)
    scaling = jnp.sqrt((2.0 * jnp.arange(order_count, dtype=jnp.float32) + 1.0) / steps_count)
    return stacked * scaling[:, None]

def phase_tables(mode_count, steps_count):
    mode_ids = jnp.arange(mode_count, dtype=jnp.int32)
    positions = jnp.arange(steps_count, dtype=jnp.int32)
    turns = mode_ids[:, None] * positions[None, :] % steps_count
    angle = 2.0 * math.pi / steps_count * turns.astype(jnp.float32)
    return (jnp.cos(angle), jnp.sin(angle))

def projection_table(legendre, mode_count, steps_count):
    cosine_table, sine_table = phase_tables(mode_count, steps_count)
    cum_real = jnp.cumsum(legendre[:, None, :] * cosine_table[None], axis=2)
    cum_imag = -jnp.cumsum(legendre[:, None, :] * sine_table[None], axis=2)
    real_back = jnp.flip(cum_real, axis=2)
    imag_back = jnp.flip(cum_imag, axis=2)
    inv_root = 1.0 / math.sqrt(steps_count)
    table_real = (cosine_table[None] * real_back + sine_table[None] * imag_back) * inv_root
    table_imag = (cosine_table[None] * imag_back - sine_table[None] * real_back) * inv_root
    return jnp.concatenate([table_real, table_imag], axis=1)

def readout_weights(mode_count, steps_count):
    mode_ids = jnp.arange(mode_count, dtype=jnp.int32)
    turns = mode_ids * (steps_count - 1) % steps_count
    angle = 2.0 * math.pi / steps_count * turns.astype(jnp.float32)
    factor = jnp.where(mode_ids == 0, 1.0, 2.0).astype(jnp.float32) / math.sqrt(steps_count)
    return (factor * jnp.cos(angle), -factor * jnp.sin(angle))

def mix_in(coeffs, weights):
    mode_count = weights.shape[1]
    coeff_real = coeffs[:, :, :mode_count]
    coeff_imag = coeffs[:, :, mode_count:]
    real_part = jnp.einsum('bnmd,mrd->bnmr', coeff_real, weights[0], precision=precise_mode) - jnp.einsum('bnmd,mrd->bnmr', coeff_imag, weights[1], precision=precise_mode)
    imag_part = jnp.einsum('bnmd,mrd->bnmr', coeff_real, weights[1], precision=precise_mode) + jnp.einsum('bnmd,mrd->bnmr', coeff_imag, weights[0], precision=precise_mode)
    return (real_part, imag_part)

def mix_out(rank_real, rank_imag, weights):
    out_real = jnp.einsum('bnmr,mrd->bnmd', rank_real, weights[0], precision=precise_mode) - jnp.einsum('bnmr,mrd->bnmd', rank_imag, weights[1], precision=precise_mode)
    out_imag = jnp.einsum('bnmr,mrd->bnmd', rank_real, weights[1], precision=precise_mode) + jnp.einsum('bnmr,mrd->bnmd', rank_imag, weights[0], precision=precise_mode)
    return (out_real, out_imag)

def unpack(stored):
    return jnp.transpose(stored.reshape(D, WINDOWS, LEN), (1, 2, 0))

def pack(windowed):
    return jnp.transpose(windowed, (2, 0, 1)).reshape(D, WINDOWS * LEN)

def reference(series, norm_gain, mode_in, mode_out, lengths, grad_out):
    windows_in = unpack(series)
    cotangent = unpack(grad_out)
    legendre = legendre_rows(ORDER, LEN)
    proj_table = projection_table(legendre, MODES, LEN)
    recon_rows = jnp.flip(legendre, axis=1)
    read_real, read_imag = readout_weights(MODES, LEN)
    valid_mask = (jnp.arange(LEN, dtype=jnp.int32)[None, :] < lengths[:, None]).astype(jnp.float32)

    def forward(series_in, gain_in, weights_in, weights_out):

        def window(window_pair):
            window_rows, mask_row = window_pair
            inv_rms = lax.rsqrt(lax.optimization_barrier(jnp.mean(window_rows * window_rows, axis=1)) + epsilon)
            normed = mask_row[:, None] * gain_in[None, :] * (window_rows * inv_rms[:, None])
            coeffs = jnp.einsum('nks,sd->nkd', proj_table, normed, precision=precise_mode)[None]
            rank_real, rank_imag = mix_in(coeffs, weights_in)
            out_real, out_imag = mix_out(rank_real, rank_imag, weights_out)
            readout = jnp.einsum('m,bnmd->bnd', read_real, out_real, precision=precise_mode) + jnp.einsum('m,bnmd->bnd', read_imag, out_imag, precision=precise_mode)
            branch = mask_row[:, None] * jnp.einsum('nt,nd->td', recon_rows, readout[0], precision=precise_mode)
            return (window_rows + branch, branch)
        return lax.map(jax.checkpoint(window), (series_in, valid_mask))
    outputs, pull_back = jax.vjp(forward, windows_in, norm_gain, mode_in, mode_out)
    layer_out, branch = outputs
    gradients = pull_back((cotangent, jnp.zeros_like(branch)))
    total_count = jnp.sum(lengths).astype(jnp.float32) * D
    masked = valid_mask[:, :, None]
    rms_in = jnp.sqrt(jnp.sum(masked * windows_in * windows_in) / total_count)
    rms_branch = jnp.sqrt(jnp.sum(masked * branch * branch) / total_count)
    rms_out = jnp.sqrt(jnp.sum(masked * layer_out * layer_out) / total_count)
    stream_rms = jnp.stack([rms_in, rms_branch, rms_out])
    return (pack(layer_out), pack(gradients[0]), gradients[1], gradients[2], gradients[3], stream_rms)
```

```python
import functools
import math

import jax
import jax.numpy as jnp
import numpy as np
from jax import lax
from jax.experimental import pallas as pl
from jax.experimental.pallas import tpu as pltpu
from jax.sharding import PartitionSpec as P

ORDER = 256
LEN = 720
LANES = 768
BLOCK = 256
epsilon = 1e-06
f32 = jnp.float32
bf16 = jnp.bfloat16


def legendre_rows():
    coords = 1.0 - (2.0 * np.arange(LEN) + 1.0) / LEN
    rows = [np.ones(LEN), coords]
    for k in range(1, ORDER - 1):
        rows.append(((2.0 * k + 1.0) * coords * rows[k] - k * rows[k - 1]) / (k + 1.0))
    table = np.stack(rows) * np.sqrt((2.0 * np.arange(ORDER) + 1.0) / LEN)[:, None]
    out = np.zeros((ORDER, LANES))
    out[:, :LEN] = table[:, ::-1]
    return out


def phase_rows(mode_count):
    modes = np.arange(mode_count)[:, None]
    steps = np.arange(LANES)[None, :]
    now = 2.0 * np.pi * ((modes * steps) % LEN) / LEN
    nxt = 2.0 * np.pi * ((modes * (steps + 1)) % LEN) / LEN
    root = 1.0 / math.sqrt(LEN)
    rows = np.stack([np.cos(now), np.sin(now), np.cos(nxt) * root, np.sin(nxt) * root])
    return rows.astype(np.float32)


def readout_rows(mode_count):
    modes = np.arange(mode_count)
    angle = 2.0 * np.pi * ((modes * (LEN - 1)) % LEN) / LEN
    factor = np.where(modes == 0, 1.0, 2.0) / math.sqrt(LEN)
    return (factor * np.cos(angle)).astype(np.float32), (-factor * np.sin(angle)).astype(np.float32)


def halves(table):
    high = table.astype(np.float32).astype(jnp.bfloat16)
    low = (table - high.astype(np.float64)).astype(np.float32).astype(jnp.bfloat16)
    return high, low


def split(x):
    high = x.astype(bf16)
    return high, (x - high.astype(f32)).astype(bf16)


def nn(a, b):
    return lax.dot_general(a, b, (((1,), (0,)), ((), ())), preferred_element_type=f32)


def nt(a, b):
    return lax.dot_general(a, b, (((1,), (1,)), ((), ())), preferred_element_type=f32)


def three(dot, a, b):
    return dot(a[0], b[0]) + dot(a[0], b[1]) + dot(a[1], b[0])


def deep(x):
    high, low = split(x)
    return jnp.concatenate([high, low, high], axis=0)


def stacked(weights, pair, rows):
    first = nn(weights, pair[0])
    return first[:rows] + first[rows:] + nn(weights[:rows], pair[1])


def stacked_nt(left, pair, rows):
    first = nt(left, pair[0])
    return first[:rows] + first[rows:] + nt(left[:rows], pair[1])


def rotate(real, imag, cos, sin):
    modes = cos.shape[0]
    shape = (real.shape[0] // modes, modes, real.shape[1])
    real, imag = real.reshape(shape), imag.reshape(shape)
    cos, sin = cos[None], sin[None]
    flat = (shape[0] * modes, shape[2])
    return (real * cos + imag * sin).reshape(flat), (imag * cos - real * sin).reshape(flat)


def triangle():
    row = lax.broadcasted_iota(jnp.int32, (BLOCK, BLOCK), 0)
    col = lax.broadcasted_iota(jnp.int32, (BLOCK, BLOCK), 1)
    return jnp.where(row <= col, 1.0, 0.0).astype(bf16)


def running_sum(x, tri):
    high, low = split(x)
    blocks, carry = [], None
    for b in range(LANES // BLOCK):
        at = slice(b * BLOCK, (b + 1) * BLOCK)
        block = nn(high[:, at], tri) + nn(low[:, at], tri)
        if carry is not None:
            block = block + carry
        carry = block[:, BLOCK - 1 : BLOCK]
        blocks.append(block)
    return jnp.concatenate(blocks, axis=1)


def running_sum_back(x, tri):
    high, low = split(x)
    blocks, carry = [], None
    for b in reversed(range(LANES // BLOCK)):
        at = slice(b * BLOCK, (b + 1) * BLOCK)
        block = nt(high[:, at], tri) + nt(low[:, at], tri)
        if carry is not None:
            block = block + carry
        carry = block[:, 0:1]
        blocks.append(block)
    return jnp.concatenate(blocks[::-1], axis=1)


def deal_kernel(split_at, with_squares, scal_ref, x_ref, *out_refs):
    own_ref, send_refs = out_refs[0], out_refs[1 : 1 + len(split_at) - 1]
    channels = x_ref.shape[0]
    windows = x_ref.shape[1] // LEN
    half = windows // 2
    lane = lax.broadcasted_iota(jnp.int32, (channels, LEN), 1)
    side = scal_ref[0]
    tail = jnp.zeros((channels, 128), f32)
    own_ref[:, :, LANES - 128 :] = jnp.zeros((half, channels, 128), f32)
    for ref in send_refs:
        ref[:, :, LANES - 128 :] = jnp.zeros((ref.shape[0], channels, 128), f32)
    if with_squares:
        squares_ref = out_refs[-1]
        squares_ref[...] = jnp.zeros(squares_ref.shape, f32)
    for w in range(windows):
        value = x_ref[:, w * LEN : (w + 1) * LEN]
        value = jnp.where(lane < scal_ref[2 + w], value, 0.0)
        if with_squares:
            squares_ref[w : w + 1, :LEN] = jnp.sum(value * value, axis=0, keepdims=True)
        j = w % half
        unit = max(u for u in range(len(split_at) - 1) if split_at[u] <= j)
        send_ref, at = send_refs[unit], j - split_at[unit]
        mine = side == (0 if w < half else 1)

        @pl.when(mine)
        def _():
            own_ref[j, :, :LEN] = value

        @pl.when(jnp.logical_not(mine))
        def _():
            send_ref[at, :, :LEN] = value


def weights_kernel(own_ref, rec_ref, down_own, down_rec, up_own, up_rec, down_both, up_both):
    channels = own_ref.shape[1] // 2
    pieces = []
    for ref, down, up in ((own_ref, down_own, up_own), (rec_ref, down_rec, up_rec)):
        high, low = split(ref[...])
        down[...] = jnp.concatenate([high[:, :channels], high[:, :channels], low[:, :channels]], axis=1)
        up[...] = jnp.concatenate([high[:, channels:], high[:, channels:], low[:, channels:]], axis=1)
        across = ref[...].T
        pieces.append(across)
    for k, ref in ((0, down_both), (1, up_both)):
        at = slice(k * channels, (k + 1) * channels)
        rows = jnp.concatenate([pieces[0][at], pieces[1][at]], axis=0)
        high, low = split(rows)
        ref[...] = jnp.concatenate([high, low], axis=0)


def read_kernel(own_ref, rec_ref, up_own, up_rec, leg_high, leg_low, out_ref):
    field = nn(up_own[...], deep(own_ref[0])) + nn(up_rec[...], deep(rec_ref[0]))
    out_ref[0] = three(nt, split(field), (leg_high[...], leg_low[...]))


def inverse_rms(ss_ref, row, full_width):
    return lax.rsqrt(ss_ref[pl.ds(row, 1), :] * (1.0 / full_width) + epsilon)


def rank_kernel(first, full_width, scal_ref, own_ref, rec_ref, ss_ref, down_own, down_rec, leg_high, leg_low, phase_ref, out_ref):
    half = scal_ref[0] * (ss_ref.shape[0] // 2)
    inv = inverse_rms(ss_ref, half + first + pl.program_id(0), full_width)
    mixed = nn(down_own[...], deep(own_ref[0] * inv)) + nn(down_rec[...], deep(rec_ref[0] * inv))
    part = mixed.shape[0] // 2
    real, imag = rotate(mixed[:part], mixed[part:], phase_ref[0], phase_ref[1])
    total = running_sum(jnp.concatenate([real, imag], axis=0), triangle())
    real, imag = rotate(total[:part], total[part:], phase_ref[2], -phase_ref[3])
    memory = jnp.concatenate([real, imag], axis=0)
    out_ref[0] = three(nt, split(memory), (leg_high[...], leg_low[...]))


def back_kernel(first, full_width, scal_ref, mid_ref, end_ref, own_ref, rec_ref, ss_ref, down_both, leg_high, leg_low, phase_ref, prev_ref, own_out, rec_out, grad_out, inner_out):
    step = pl.program_id(0)
    half = scal_ref[0] * (ss_ref.shape[0] // 2)
    row = half + first + step
    inv = inverse_rms(ss_ref, row, full_width)
    channels = own_ref.shape[1]
    total = jnp.where(scal_ref[1] == 1, end_ref[0], mid_ref[0])
    memory = three(nn, split(total), (leg_high[...], leg_low[...]))
    part = memory.shape[0] // 2
    real, imag = rotate(memory[:part], memory[part:], phase_ref[2], phase_ref[3])
    back = running_sum_back(jnp.concatenate([real, imag], axis=0), triangle())
    real, imag = rotate(back[:part], back[part:], phase_ref[0], -phase_ref[1])
    pair = split(jnp.concatenate([real, imag], axis=0))
    scaled = stacked(down_both[...], pair, 2 * channels)
    lane = lax.broadcasted_iota(jnp.int32, scaled.shape, 1)
    scaled = jnp.where(lane < scal_ref[2 + row], scaled, 0.0)
    own_out[0] = scaled[:channels]
    rec_out[0] = scaled[channels:]
    both = jnp.concatenate([own_ref[0], rec_ref[0]], axis=0)
    inner_out[0] = jnp.sum(scaled * both, axis=0, keepdims=True)
    high, low = split(both * inv)
    grads = stacked_nt(jnp.concatenate([high, low], axis=0), pair, 2 * channels)

    @pl.when(step == 0)
    def _():
        grad_out[...] = prev_ref[...] + grads

    @pl.when(step > 0)
    def _():
        grad_out[...] += grads


def branch_kernel(first, scal_ref, mid_ref, end_ref, ser_own, ser_rec, cot_own, cot_rec, up_both, leg_high, leg_low, prev_ref, own_out, rec_out, grad_out):
    step = pl.program_id(0)
    channels = ser_own.shape[1]
    rows = 2 * channels
    row = scal_ref[0] * ((scal_ref.shape[0] - 2) // 2) + first + step
    total = jnp.where(scal_ref[1] == 1, end_ref[0], mid_ref[0])
    field = three(nn, split(total), (leg_high[...], leg_low[...]))
    pair = split(field)
    branch = stacked(up_both[...], pair, rows)
    lane = lax.broadcasted_iota(jnp.int32, branch.shape, 1)
    branch = jnp.where(lane < scal_ref[2 + row], branch, 0.0)
    own_out[0] = branch[:channels]
    rec_out[0] = branch[channels:]
    high, low = split(jnp.concatenate([cot_own[0], cot_rec[0]], axis=0))
    grads = stacked_nt(jnp.concatenate([high, low], axis=0), pair, rows)
    series = jnp.concatenate([ser_own[0], ser_rec[0]], axis=0)
    stats = []
    for v in (series, branch, series + branch):
        v = jnp.sum(v * v, axis=0, keepdims=True)
        stats.append(v[:, :256] + v[:, 256:512] + v[:, 512:])
    stats = jnp.concatenate(stats + [jnp.zeros((5, 256), f32)], axis=0)
    grads = jnp.concatenate([grads, stats], axis=0)

    @pl.when(step == 0)
    def _():
        grad_out[...] = prev_ref[...] + grads

    @pl.when(step > 0)
    def _():
        grad_out[...] += grads


def layer_kernel(units, scal_ref, x_ref, *refs):
    own_refs, rec_refs, out_ref = refs[: len(units)], refs[len(units) : 2 * len(units)], refs[-1]
    windows = x_ref.shape[1] // LEN
    half = windows // 2
    first_side = scal_ref[0] == 0
    for w in range(windows):
        j = w % half
        u = max(k for k in range(len(units)) if units[k][0] <= j)
        mine = own_refs[u][j - units[u][0], :, :LEN]
        theirs = rec_refs[u][j - units[u][0], :, :LEN]
        value = jnp.where(first_side == (w < half), mine, theirs)
        at = slice(w * LEN, (w + 1) * LEN)
        out_ref[:, at] = x_ref[:, at] + value


def series_grad_kernel(units, full_width, scal_ref, cot_ref, x_ref, ss_ref, in_own, in_rec, *refs):
    own_refs, rec_refs, out_ref = refs[: len(units)], refs[len(units) : 2 * len(units)], refs[-1]
    windows = x_ref.shape[1] // LEN
    half = windows // 2
    first_side = scal_ref[0] == 0
    for w in range(windows):
        j = w % half
        u = max(k for k in range(len(units)) if units[k][0] <= j)
        mine = own_refs[u][j - units[u][0], :, :LEN]
        theirs = rec_refs[u][j - units[u][0], :, :LEN]
        keep = first_side == (w < half)
        scaled = jnp.where(keep, mine, theirs)
        inner = jnp.where(keep, in_own[j], in_rec[j])[:, :LEN]
        inv = inverse_rms(ss_ref, w, full_width)[:, :LEN]
        at = slice(w * LEN, (w + 1) * LEN)
        shift = inv * inv * inner * (1.0 / full_width)
        out_ref[:, at] = cot_ref[:, at] + inv * (scaled - x_ref[:, at] * shift)


def whole(shape):
    return pl.BlockSpec(shape, lambda *_: (0,) * len(shape))


SMEM = pl.BlockSpec(memory_space=pltpu.SMEM)
PARAMS = pltpu.CompilerParams(vmem_limit_bytes=48 * 1024 * 1024)


def window_spec(shape, offset):
    return pl.BlockSpec((1,) + shape[1:], lambda i: (i + offset,) + (0,) * (len(shape) - 1))


def cost(flops, byte_count):
    return pl.CostEstimate(flops=int(flops), bytes_accessed=int(byte_count), transcendentals=0)


def struct(shape, dtype=f32):
    return jax.ShapeDtypeStruct(shape, dtype)


def deal(array, scal, units, with_squares):
    channels = array.shape[0]
    windows = array.shape[1] // LEN
    half = windows // 2
    edges = [u[0] for u in units] + [half]
    shapes = [struct((half, channels, LANES))] + [struct((n, channels, LANES)) for _, n in units]
    if with_squares:
        shapes.append(struct((windows, LANES)))
    return pl.pallas_call(
        functools.partial(deal_kernel, edges, with_squares),
        out_shape=shapes,
        in_specs=[SMEM, whole(array.shape)],
        out_specs=[whole(s.shape) for s in shapes],
        grid=(1,),
        compiler_params=PARAMS,
        cost_estimate=cost(array.size * 4, array.size * 8),
    )(scal, array)


def prepare_weights(own, rec):
    rows, channels = own.shape[0], own.shape[1] // 2
    shapes = [struct((rows, 3 * channels), bf16)] * 4 + [struct((4 * channels, rows), bf16)] * 2
    return pl.pallas_call(
        weights_kernel,
        out_shape=shapes,
        in_specs=[whole(own.shape)] * 2,
        out_specs=[whole(s.shape) for s in shapes],
        grid=(1,),
        compiler_params=PARAMS,
        cost_estimate=cost(own.size * 8, own.size * 16),
    )(own, rec)


MATMUL = 2 * 256 * 256 * 256


def unit_call(kernel, unit, smem, arrays, consts, outs, units_of_work):
    first, count = unit
    specs = [SMEM] * len(smem)
    specs += [window_spec(a.shape, offset) for a, offset in arrays]
    specs += [whole(c.shape) for c in consts]
    out_specs, shapes = [], []
    for shape, per_window in outs:
        shapes.append(struct(shape))
        out_specs.append(window_spec(shape, 0) if per_window else whole(shape))
    moved = sum(a.size * 4 * count // a.shape[0] for a, _ in arrays) + sum(c.size * c.dtype.itemsize for c in consts)
    return pl.pallas_call(
        kernel,
        out_shape=shapes,
        in_specs=specs,
        out_specs=out_specs,
        grid=(count,),
        compiler_params=PARAMS,
        cost_estimate=cost(units_of_work * MATMUL * count, moved),
    )(*smem, *[a for a, _ in arrays], *consts)


def swap(x, axis, bit):
    size = lax.axis_size(axis)
    return lax.ppermute(x, axis, [(i, i ^ bit) for i in range(size)])


def add_over(x, axis, bits):
    for bit in bits:
        x = x + swap(x, axis, bit)
    return x


def bits_of(size, start=1):
    bits, bit = [], start
    while bit < size:
        bits.append(bit)
        bit *= 2
    return bits


def line_sum(x):
    size = lax.axis_size("order")
    if size != 8:
        lines = [[2 * i + side for i in range(size // 2)] for side in (0, 1)]
        total = lax.psum(x, "order", axis_index_groups=lines)
        return total, total
    inward = [(0, 2), (1, 3), (6, 4), (7, 5)]
    middle = [(2, 4), (3, 5), (4, 2), (5, 3)]
    outward = [(2, 0), (3, 1), (4, 6), (5, 7)]
    pair = x + lax.ppermute(x, "order", inward)
    total = pair + lax.ppermute(pair, "order", middle)
    return total, lax.ppermute(total, "order", outward)


UNITS = 2


def local(series, norm_gain, mode_in, mode_out, lengths, grad_out):
    channels = series.shape[0]
    windows = series.shape[1] // LEN
    half = windows // 2
    order_devices = lax.axis_size("order")
    batch_devices = lax.axis_size("batch")
    mode_count, rank_count = mode_in.shape[1], mode_in.shape[2]
    full_width = channels * order_devices
    rows = 2 * rank_count * mode_count
    per = half // UNITS
    units = [(u * per, per) for u in range(UNITS)]

    place = lax.axis_index("order")
    line = place // 2
    at_end = jnp.logical_or(line == 0, line == order_devices // 2 - 1)
    scal = jnp.concatenate([jnp.stack([place % 2, at_end.astype(jnp.int32)]), lengths])

    table_high, table_low = (jnp.asarray(h) for h in halves(legendre_rows()))
    phase = jnp.asarray(phase_rows(mode_count))
    read_real, read_imag = (jnp.asarray(r)[None, :, None] for r in readout_rows(mode_count))

    into = jnp.transpose(mode_in, (0, 2, 1, 3))
    outof = jnp.transpose(mode_out, (0, 2, 1, 3))
    second = jnp.stack([
        read_real * outof[0] + read_imag * outof[1],
        read_imag * outof[0] - read_real * outof[1],
    ])
    weights = jnp.concatenate(
        [(into * norm_gain).reshape(rows, channels), second.reshape(rows, channels)], axis=1
    )

    cot = deal(grad_out, scal, units, False)
    weights_rec = swap(weights, "order", 1)
    cot_own = cot[0]
    cot_rec = [swap(c, "order", 1) for c in cot[1:]]
    ser = deal(series, scal, units, True)
    squares = add_over(ser[-1], "order", bits_of(order_devices))
    ser_own = ser[0]
    ser_rec = [swap(s, "order", 1) for s in ser[1:-1]]
    down_own, down_rec, up_own, up_rec, down_both, up_both = prepare_weights(weights, weights_rec)

    grad_sums = []
    for u, (first, count) in enumerate(units):
        (read,) = unit_call(
            read_kernel, units[u], [], [(cot_own, first), (cot_rec[u], 0)],
            [up_own, up_rec, table_high, table_low], [((count, rows, ORDER), True)], 15,
        )
        grad_sums.append(line_sum(read))

    rank_sums = []
    for u, (first, count) in enumerate(units):
        (ranks,) = unit_call(
            functools.partial(rank_kernel, first, full_width), units[u], [scal], [(ser_own, first), (ser_rec[u], 0)],
            [squares, down_own, down_rec, table_high, table_low, phase], [((count, rows, ORDER), True)], 21,
        )
        rank_sums.append(line_sum(ranks))

    grad_in = jnp.zeros((2 * channels, rows), f32)
    scaled_own, scaled_rec, inner = [], [], []
    for u, (first, count) in enumerate(units):
        mine, theirs, grad_in, dots = unit_call(
            functools.partial(back_kernel, first, full_width), units[u], [scal],
            [(grad_sums[u][0], 0), (grad_sums[u][1], 0), (ser_own, first), (ser_rec[u], 0)],
            [squares, down_both, table_high, table_low, phase, grad_in],
            [((count, channels, LANES), True)] * 2 + [((2 * channels, rows), False), ((count, 1, LANES), True)], 24,
        )
        scaled_own.append(mine)
        scaled_rec.append(swap(theirs, "order", 1))
        inner.append(dots)
    inner = jnp.concatenate(inner, axis=0)
    if order_devices == 8:
        inner = add_over(inner, "order", bits_of(order_devices, 2))
    else:
        inner = line_sum(inner)[0]
    inner_rec = swap(inner, "order", 1)

    grad_series = pl.pallas_call(
        functools.partial(series_grad_kernel, units, full_width),
        out_shape=struct(series.shape),
        in_specs=[SMEM] + [whole(series.shape)] * 2 + [whole(squares.shape)] + [whole(inner.shape)] * 2 + [whole(s.shape) for s in scaled_own + scaled_rec],
        out_specs=whole(series.shape),
        grid=(1,),
        compiler_params=PARAMS,
        cost_estimate=cost(series.size * 8, series.size * 16),
    )(scal, grad_out, series, squares, inner, inner_rec, *scaled_own, *scaled_rec)

    row = lax.broadcasted_iota(jnp.int32, (2 * channels + 8, rows), 0)
    col = lax.broadcasted_iota(jnp.int32, (2 * channels + 8, rows), 1)
    here = jnp.logical_and(row == 2 * channels + 3, col == 0)
    grad_mix = jnp.where(here, jnp.sum(lengths).astype(f32), 0.0)
    branch_own, branch_rec = [], []
    for u, (first, count) in enumerate(units):
        mine, theirs, grad_mix = unit_call(
            functools.partial(branch_kernel, first), units[u], [scal],
            [(rank_sums[u][0], 0), (rank_sums[u][1], 0), (ser_own, first), (ser_rec[u], 0), (cot_own, first), (cot_rec[u], 0)],
            [up_both, table_high, table_low, grad_mix],
            [((count, channels, LANES), True)] * 2 + [((2 * channels + 8, rows), False)], 18,
        )
        branch_own.append(mine)
        branch_rec.append(swap(theirs, "order", 1))

    layer_out = pl.pallas_call(
        functools.partial(layer_kernel, units),
        out_shape=struct(series.shape),
        in_specs=[SMEM] + [whole(series.shape)] + [whole(b.shape) for b in branch_own + branch_rec],
        out_specs=whole(series.shape),
        grid=(1,),
        compiler_params=PARAMS,
        cost_estimate=cost(series.size * 2, series.size * 12),
    )(scal, series, *branch_own, *branch_rec)

    stats = grad_mix[2 * channels :]
    own_part = jnp.concatenate([grad_in[:channels], grad_mix[:channels], stats], axis=0)
    rec_part = jnp.concatenate([grad_in[channels:], grad_mix[channels : 2 * channels], stats], axis=0)
    sums = own_part + swap(rec_part, "order", 1)
    if batch_devices == 4:
        sums = add_over(sums, "batch", bits_of(batch_devices))
    else:
        sums = lax.psum(sums, "batch")
    stats = sums[2 * channels :]
    if order_devices == 8:
        stats = add_over(stats, "order", bits_of(order_devices, 2))
    else:
        stats = line_sum(stats)[0]

    into_sum, mix_sum = sums[:channels].T, sums[channels : 2 * channels].T
    shape = (2, rank_count, mode_count, channels)
    into_sum, mix_sum = into_sum.reshape(shape), mix_sum.reshape(shape)
    grad_gain = jnp.sum(into_sum * into, axis=(0, 1, 2))
    grad_mode_in = jnp.transpose(into_sum * norm_gain, (0, 2, 1, 3))
    grad_mode_out = jnp.transpose(
        jnp.stack([
            read_real * mix_sum[0] + read_imag * mix_sum[1],
            read_imag * mix_sum[0] - read_real * mix_sum[1],
        ]),
        (0, 2, 1, 3),
    )
    stats = jnp.sum(stats, axis=1)
    count = stats[3] * (1.0 / order_devices)
    stream_rms = jnp.sqrt(stats[:3] / (count * full_width))
    return layer_out, grad_series, grad_gain, grad_mode_in, grad_mode_out, stream_rms


def solution(mesh):
    wide = P("order", "batch")
    weight = P(None, None, None, "order")
    in_specs = (wide, P("order"), weight, weight, P("batch"), wide)
    out_specs = (wide, wide, P("order"), weight, weight, P())
    return jax.shard_map(local, mesh=mesh, in_specs=in_specs, out_specs=out_specs, check_vma=False)
```

```python
import functools
import math

import jax
import jax.numpy as jnp
import numpy as np
from jax import lax
from jax.experimental import pallas as pl
from jax.experimental.pallas import tpu as pltpu
from jax.sharding import PartitionSpec as P

ORDER = 256
LEN = 720
LANES = 768
BLOCK = 256
epsilon = 1e-06
f32 = jnp.float32
bf16 = jnp.bfloat16


def legendre_rows():
    coords = 1.0 - (2.0 * np.arange(LEN) + 1.0) / LEN
    rows = [np.ones(LEN), coords]
    for k in range(1, ORDER - 1):
        rows.append(((2.0 * k + 1.0) * coords * rows[k] - k * rows[k - 1]) / (k + 1.0))
    table = np.stack(rows) * np.sqrt((2.0 * np.arange(ORDER) + 1.0) / LEN)[:, None]
    out = np.zeros((ORDER, LANES))
    out[:, :LEN] = table[:, ::-1]
    return out


def phase_rows(mode_count):
    modes = np.arange(mode_count)[:, None]
    steps = np.arange(LANES)[None, :]
    now = 2.0 * np.pi * ((modes * steps) % LEN) / LEN
    nxt = 2.0 * np.pi * ((modes * (steps + 1)) % LEN) / LEN
    root = 1.0 / math.sqrt(LEN)
    rows = np.stack([np.cos(now), np.sin(now), np.cos(nxt) * root, np.sin(nxt) * root])
    return rows.astype(np.float32)


def halves(table):
    high = table.astype(np.float32).astype(jnp.bfloat16)
    low = (table - high.astype(np.float64)).astype(np.float32).astype(jnp.bfloat16)
    return high, low


def split(x):
    high = x.astype(bf16)
    return high, (x - high.astype(f32)).astype(bf16)


def nn(a, b):
    return lax.dot_general(a, b, (((1,), (0,)), ((), ())), preferred_element_type=f32)


def nt(a, b):
    return lax.dot_general(a, b, (((1,), (1,)), ((), ())), preferred_element_type=f32)


def three(dot, a, b):
    return dot(a[0], b[0]) + dot(a[0], b[1]) + dot(a[1], b[0])


def deep(x):
    high, low = split(x)
    return jnp.concatenate([high, low, high], axis=0)


def stacked(weights, pair, rows):
    first = nn(weights, pair[0])
    return first[:rows] + first[rows:] + nn(weights[:rows], pair[1])


def stacked_nt(left, pair, rows):
    first = nt(left, pair[0])
    return first[:rows] + first[rows:] + nt(left[:rows], pair[1])


def rotate(real, imag, cos, sin):
    modes = cos.shape[0]
    shape = (real.shape[0] // modes, modes, real.shape[1])
    real, imag = real.reshape(shape), imag.reshape(shape)
    cos, sin = cos[None], sin[None]
    flat = (shape[0] * modes, shape[2])
    return (real * cos + imag * sin).reshape(flat), (imag * cos - real * sin).reshape(flat)


def triangle():
    row = lax.broadcasted_iota(jnp.int32, (BLOCK, BLOCK), 0)
    col = lax.broadcasted_iota(jnp.int32, (BLOCK, BLOCK), 1)
    return jnp.where(row <= col, 1.0, 0.0).astype(bf16)


def running_sum(x, tri):
    high, low = split(x)
    blocks, carry = [], None
    for b in range(LANES // BLOCK):
        at = slice(b * BLOCK, (b + 1) * BLOCK)
        block = nn(high[:, at], tri) + nn(low[:, at], tri)
        if carry is not None:
            block = block + carry
        carry = block[:, BLOCK - 1 : BLOCK]
        blocks.append(block)
    return jnp.concatenate(blocks, axis=1)


def running_sum_back(x, tri):
    high, low = split(x)
    blocks, carry = [], None
    for b in reversed(range(LANES // BLOCK)):
        at = slice(b * BLOCK, (b + 1) * BLOCK)
        block = nt(high[:, at], tri) + nt(low[:, at], tri)
        if carry is not None:
            block = block + carry
        carry = block[:, 0:1]
        blocks.append(block)
    return jnp.concatenate(blocks[::-1], axis=1)


def side_of():
    return lax.rem(lax.axis_index("order"), 2)


def at_line_end(line_length):
    line = lax.div(lax.axis_index("order"), 2)
    return jnp.logical_or(line == 0, line == line_length - 1)


def locate(units, j):
    u = max(k for k in range(len(units)) if units[k][0] <= j)
    return u, j - units[u][0]


def chunk_ends(windows):
    return [-(-LEN * min(w + 2, windows) // 128) * 128 for w in range(0, windows, 2)]


def deal_windows(split_at, len_hbm, hbm_ref, len_ref, buffer, sems, out_refs, use):
    lengths_copy = pltpu.make_async_copy(len_hbm, len_ref, sems.at[0])
    lengths_copy.start()
    own_ref, send_refs = out_refs[0], out_refs[1:]
    channels = hbm_ref.shape[0]
    windows = hbm_ref.shape[1] // LEN
    half = windows // 2
    ends = chunk_ends(windows)
    copies = []
    for c, end in enumerate(ends):
        at = slice(ends[c - 1] if c else 0, end)
        copies.append(pltpu.make_async_copy(hbm_ref.at[:, at], buffer.at[:, at], sems.at[1 + c]))
        copies[-1].start()
    lane = lax.broadcasted_iota(jnp.int32, (channels, LEN), 1)
    side = side_of()
    for ref in out_refs:
        ref[:, :, LANES - 128 :] = jnp.zeros((ref.shape[0], channels, 128), f32)
    lengths_copy.wait()
    for w in range(windows):
        if w % 2 == 0:
            copies[w // 2].wait()
        value = buffer[:, w * LEN : (w + 1) * LEN]
        value = jnp.where(lane < len_ref[w], value, 0.0)
        use(w, value)
        unit, at = locate(split_at, w % half)
        send_ref = send_refs[unit]
        mine = side == (0 if w < half else 1)

        @pl.when(mine)
        def _():
            own_ref[w % half, :, :LEN] = value

        @pl.when(jnp.logical_not(mine))
        def _():
            send_ref[at, :, :LEN] = value


PACK = 48
STATS = 8


def readout_columns(modes, channels):
    mode = lax.broadcasted_iota(jnp.int32, (modes, channels), 0)
    angle = mode.astype(f32) * (2.0 * math.pi / LEN)
    factor = jnp.where(mode == 0, 1.0, 2.0) * (1.0 / math.sqrt(LEN))
    return factor * jnp.cos(angle), factor * jnp.sin(angle)


def front_kernel(units, len_hbm, in_hbm, out_hbm, gain_hbm, x_hbm, message_ref, *refs):
    out_refs, (len_ref, in_ref, out_ref, gain_ref, buffer, packed, sems, weight_sems) = refs[:-8], refs[-8:]
    windows = x_hbm.shape[1] // LEN
    weights = [(in_hbm, in_ref), (out_hbm, out_ref), (gain_hbm, gain_ref)]
    weights = [pltpu.make_async_copy(a, b, weight_sems.at[k]) for k, (a, b) in enumerate(weights)]
    for copy in weights:
        copy.start()
    message_ref[...] = jnp.zeros(message_ref.shape, f32)

    def use(w, value):
        message_ref[w : w + 1, :LEN] = jnp.sum(value * value, axis=0, keepdims=True)

    deal_windows(units, len_hbm, x_hbm, len_ref, buffer, sems, out_refs, use)
    for copy in weights:
        copy.wait()
    modes, ranks, channels = in_ref.shape[1:]
    packed[...] = jnp.zeros(packed.shape, f32)
    read_real, read_imag = readout_columns(modes, channels)
    for r in range(ranks):
        real, imag = out_ref[0, :, r, :], out_ref[1, :, r, :]
        second = (read_real * real + read_imag * imag, read_imag * real - read_real * imag)
        for part in range(2):
            at = slice((part * ranks + r) * modes, (part * ranks + r + 1) * modes)
            packed[at, :channels] = in_ref[part, :, r, :] * gain_ref[...]
            packed[at, channels : 2 * channels] = second[part]
    rows = packed.shape[0]
    for k in range(-(-rows // PACK)):
        count = min(PACK, rows - k * PACK)
        message_ref[windows : windows + count, k * 128 : (k + 1) * 128] = packed[k * PACK : k * PACK + count]


def unpack(message_ref, windows, rows):
    pieces = []
    for k in range(-(-rows // PACK)):
        count = min(PACK, rows - k * PACK)
        pieces.append(message_ref[windows : windows + count, k * 128 : (k + 1) * 128])
    return jnp.concatenate(pieces, axis=0)


def cot_kernel(units, len_hbm, x_hbm, *refs):
    deal_windows(units, len_hbm, x_hbm, *refs[-3:], refs[:-3], lambda w, value: None)


def weights_kernel(windows, own_ref, rec_ref, down_own, down_rec, up_own, up_rec, down_both, up_both):
    rows, channels = down_own.shape[0], down_own.shape[1] // 3
    pieces = []
    for ref, down, up in ((own_ref, down_own, up_own), (rec_ref, down_rec, up_rec)):
        packed = unpack(ref, windows, rows)
        high, low = split(packed)
        down[...] = jnp.concatenate([high[:, :channels], high[:, :channels], low[:, :channels]], axis=1)
        upper = slice(channels, 2 * channels)
        up[...] = jnp.concatenate([high[:, upper], high[:, upper], low[:, upper]], axis=1)
        pieces.append(packed.T)
    for k, ref in ((0, down_both), (1, up_both)):
        at = slice(k * channels, (k + 1) * channels)
        both = jnp.concatenate([pieces[0][at], pieces[1][at]], axis=0)
        high, low = split(both)
        ref[...] = jnp.concatenate([high, low], axis=0)


def read_kernel(own_ref, rec_ref, up_own, up_rec, leg_high, leg_low, out_ref):
    field = nn(up_own[...], deep(own_ref[0])) + nn(up_rec[...], deep(rec_ref[0]))
    out_ref[0] = three(nt, split(field), (leg_high[...], leg_low[...]))


def inverse_rms(ss_ref, row, full_width):
    return lax.rsqrt(ss_ref[pl.ds(row, 1), :] * (1.0 / full_width) + epsilon)


def rank_kernel(first, full_width, own_ref, rec_ref, ss_ref, down_own, down_rec, leg_high, leg_low, phase_ref, out_ref):
    half = side_of() * (ss_ref.shape[0] // 2)
    inv = inverse_rms(ss_ref, half + first + pl.program_id(0), full_width)
    mixed = nn(down_own[...], deep(own_ref[0] * inv)) + nn(down_rec[...], deep(rec_ref[0] * inv))
    part = mixed.shape[0] // 2
    real, imag = rotate(mixed[:part], mixed[part:], phase_ref[0], phase_ref[1])
    total = running_sum(jnp.concatenate([real, imag], axis=0), triangle())
    real, imag = rotate(total[:part], total[part:], phase_ref[2], -phase_ref[3])
    memory = jnp.concatenate([real, imag], axis=0)
    out_ref[0] = three(nt, split(memory), (leg_high[...], leg_low[...]))


def opening(refs, outs):
    return None if len(refs) == outs else refs[0], refs[-outs:]


def back_kernel(first, full_width, line_length, len_ref, mid_ref, end_ref, own_ref, rec_ref, ss_ref, down_both, leg_high, leg_low, phase_ref, *refs):
    prev_ref, (own_out, rec_out, grad_out, inner_out) = opening(refs, 4)
    step = pl.program_id(0)
    half = side_of() * (ss_ref.shape[0] // 2)
    row = half + first + step
    inv = inverse_rms(ss_ref, row, full_width)
    channels = own_ref.shape[1]
    total = jnp.where(at_line_end(line_length), end_ref[0], mid_ref[0])
    memory = three(nn, split(total), (leg_high[...], leg_low[...]))
    part = memory.shape[0] // 2
    real, imag = rotate(memory[:part], memory[part:], phase_ref[2], phase_ref[3])
    back = running_sum_back(jnp.concatenate([real, imag], axis=0), triangle())
    real, imag = rotate(back[:part], back[part:], phase_ref[0], -phase_ref[1])
    pair = split(jnp.concatenate([real, imag], axis=0))
    scaled = stacked(down_both[...], pair, 2 * channels)
    lane = lax.broadcasted_iota(jnp.int32, scaled.shape, 1)
    scaled = jnp.where(lane < len_ref[row], scaled, 0.0)
    own_out[0] = scaled[:channels]
    rec_out[0] = scaled[channels:]
    both = jnp.concatenate([own_ref[0], rec_ref[0]], axis=0)
    inner = jnp.sum(scaled * both, axis=0, keepdims=True)
    pieces = [inner[:, p * 256 : (p + 1) * 256] for p in range(LANES // 256)]
    inner_out[0] = jnp.concatenate(pieces + [jnp.zeros((STATS - len(pieces), 256), f32)], axis=0)
    high, low = split(both * inv)
    grads = stacked_nt(jnp.concatenate([high, low], axis=0), pair, 2 * channels)

    @pl.when(step == 0)
    def _():
        grad_out[...] = grads if prev_ref is None else prev_ref[...] + grads

    @pl.when(step > 0)
    def _():
        grad_out[...] += grads


def branch_kernel(first, line_length, len_ref, mid_ref, end_ref, ser_own, ser_rec, cot_own, cot_rec, up_both, leg_high, leg_low, *refs):
    prev_ref, (own_out, rec_out, grad_out) = opening(refs, 3)
    step = pl.program_id(0)
    channels = ser_own.shape[1]
    rows = 2 * channels
    row = side_of() * (len_ref.shape[0] // 2) + first + step
    total = jnp.where(at_line_end(line_length), end_ref[0], mid_ref[0])
    field = three(nn, split(total), (leg_high[...], leg_low[...]))
    pair = split(field)
    branch = stacked(up_both[...], pair, rows)
    lane = lax.broadcasted_iota(jnp.int32, branch.shape, 1)
    branch = jnp.where(lane < len_ref[row], branch, 0.0)
    own_out[0] = branch[:channels]
    rec_out[0] = branch[channels:]
    high, low = split(jnp.concatenate([cot_own[0], cot_rec[0]], axis=0))
    grads = stacked_nt(jnp.concatenate([high, low], axis=0), pair, rows)
    series = jnp.concatenate([ser_own[0], ser_rec[0]], axis=0)
    stats = []
    for v in (series, branch, series + branch):
        v = jnp.sum(jnp.sum(v * v, axis=0, keepdims=True), axis=1, keepdims=True)
        stats.append(jnp.broadcast_to(v, (1, grads.shape[1])))
    steps = functools.reduce(lambda a, b: a + b, [len_ref[w] for w in range(len_ref.shape[0])])
    steps = jnp.where(jnp.logical_and(first == 0, step == 0), steps, 0).astype(f32)
    stats.append(jnp.full((1, grads.shape[1]), steps, f32))
    stats = jnp.concatenate(stats + [jnp.zeros((4, grads.shape[1]), f32)], axis=0)
    grads = jnp.concatenate([grads, stats], axis=0)

    @pl.when(step == 0)
    def _():
        grad_out[...] = grads if prev_ref is None else prev_ref[...] + grads

    @pl.when(step > 0)
    def _():
        grad_out[...] += grads


def layer_kernel(units, x_ref, *refs):
    own_refs, rec_refs, out_ref = refs[: len(units)], refs[len(units) : 2 * len(units)], refs[-1]
    windows = x_ref.shape[1] // LEN
    half = windows // 2
    first_side = side_of() == 0
    for w in range(windows):
        u, j = locate(units, w % half)
        value = jnp.where(first_side == (w < half), own_refs[u][j], rec_refs[u][j])
        at = slice(w * LEN, (w + 1) * LEN)
        out_ref[:, at] = x_ref[:, at] + value[:, :LEN]


def inner_row(small_ref, j):
    row = STATS * (1 + j)
    return jnp.concatenate([small_ref[row + p : row + p + 1, :] for p in range(LANES // 256)], axis=1)


def series_grad_kernel(units, full_width, cot_ref, x_ref, ss_ref, in_own, in_rec, *refs):
    own_refs, rec_refs, out_ref = refs[: len(units)], refs[len(units) : 2 * len(units)], refs[-1]
    windows = x_ref.shape[1] // LEN
    half = windows // 2
    first_side = side_of() == 0
    for w in range(windows):
        u, j = locate(units, w % half)
        keep = first_side == (w < half)
        scaled = jnp.where(keep, own_refs[u][j], rec_refs[u][j])[:, :LEN]
        inner = jnp.where(keep, inner_row(in_own, w % half), inner_row(in_rec, w % half))[:, :LEN]
        inv = inverse_rms(ss_ref, w, full_width)[:, :LEN]
        at = slice(w * LEN, (w + 1) * LEN)
        shift = inv * inv * inner * (1.0 / full_width)
        out_ref[:, at] = cot_ref[:, at] + inv * (scaled - x_ref[:, at] * shift)


def close_kernel(share, own_ref, rec_ref, in_ref, gain_ref, grad_in_ref, grad_out_ref, grad_gain_ref, rms_ref):
    modes, ranks, channels = in_ref.shape[1:]
    sums = own_ref[...] + rec_ref[...]
    into, mix, stats = sums[:channels].T, sums[channels : 2 * channels].T, sums[2 * channels : 2 * channels + STATS]
    total = jnp.zeros((modes, channels), f32)
    read_real, read_imag = readout_columns(modes, channels)
    for r in range(ranks):
        pieces = []
        for part in range(2):
            at = slice((part * ranks + r) * modes, (part * ranks + r + 1) * modes)
            grad = into[at]
            total = total + grad * in_ref[part, :, r, :]
            grad_in_ref[part, :, r, :] = grad * gain_ref[...]
            pieces.append(mix[at])
        grad_out_ref[0, :, r, :] = read_real * pieces[0] + read_imag * pieces[1]
        grad_out_ref[1, :, r, :] = read_imag * pieces[0] - read_real * pieces[1]
    grad_gain_ref[...] = jnp.sum(total, axis=0, keepdims=True)
    rms = jnp.sqrt(stats * share / stats[3:4])
    for k in range(3):
        rms_ref[k] = rms[k, 0]


def whole(shape):
    return pl.BlockSpec(shape, lambda *_: (0,) * len(shape))


SMEM = pl.BlockSpec(memory_space=pltpu.SMEM)
PARAMS = pltpu.CompilerParams(vmem_limit_bytes=8 * 1024 * 1024)


def window_spec(shape, offset):
    return pl.BlockSpec((1,) + shape[1:], lambda i: (i + offset,) + (0,) * (len(shape) - 1))


def cost(flops, byte_count, weight=1):
    return pl.CostEstimate(flops=int(flops * weight), bytes_accessed=int(byte_count * weight), transcendentals=0)


def struct(shape, dtype=f32):
    return jax.ShapeDtypeStruct(shape, dtype)


def one_call(kernel, outs, args, smem=0, scalars_out=0):
    single = not isinstance(outs, list)
    shapes = [outs] if single else outs
    specs = [SMEM] * smem + [whole(a.shape) for a in args[smem:]]
    moved = sum(a.size * a.dtype.itemsize for a in args) + sum(math.prod(o.shape) * 4 for o in shapes)
    result = pl.pallas_call(
        kernel,
        out_shape=shapes,
        in_specs=specs,
        out_specs=[whole(o.shape) for o in shapes[: len(shapes) - scalars_out]] + [SMEM] * scalars_out,
        grid=(1,),
        compiler_params=PARAMS,
        cost_estimate=cost(moved, moved),
    )(*args)
    return result[0] if single else result


HBM = pl.BlockSpec(memory_space=pltpu.MemorySpace.HBM)


def in_hbm(arrays):
    return [pltpu.with_memory_space_constraint(a, pltpu.MemorySpace.HBM) for a in arrays]


def deal_scratch(array, lengths):
    windows = array.shape[1] // LEN
    return [pltpu.SMEM(lengths.shape, jnp.int32)], [
        pltpu.VMEM(array.shape, f32),
        pltpu.SemaphoreType.DMA((1 + len(chunk_ends(windows)),)),
    ]


def front(series, lengths, weights, units, rows):
    channels, windows = series.shape[0], series.shape[1] // LEN
    shapes = [struct((windows + PACK, LANES)), struct((windows // 2, channels, LANES))]
    shapes += [struct((n, channels, LANES)) for _, n in units]
    first, (buffer, sems) = deal_scratch(series, lengths)
    scratch = first + [pltpu.VMEM(a.shape, f32) for a in weights] + [buffer, pltpu.VMEM((rows, 128), f32), sems]
    return pl.pallas_call(
        functools.partial(front_kernel, units),
        out_shape=shapes,
        in_specs=[HBM] * (2 + len(weights)),
        out_specs=[whole(o.shape) for o in shapes],
        grid=(1,),
        scratch_shapes=scratch + [pltpu.SemaphoreType.DMA((len(weights),))],
        compiler_params=PARAMS,
        cost_estimate=cost(series.size * 4, series.size * 8),
    )(*in_hbm([lengths, *weights, series]))


def deal(array, lengths, units):
    channels, windows = array.shape[0], array.shape[1] // LEN
    shapes = [struct((windows // 2, channels, LANES))] + [struct((n, channels, LANES)) for _, n in units]
    first, rest = deal_scratch(array, lengths)
    return pl.pallas_call(
        functools.partial(cot_kernel, units),
        out_shape=shapes,
        in_specs=[HBM] * 2,
        out_specs=[whole(o.shape) for o in shapes],
        grid=(1,),
        scratch_shapes=first + rest,
        compiler_params=PARAMS,
        cost_estimate=cost(array.size * 4, array.size * 8),
    )(*in_hbm([lengths, array]))


def prepare_weights(own, rec, windows, rows, channels):
    shapes = [struct((rows, 3 * channels), bf16)] * 4 + [struct((4 * channels, rows), bf16)] * 2
    return one_call(functools.partial(weights_kernel, windows), shapes, [own, rec])


MATMUL = 2 * 256 * 256 * 256


def unit_call(kernel, unit, smem, arrays, consts, outs, units_of_work, carried=(), weight=1):
    count = unit[1]
    specs = [SMEM] * len(smem)
    specs += [window_spec(a.shape, offset) for a, offset in arrays]
    specs += [whole(c.shape) for c in consts]
    aliases = {len(specs) + k: out for k, (out, _) in enumerate(carried)}
    specs += [pl.BlockSpec(memory_space=pl.ANY)] * len(carried)
    out_specs, shapes = [], []
    for shape, offset in outs:
        shapes.append(struct(shape))
        out_specs.append(whole(shape) if offset is None else window_spec(shape, offset))
    moved = sum(a.size * 4 * count // a.shape[0] for a, _ in arrays) + sum(c.size * c.dtype.itemsize for c in consts)
    return pl.pallas_call(
        kernel,
        out_shape=shapes,
        in_specs=specs,
        out_specs=out_specs,
        grid=(count,),
        input_output_aliases=aliases,
        compiler_params=PARAMS,
        cost_estimate=cost(units_of_work * MATMUL * count, moved, weight),
    )(*smem, *[a for a, _ in arrays], *consts, *[a for _, a in carried])


def swap(x, axis, bit):
    size = lax.axis_size(axis)
    return lax.ppermute(x, axis, [(i, i ^ bit) for i in range(size)])


def add_over(x, axis, bits):
    for bit in bits:
        x = x + swap(x, axis, bit)
    return x


def bits_of(size, start=1):
    bits, bit = [], start
    while bit < size:
        bits.append(bit)
        bit *= 2
    return bits


def hop(x, pairs):
    return lax.ppermute(x, "order", [(2 * a + side, 2 * b + side) for a, b in pairs for side in (0, 1)])


def inward(x):
    size = lax.axis_size("order")
    if size == 8:
        return hop(x, [(0, 1), (3, 2)])
    return lax.psum(x, "order", axis_index_groups=[list(range(side, size, 2)) for side in (0, 1)])


def middle(x):
    return hop(x, [(1, 2), (2, 1)]) if lax.axis_size("order") == 8 else x


def outward(x):
    return hop(x, [(1, 0), (2, 3)]) if lax.axis_size("order") == 8 else x


def join(kept, came):
    return kept + came if lax.axis_size("order") == 8 else came


def after(x, tokens):
    tokens = tokens if isinstance(tokens, tuple) else (tokens,)
    return lax.optimization_barrier((x, *tokens))[0]


WEIGHT = ((3,10),(10,10),(10,10),(10,10))
COT = (2, 2)
SER = (4,)
READ = (2, 2)
RANK = (2, 2)
PLAN = (
    "q", "R0", "Q", "R1", "hm0", "K0", "hm1", "K1", "ho0", "zm0", "ho1", "B0", "zm1", "zo0", "s0",
    "B1", "zo1", "M0", "s1", "M1", "st1", "b0", "st2", "se", "G", "F1", "gc", "gy", "F2",
)


def units_of(half, counts):
    counts = counts if sum(counts) == half else (1,) * half
    return [(sum(counts[:u]), counts[u]) for u in range(len(counts))]


def local(series, norm_gain, mode_in, mode_out, lengths, grad_out):
    channels = series.shape[0]
    windows = series.shape[1] // LEN
    half = windows // 2
    order_devices = lax.axis_size("order")
    line_length = order_devices // 2
    mode_count, rank_count = mode_in.shape[1], mode_in.shape[2]
    full_width = channels * order_devices
    rows = 2 * rank_count * mode_count
    cot_units, ser_units = units_of(half, COT), units_of(half, SER)
    read_units, rank_units = units_of(half, READ), units_of(half, RANK)

    legendre = [jnp.asarray(h) for h in halves(legendre_rows())]
    phase = jnp.asarray(phase_rows(mode_count))
    gain = norm_gain.reshape(1, channels)

    message, ser_own, *ser_rec = front(series, lengths, [mode_in, mode_out, gain], ser_units, rows)
    with jax.named_scope("message_x"):
        message_rec = swap(message, "order", 1)
    cot_own, *cot_rec = deal(after(grad_out, message), lengths, cot_units)
    message_rec = after(message_rec, cot_own)
    with jax.named_scope("cot_x"):
        cot_rec = [swap(c if u == 0 else after(c, message_rec), "order", 1) for u, c in enumerate(cot_rec)]
    down_own, down_rec, up_own, up_rec, down_both, up_both = prepare_weights(message, message_rec, windows, rows, channels)
    with jax.named_scope("squares_z1"):
        squares = message[:windows] + message_rec[:windows]
        squares_rec = swap(squares, "order", 2)
    with jax.named_scope("ser_x"):
        ser_rec = [swap(after(c, message_rec), "order", 1) for c in ser_rec]

    def windows_of(own, received, units, first, count):
        u, offset = locate(units, first)
        v, _ = locate(units, first + count - 1)
        if u < v:
            return [(own, first), (jnp.concatenate(received[u : v + 1], axis=0), offset)]
        return [(own, first), (received[u], offset)]

    chains = {}
    backs, branches, kept = {}, {}, {}
    state = {"squares": squares, "squares_rec": squares_rec, "token": up_own}

    def sums_of(name, token):
        return [(chains[name], 0), (after(chains[name + "out"], token), 0)]

    def do_read(u, token):
        first, count = read_units[u]
        own, rec = windows_of(cot_own, cot_rec, cot_units, first, count)
        (out,) = unit_call(
            read_kernel, read_units[u], [], [own, (after(rec[0], token), rec[1])],
            [up_own, up_rec, *legendre], [((count, rows, ORDER), 0)], 15, weight=WEIGHT[0][u],
        )
        start("h", u, out, inward)
        return out

    def do_rank(u, token):
        first, count = rank_units[u]
        own, rec = windows_of(ser_own, ser_rec, ser_units, first, count)
        (out,) = unit_call(
            functools.partial(rank_kernel, first, full_width), rank_units[u], [], [own, (after(rec[0], token), rec[1])],
            [state["squares"], down_own, down_rec, *legendre, phase], [((count, rows, ORDER), 0)], 21, weight=WEIGHT[1][u],
        )
        start("z", u, out, inward)
        return out

    def start(kind, u, value, move):
        name = f"{kind}{u}"
        chains[name] = value
        with jax.named_scope(f"{name}_{move.__name__}"):
            chains[name + ("out" if move is outward else "")] = (value, move(value)) if move is not outward else move(value)

    def do_join(kind, u, move, token):
        value, came = chains[f"{kind}{u}"]
        value = join(value, after(came, token))
        start(kind, u, value, move)
        if move is outward:
            chains[f"{kind}{u}"] = value
        return value

    def do_back(u, token):
        first, count = read_units[u]
        previous = [state["grad_in"]] if "grad_in" in state else []
        mine, theirs, state["grad_in"], dots = unit_call(
            functools.partial(back_kernel, first, full_width, line_length), read_units[u], [lengths],
            [*sums_of(f"h{u}", token), *windows_of(ser_own, ser_rec, ser_units, first, count)],
            [state["squares"], down_both, *legendre, phase, *previous],
            [((count, channels, LANES), 0)] * 2 + [((2 * channels, rows), None), ((count, STATS, 256), 0)], 24, weight=WEIGHT[2][u],
        )
        with jax.named_scope("scaled_x"):
            backs[u] = (mine, swap(theirs, "order", 1), dots)
        return state["grad_in"]

    def do_mix(u, token):
        first, count = rank_units[u]
        previous = [state["grad_mix"]] if "grad_mix" in state else []
        mine, theirs, state["grad_mix"] = unit_call(
            functools.partial(branch_kernel, first, line_length), rank_units[u], [lengths],
            [*sums_of(f"z{u}", token), *windows_of(ser_own, ser_rec, ser_units, first, count), *windows_of(cot_own, cot_rec, cot_units, first, count)],
            [up_both, *legendre, *previous],
            [((count, channels, LANES), 0)] * 2 + [((2 * channels + 8, rows), None)], 18, weight=WEIGHT[3][u],
        )
        branches[u] = mine
        with jax.named_scope("branch_x"):
            kept[u] = swap(theirs, "order", 1)
        return state["grad_mix"]

    def do_grads(token):
        grad_in, grad_mix, small = state["grad_in"], state["grad_mix"], state["small"]
        state["own"] = jnp.concatenate([grad_in[:channels], grad_mix[:channels], small], axis=0)
        rec = jnp.concatenate([grad_in[channels:], grad_mix[channels : 2 * channels], small], axis=0)
        with jax.named_scope("grads_x"):
            state["rec"] = swap(after(rec, token), "order", 1)
        return rec

    def do_series(token):
        count = len(read_units)
        return one_call(
            functools.partial(series_grad_kernel, read_units, full_width), struct(series.shape),
            [grad_out, series, state["squares"], state["small"], after(state["small_rec"], token)]
            + [backs[u][0] for u in range(count)] + [backs[u][1] for u in range(count)],
        )

    def do_layer(token):
        count = len(rank_units)
        return one_call(
            functools.partial(layer_kernel, rank_units), struct(series.shape),
            [after(series, token)] + [branches[u] for u in range(count)] + [kept[u] for u in range(count)],
        )

    for step in PLAN:
        name, token = step.rstrip("0123456789"), state["token"]
        u = int(step[len(name) :] or 0)
        if name == "q":
            with jax.named_scope("squares_z2"):
                out = state["squares"] + after(state["squares_rec"], token)
                state["squares"] = add_over(out, "order", bits_of(order_devices, 4))
        elif name == "s":
            out = after(backs[u][1], token)
            backs[u] = (backs[u][0], out, backs[u][2])
        elif name == "b":
            out = kept[u] = after(kept[u], token)
        elif name == "Q":
            out = state["squares"] = after(state["squares"], token)
        elif name == "R":
            out = do_read(u, token)
        elif name == "K":
            out = do_rank(u, token)
        elif name in ("hm", "zm"):
            out = do_join(name[0], u, middle, token)
        elif name in ("ho", "zo"):
            out = do_join(name[0], u, outward, token)
        elif name == "B":
            out = do_back(u, token)
        elif name == "M":
            out = do_mix(u, token)
        elif name == "st":
            with jax.named_scope("stats_z"):
                if u == 1:
                    out = jnp.concatenate([state["grad_mix"][2 * channels :]] + [backs[k][2].reshape(-1, 256) for k in range(len(read_units))], axis=0)
                else:
                    out = state["small"] + after(state["small_rec"], token)
                state["small"], state["small_rec"] = out, swap(out, "order", 1 << u)
        elif name == "se":
            with jax.named_scope("stats_z"):
                out = state["small"] + after(state["small_rec"], token)
                state["small"] = out = add_over(out, "order", bits_of(order_devices, 8))
        elif name == "G":
            out = do_grads(token)
        elif name == "gc":
            with jax.named_scope("grads_core"):
                rec = after(state["rec"], token)
                state["small_rec"] = rec[2 * channels :]
                out = state["own"] + rec
                state["own"], state["rec"] = out, swap(out, "batch", 1)
        elif name == "gy":
            with jax.named_scope("grads_y"):
                out = state["own"] + after(state["rec"], token)
                out = add_over(out, "batch", bits_of(lax.axis_size("batch") // 2, 2))
                state["own"], state["rec"] = out, swap(out, "batch", lax.axis_size("batch") // 2)
        elif name == "F":
            out = state[step] = do_layer(token) if u == 1 else do_series(token)
        state["token"] = out
    grad_mode_in, grad_mode_out, grad_gain, stream_rms = one_call(
        functools.partial(close_kernel, order_devices / full_width),
        [struct(mode_in.shape), struct(mode_out.shape), struct((1, channels)), struct((3,))],
        [state["own"], after(state["rec"], state["token"]), mode_in, gain], scalars_out=1,
    )
    return state["F1"], state["F2"], grad_gain.reshape(channels), grad_mode_in, grad_mode_out, stream_rms


def solution(mesh):
    wide = P("order", "batch")
    weight = P(None, None, None, "order")
    in_specs = (wide, P("order"), weight, weight, P("batch"), wide)
    out_specs = (wide, wide, P("order"), weight, weight, P())
    return jax.shard_map(local, mesh=mesh, in_specs=in_specs, out_specs=out_specs, check_vma=False)
```

```python
import functools
import math

import jax
import jax.numpy as jnp
import numpy as np
from jax import lax
from jax.experimental import pallas as pl
from jax.experimental.pallas import tpu as pltpu
from jax.sharding import PartitionSpec as P

ORDER = 256
LEN = 720
LANES = 768
BLOCK = 256
epsilon = 1e-06
f32 = jnp.float32
bf16 = jnp.bfloat16


def legendre_rows():
    coords = 1.0 - (2.0 * np.arange(LEN) + 1.0) / LEN
    rows = [np.ones(LEN), coords]
    for k in range(1, ORDER - 1):
        rows.append(((2.0 * k + 1.0) * coords * rows[k] - k * rows[k - 1]) / (k + 1.0))
    table = np.stack(rows) * np.sqrt((2.0 * np.arange(ORDER) + 1.0) / LEN)[:, None]
    out = np.zeros((ORDER, LANES))
    out[:, :LEN] = table[:, ::-1]
    return out


def phase_rows(mode_count):
    modes = np.arange(mode_count)[:, None]
    steps = np.arange(LANES)[None, :]
    now = 2.0 * np.pi * ((modes * steps) % LEN) / LEN
    nxt = 2.0 * np.pi * ((modes * (steps + 1)) % LEN) / LEN
    root = 1.0 / math.sqrt(LEN)
    rows = np.stack([np.cos(now), np.sin(now), np.cos(nxt) * root, np.sin(nxt) * root])
    return rows.astype(np.float32)


def halves(table):
    high = table.astype(np.float32).astype(jnp.bfloat16)
    low = (table - high.astype(np.float64)).astype(np.float32).astype(jnp.bfloat16)
    return high, low


def split(x):
    high = x.astype(bf16)
    return high, (x - high.astype(f32)).astype(bf16)


def nn(a, b):
    return lax.dot_general(a, b, (((1,), (0,)), ((), ())), preferred_element_type=f32)


def nt(a, b):
    return lax.dot_general(a, b, (((1,), (1,)), ((), ())), preferred_element_type=f32)


def three(dot, pairs, table):
    rows = pairs[0][0].shape[0]
    high = dot(jnp.concatenate([half for pair in pairs for half in pair], axis=0), table[0])
    low = dot(jnp.concatenate([pair[0] for pair in pairs], axis=0), table[1])
    out = []
    for k in range(len(pairs)):
        at = 2 * k * rows
        out.append(high[at : at + rows] + high[at + rows : at + 2 * rows] + low[k * rows : (k + 1) * rows])
    return out


def deep(x):
    high, low = split(x)
    return jnp.concatenate([high, low, high], axis=0)


def stacked(weights, pair, rows):
    first = nn(weights, pair[0])
    return first[:rows] + first[rows:] + nn(weights[:rows], pair[1])


def stacked_nt(left, pair, rows):
    first = nt(left, pair[0])
    return first[:rows] + first[rows:] + nt(left[:rows], pair[1])


def rotate(real, imag, cos, sin):
    modes = cos.shape[0]
    shape = (real.shape[0] // modes, modes, real.shape[1])
    real, imag = real.reshape(shape), imag.reshape(shape)
    cos, sin = cos[None], sin[None]
    flat = (shape[0] * modes, shape[2])
    return (real * cos + imag * sin).reshape(flat), (imag * cos - real * sin).reshape(flat)


def triangle():
    row = lax.broadcasted_iota(jnp.int32, (BLOCK, BLOCK), 0)
    col = lax.broadcasted_iota(jnp.int32, (BLOCK, BLOCK), 1)
    return jnp.where(row <= col, 1.0, 0.0).astype(bf16)


def block_sums(dot, x):
    rows, blocks = x.shape[0], LANES // BLOCK
    halves_of = split(x)
    stack = [half[:, b * BLOCK : (b + 1) * BLOCK] for half in halves_of for b in range(blocks)]
    sums = dot(jnp.concatenate(stack, axis=0), triangle())
    return [sums[b * rows : (b + 1) * rows] + sums[(blocks + b) * rows : (blocks + b + 1) * rows] for b in range(blocks)]


def running_sum(x):
    blocks = block_sums(nn, x)
    for b in range(1, len(blocks)):
        blocks[b] = blocks[b] + blocks[b - 1][:, BLOCK - 1 : BLOCK]
    return jnp.concatenate(blocks, axis=1)


def running_sum_back(x):
    blocks = block_sums(nt, x)
    for b in reversed(range(len(blocks) - 1)):
        blocks[b] = blocks[b] + blocks[b + 1][:, 0:1]
    return jnp.concatenate(blocks, axis=1)


def side_of():
    return lax.rem(lax.axis_index("order"), 2)


def at_line_end(line_length):
    line = lax.div(lax.axis_index("order"), 2)
    return jnp.logical_or(line == 0, line == line_length - 1)


def locate(units, j):
    u = max(k for k in range(len(units)) if units[k][0] <= j)
    return u, j - units[u][0]


def chunk_ends(windows):
    return [-(-LEN * min(w + 2, windows) // 128) * 128 for w in range(0, windows, 2)]


def deal_windows(split_at, len_hbm, hbm_ref, len_ref, buffer, sems, out_refs, use):
    lengths_copy = pltpu.make_async_copy(len_hbm, len_ref, sems.at[0])
    lengths_copy.start()
    own_ref, send_refs = out_refs[0], out_refs[1:]
    channels = hbm_ref.shape[0]
    windows = hbm_ref.shape[1] // LEN
    half = windows // 2
    ends = chunk_ends(windows)
    copies = []
    for c, end in enumerate(ends):
        at = slice(ends[c - 1] if c else 0, end)
        copies.append(pltpu.make_async_copy(hbm_ref.at[:, at], buffer.at[:, at], sems.at[1 + c]))
        copies[-1].start()
    lane = lax.broadcasted_iota(jnp.int32, (channels, LEN), 1)
    side = side_of()
    for ref in out_refs:
        ref[:, :, LANES - 128 :] = jnp.zeros((ref.shape[0], channels, 128), f32)
    lengths_copy.wait()
    for w in range(windows):
        if w % 2 == 0:
            copies[w // 2].wait()
        value = buffer[:, w * LEN : (w + 1) * LEN]
        value = jnp.where(lane < len_ref[w], value, 0.0)
        use(w, value)
        unit, at = locate(split_at, w % half)
        send_ref = send_refs[unit]
        mine = side == (0 if w < half else 1)

        @pl.when(mine)
        def _():
            own_ref[w % half, :, :LEN] = value

        @pl.when(jnp.logical_not(mine))
        def _():
            send_ref[at, :, :LEN] = value


PACK = 48
STATS = 8


def readout_columns(modes, channels):
    mode = lax.broadcasted_iota(jnp.int32, (modes, channels), 0)
    angle = mode.astype(f32) * (2.0 * math.pi / LEN)
    factor = jnp.where(mode == 0, 1.0, 2.0) * (1.0 / math.sqrt(LEN))
    return factor * jnp.cos(angle), factor * jnp.sin(angle)


def front_kernel(units, line_length, len_hbm, in_hbm, out_hbm, gain_hbm, x_hbm, message_ref, end_ref, *refs):
    out_refs, (len_ref, in_ref, out_ref, gain_ref, buffer, packed, sems, weight_sems) = refs[:-8], refs[-8:]
    windows = x_hbm.shape[1] // LEN
    end_ref[...] = jnp.where(at_line_end(line_length), jnp.ones(end_ref.shape, f32), 0.0)
    weights = [(in_hbm, in_ref), (out_hbm, out_ref), (gain_hbm, gain_ref)]
    weights = [pltpu.make_async_copy(a, b, weight_sems.at[k]) for k, (a, b) in enumerate(weights)]
    for copy in weights:
        copy.start()
    message_ref[...] = jnp.zeros(message_ref.shape, f32)

    def use(w, value):
        message_ref[w : w + 1, :LEN] = jnp.sum(value * value, axis=0, keepdims=True)

    deal_windows(units, len_hbm, x_hbm, len_ref, buffer, sems, out_refs, use)
    for copy in weights:
        copy.wait()
    modes, ranks, channels = in_ref.shape[1:]
    packed[...] = jnp.zeros(packed.shape, f32)
    read_real, read_imag = readout_columns(modes, channels)
    for r in range(ranks):
        real, imag = out_ref[0, :, r, :], out_ref[1, :, r, :]
        second = (read_real * real + read_imag * imag, read_imag * real - read_real * imag)
        for part in range(2):
            at = slice((part * ranks + r) * modes, (part * ranks + r + 1) * modes)
            packed[at, :channels] = in_ref[part, :, r, :] * gain_ref[...]
            packed[at, channels : 2 * channels] = second[part]
    rows = packed.shape[0]
    for k in range(-(-rows // PACK)):
        count = min(PACK, rows - k * PACK)
        message_ref[windows : windows + count, k * 128 : (k + 1) * 128] = packed[k * PACK : k * PACK + count]


def unpack(message_ref, windows, rows):
    pieces = []
    for k in range(-(-rows // PACK)):
        count = min(PACK, rows - k * PACK)
        pieces.append(message_ref[windows : windows + count, k * 128 : (k + 1) * 128])
    return jnp.concatenate(pieces, axis=0)


def cot_kernel(units, len_hbm, x_hbm, *refs):
    deal_windows(units, len_hbm, x_hbm, *refs[-3:], refs[:-3], lambda w, value: None)


def weights_kernel(windows, own_ref, rec_ref, down_own, down_rec, up_own, up_rec, down_both, up_both):
    rows, channels = down_own.shape[0], down_own.shape[1] // 3
    pieces = []
    for ref, down, up in ((own_ref, down_own, up_own), (rec_ref, down_rec, up_rec)):
        packed = unpack(ref, windows, rows)
        high, low = split(packed)
        down[...] = jnp.concatenate([high[:, :channels], high[:, :channels], low[:, :channels]], axis=1)
        upper = slice(channels, 2 * channels)
        up[...] = jnp.concatenate([high[:, upper], high[:, upper], low[:, upper]], axis=1)
        pieces.append(packed.T)
    for k, ref in ((0, down_both), (1, up_both)):
        at = slice(k * channels, (k + 1) * channels)
        both = jnp.concatenate([pieces[0][at], pieces[1][at]], axis=0)
        high, low = split(both)
        ref[...] = jnp.concatenate([high, low], axis=0)


def read_kernel(own_ref, rec_ref, up_own, up_rec, leg_high, leg_low, *out_refs):
    pairs = []
    for k in range(len(out_refs)):
        pairs.append(split(nn(up_own[...], deep(own_ref[k])) + nn(up_rec[...], deep(rec_ref[k]))))
    for ref, value in zip(out_refs, three(nt, pairs, (leg_high[...], leg_low[...]))):
        ref[...] = value


def inverse_rms(ss_ref, row, full_width):
    return lax.rsqrt(ss_ref[pl.ds(row, 1), :] * (1.0 / full_width) + epsilon)


def rank_kernel(first, full_width, own_ref, rec_ref, ss_ref, down_own, down_rec, leg_high, leg_low, phase_ref, *out_refs):
    row = side_of() * (ss_ref.shape[0] // 2) + first
    pairs = []
    for k in range(len(out_refs)):
        inv = inverse_rms(ss_ref, row + k, full_width)
        mixed = nn(down_own[...], deep(own_ref[k] * inv)) + nn(down_rec[...], deep(rec_ref[k] * inv))
        part = mixed.shape[0] // 2
        real, imag = rotate(mixed[:part], mixed[part:], phase_ref[0], phase_ref[1])
        total = running_sum(jnp.concatenate([real, imag], axis=0))
        real, imag = rotate(total[:part], total[part:], phase_ref[2], -phase_ref[3])
        pairs.append(split(jnp.concatenate([real, imag], axis=0)))
    for ref, value in zip(out_refs, three(nt, pairs, (leg_high[...], leg_low[...]))):
        ref[...] = value


def totals(line_length, refs):
    count, at_end = len(refs) // 2, at_line_end(line_length)
    return [split(jnp.where(at_end, refs[count + k][...], refs[k][...])) for k in range(count)]


def masked(value, length):
    lane = lax.broadcasted_iota(jnp.int32, value.shape, 1)
    return jnp.where(lane < length, value, 0.0)


def opening(refs, outs):
    return 0.0 if len(refs) == outs else refs[0][...], refs[-outs:]


def back_kernel(first, full_width, line_length, len_ref, own_ref, rec_ref, *refs):
    sums, refs = refs[: 2 * own_ref.shape[0]], refs[2 * own_ref.shape[0] :]
    ss_ref, down_both, leg_high, leg_low, phase_ref, *refs = refs
    grads, (own_out, rec_out, grad_out, inner_out) = opening(refs, 4)
    row = side_of() * (ss_ref.shape[0] // 2) + first
    channels = own_ref.shape[1]
    for k, total in enumerate(totals(line_length, sums)):
        (memory,) = three(nn, [total], (leg_high[...], leg_low[...]))
        part = memory.shape[0] // 2
        real, imag = rotate(memory[:part], memory[part:], phase_ref[2], phase_ref[3])
        back = running_sum_back(jnp.concatenate([real, imag], axis=0))
        real, imag = rotate(back[:part], back[part:], phase_ref[0], -phase_ref[1])
        pair = split(jnp.concatenate([real, imag], axis=0))
        scaled = masked(stacked(down_both[...], pair, 2 * channels), len_ref[row + k])
        own_out[k] = scaled[:channels]
        rec_out[k] = scaled[channels:]
        both = jnp.concatenate([own_ref[k], rec_ref[k]], axis=0)
        inner = jnp.sum(scaled * both, axis=0, keepdims=True)
        pieces = [inner[:, p * 256 : (p + 1) * 256] for p in range(LANES // 256)]
        inner_out[k] = jnp.concatenate(pieces + [jnp.zeros((STATS - len(pieces), 256), f32)], axis=0)
        high, low = split(both * inverse_rms(ss_ref, row + k, full_width))
        grads = grads + stacked_nt(jnp.concatenate([high, low], axis=0), pair, 2 * channels)
    grad_out[...] = grads


def branch_kernel(first, line_length, len_ref, ser_own, ser_rec, cot_own, cot_rec, *refs):
    sums, refs = refs[: 2 * ser_own.shape[0]], refs[2 * ser_own.shape[0] :]
    up_both, leg_high, leg_low, *refs = refs
    before, (own_out, rec_out, grad_out) = opening(refs, 3)
    channels = ser_own.shape[1]
    rows = 2 * channels
    windows = len_ref.shape[0]
    row = side_of() * (windows // 2) + first
    grads, stats = 0.0, [0.0, 0.0, 0.0]
    for k, total in enumerate(totals(line_length, sums)):
        pair = split(three(nn, [total], (leg_high[...], leg_low[...]))[0])
        branch = masked(stacked(up_both[...], pair, rows), len_ref[row + k])
        own_out[k] = branch[:channels]
        rec_out[k] = branch[channels:]
        high, low = split(jnp.concatenate([cot_own[k], cot_rec[k]], axis=0))
        grads = grads + stacked_nt(jnp.concatenate([high, low], axis=0), pair, rows)
        series = jnp.concatenate([ser_own[k], ser_rec[k]], axis=0)
        for i, v in enumerate((series, branch, series + branch)):
            stats[i] = stats[i] + jnp.sum(v * v, axis=0, keepdims=True)
    width = grads.shape[1]
    stats = [jnp.broadcast_to(jnp.sum(v, axis=1, keepdims=True), (1, width)) for v in stats]
    steps = functools.reduce(lambda a, b: a + b, [len_ref[w] for w in range(windows)]) if first == 0 else 0
    stats.append(jnp.full((1, width), steps, jnp.int32).astype(f32))
    stats = jnp.concatenate(stats + [jnp.zeros((STATS - 4, width), f32)], axis=0)
    grad_out[...] = before + jnp.concatenate([grads, stats], axis=0)


def layer_kernel(units, x_ref, *refs):
    own_refs, rec_refs, out_ref = refs[: len(units)], refs[len(units) : 2 * len(units)], refs[-1]
    windows = x_ref.shape[1] // LEN
    half = windows // 2
    first_side = side_of() == 0
    for w in range(windows):
        u, j = locate(units, w % half)
        value = jnp.where(first_side == (w < half), own_refs[u][j], rec_refs[u][j])
        at = slice(w * LEN, (w + 1) * LEN)
        out_ref[:, at] = x_ref[:, at] + value[:, :LEN]


def inner_row(small_ref, j):
    row = STATS * (1 + j)
    return jnp.concatenate([small_ref[row + p : row + p + 1, :] for p in range(LANES // 256)], axis=1)


def series_grad_kernel(units, full_width, cot_ref, x_ref, ss_ref, in_own, in_rec, *refs):
    own_refs, rec_refs, out_ref = refs[: len(units)], refs[len(units) : 2 * len(units)], refs[-1]
    windows = x_ref.shape[1] // LEN
    half = windows // 2
    first_side = side_of() == 0
    for w in range(windows):
        u, j = locate(units, w % half)
        keep = first_side == (w < half)
        scaled = jnp.where(keep, own_refs[u][j], rec_refs[u][j])[:, :LEN]
        inner = jnp.where(keep, inner_row(in_own, w % half), inner_row(in_rec, w % half))[:, :LEN]
        inv = inverse_rms(ss_ref, w, full_width)[:, :LEN]
        at = slice(w * LEN, (w + 1) * LEN)
        shift = inv * inv * inner * (1.0 / full_width)
        out_ref[:, at] = cot_ref[:, at] + inv * (scaled - x_ref[:, at] * shift)


def close_kernel(share, own_ref, rec_ref, in_ref, gain_ref, grad_in_ref, grad_out_ref, grad_gain_ref, rms_ref):
    modes, ranks, channels = in_ref.shape[1:]
    sums = own_ref[...] + rec_ref[...]
    into, mix, stats = sums[:channels].T, sums[channels : 2 * channels].T, sums[2 * channels : 2 * channels + STATS]
    total = jnp.zeros((modes, channels), f32)
    read_real, read_imag = readout_columns(modes, channels)
    for r in range(ranks):
        pieces = []
        for part in range(2):
            at = slice((part * ranks + r) * modes, (part * ranks + r + 1) * modes)
            grad = into[at]
            total = total + grad * in_ref[part, :, r, :]
            grad_in_ref[part, :, r, :] = grad * gain_ref[...]
            pieces.append(mix[at])
        grad_out_ref[0, :, r, :] = read_real * pieces[0] + read_imag * pieces[1]
        grad_out_ref[1, :, r, :] = read_imag * pieces[0] - read_real * pieces[1]
    grad_gain_ref[...] = jnp.sum(total, axis=0, keepdims=True)
    rms = jnp.sqrt(stats * share / stats[3:4])
    for k in range(3):
        rms_ref[k] = rms[k, 0]


def whole(shape):
    return pl.BlockSpec(shape, lambda *_: (0,) * len(shape))


SMEM = pl.BlockSpec(memory_space=pltpu.SMEM)
PARAMS = pltpu.CompilerParams(vmem_limit_bytes=8 * 1024 * 1024)


def cost(flops, byte_count, weight=1):
    return pl.CostEstimate(flops=int(flops * weight), bytes_accessed=int(byte_count * weight), transcendentals=0)


def struct(shape, dtype=f32):
    return jax.ShapeDtypeStruct(shape, dtype)


def one_call(kernel, outs, args, smem=0, scalars_out=0):
    single = not isinstance(outs, list)
    shapes = [outs] if single else outs
    specs = [SMEM] * smem + [whole(a.shape) for a in args[smem:]]
    moved = sum(a.size * a.dtype.itemsize for a in args) + sum(math.prod(o.shape) * 4 for o in shapes)
    result = pl.pallas_call(
        kernel,
        out_shape=shapes,
        in_specs=specs,
        out_specs=[whole(o.shape) for o in shapes[: len(shapes) - scalars_out]] + [SMEM] * scalars_out,
        grid=(1,),
        compiler_params=PARAMS,
        cost_estimate=cost(moved, moved),
    )(*args)
    return result[0] if single else result


HBM = pl.BlockSpec(memory_space=pltpu.MemorySpace.HBM)


def in_hbm(arrays):
    return [pltpu.with_memory_space_constraint(a, pltpu.MemorySpace.HBM) for a in arrays]


def deal_scratch(array, lengths):
    windows = array.shape[1] // LEN
    return [pltpu.SMEM(lengths.shape, jnp.int32)], [
        pltpu.VMEM(array.shape, f32),
        pltpu.SemaphoreType.DMA((1 + len(chunk_ends(windows)),)),
    ]


def front(series, lengths, weights, units, rows, line_length):
    channels, windows = series.shape[0], series.shape[1] // LEN
    shapes = [struct((windows + PACK, LANES)), struct((8, ORDER)), struct((windows // 2, channels, LANES))]
    shapes += [struct((n, channels, LANES)) for _, n in units]
    first, (buffer, sems) = deal_scratch(series, lengths)
    scratch = first + [pltpu.VMEM(a.shape, f32) for a in weights] + [buffer, pltpu.VMEM((rows, 128), f32), sems]
    return pl.pallas_call(
        functools.partial(front_kernel, units, line_length),
        out_shape=shapes,
        in_specs=[HBM] * (2 + len(weights)),
        out_specs=[whole(o.shape) for o in shapes],
        grid=(1,),
        scratch_shapes=scratch + [pltpu.SemaphoreType.DMA((len(weights),))],
        compiler_params=PARAMS,
        cost_estimate=cost(series.size * 4, series.size * 8),
    )(*in_hbm([lengths, *weights, series]))


def deal(array, lengths, units):
    channels, windows = array.shape[0], array.shape[1] // LEN
    shapes = [struct((windows // 2, channels, LANES))] + [struct((n, channels, LANES)) for _, n in units]
    first, rest = deal_scratch(array, lengths)
    return pl.pallas_call(
        functools.partial(cot_kernel, units),
        out_shape=shapes,
        in_specs=[HBM] * 2,
        out_specs=[whole(o.shape) for o in shapes],
        grid=(1,),
        scratch_shapes=first + rest,
        compiler_params=PARAMS,
        cost_estimate=cost(array.size * 4, array.size * 8),
    )(*in_hbm([lengths, array]))


def prepare_weights(own, rec, windows, rows, channels):
    shapes = [struct((rows, 3 * channels), bf16)] * 4 + [struct((4 * channels, rows), bf16)] * 2
    return one_call(functools.partial(weights_kernel, windows), shapes, [own, rec])


MATMUL = 2 * 256 * 256 * 256


def unit_call(kernel, unit, smem, arrays, consts, outs, units_of_work, weight=1):
    count = unit[1]
    specs = [SMEM] * len(smem)
    assert all(o % count == 0 for _, o in arrays)
    specs += [pl.BlockSpec((count,) + a.shape[1:], lambda i, o=o // count, r=a.ndim - 1: (o,) + (0,) * r) for a, o in arrays]
    specs += [whole(c.shape) for c in consts]
    moved = sum(a.size * 4 * count // a.shape[0] for a, _ in arrays) + sum(c.size * c.dtype.itemsize for c in consts)
    return pl.pallas_call(
        kernel,
        out_shape=[struct(shape) for shape in outs],
        in_specs=specs,
        out_specs=[whole(shape) for shape in outs],
        grid=(1,),
        compiler_params=PARAMS,
        cost_estimate=cost(units_of_work * MATMUL * count, moved, weight),
    )(*smem, *[a for a, _ in arrays], *consts)


def swap(x, axis, bit):
    size = lax.axis_size(axis)
    return lax.ppermute(x, axis, [(i, i ^ bit) for i in range(size)])


def add_over(x, axis, bits):
    for bit in bits:
        x = x + swap(x, axis, bit)
    return x


def bits_of(size, start=1):
    bits, bit = [], start
    while bit < size:
        bits.append(bit)
        bit *= 2
    return bits


def cross(x):
    batch, order = lax.axis_size("batch"), lax.axis_size("order")
    pairs = []
    for b in range(batch):
        for o in range(order):
            inner = o // 2 in (1, 2)
            pairs.append((b * order + o, b * order + (o ^ 6) if inner else (b ^ 1) * order + o))
    return lax.ppermute(x, ("batch", "order"), pairs)


def line_sum(x):
    size = lax.axis_size("order")
    return lax.psum(x, "order", axis_index_groups=[list(range(side, size, 2)) for side in (0, 1)])


def after(x, tokens):
    tokens = tokens if isinstance(tokens, tuple) else (tokens,)
    return lax.optimization_barrier((x, *tokens))[0]


WEIGHT = ((10,) * 4, (10,) * 4, (10,) * 4, (10,) * 4)
COT = (1, 1, 2)
SER = (2, 2)
READ = (1, 1, 2)
RANK = (2, 2)
BACK = (2, 2)
MIX = (2, 1, 1)
LAG = 3
PLAN = (
    "q", "R0", "e0", "R1", "e1", "Q", "m0", "R2", "e2", "m1", "e3", "m2", "K0", "e4", "m3", "e5",
    "m4", "K1", "e6", "m5", "B0", "e7", "m6", "e8", "m7", "s0", "B1", "e9", "M0", "e10", "M1",
    "s1", "M2", "st1", "b0", "st2", "b1", "se", "G", "F1", "gc", "gy", "F2",
)


def units_of(half, counts):
    counts = counts if sum(counts) == half else (1,) * half
    return [(sum(counts[:u]), counts[u]) for u in range(len(counts))]


def local(series, norm_gain, mode_in, mode_out, lengths, grad_out):
    channels = series.shape[0]
    windows = series.shape[1] // LEN
    half = windows // 2
    order_devices = lax.axis_size("order")
    line_length = order_devices // 2
    mode_count, rank_count = mode_in.shape[1], mode_in.shape[2]
    full_width = channels * order_devices
    rows = 2 * rank_count * mode_count
    cot_units, ser_units = units_of(half, COT), units_of(half, SER)
    read_units, rank_units = units_of(half, READ), units_of(half, RANK)
    back_units, mix_units = units_of(half, BACK), units_of(half, MIX)

    legendre = [jnp.asarray(h) for h in halves(legendre_rows())]
    phase = jnp.asarray(phase_rows(mode_count))
    gain = norm_gain.reshape(1, channels)

    message, end_mask, ser_own, *ser_rec = front(series, lengths, [mode_in, mode_out, gain], ser_units, rows, line_length)
    with jax.named_scope("message_x"):
        message_rec = swap(message, "order", 1)
    cot_own, *cot_rec = deal(after(grad_out, message), lengths, cot_units)
    message_rec = after(message_rec, cot_own)
    with jax.named_scope("cot_x"):
        cot_rec = [swap(c if u == 0 else after(c, message_rec), "order", 1) for u, c in enumerate(cot_rec)]
    down_own, down_rec, up_own, up_rec, down_both, up_both = prepare_weights(message, message_rec, windows, rows, channels)
    with jax.named_scope("squares_z1"):
        squares = message[:windows] + message_rec[:windows]
        squares_rec = swap(squares, "order", 2)
    with jax.named_scope("ser_x"):
        ser_rec = [swap(after(c, message_rec), "order", 1) for c in ser_rec]

    def windows_of(own, received, units, first, count):
        u, offset = locate(units, first)
        v, _ = locate(units, first + count - 1)
        if u < v:
            return [(own, first), (jnp.concatenate(received[u : v + 1], axis=0), offset)]
        return [(own, first), (received[u], offset)]

    chained = order_devices == 8
    at_end = end_mask[:1] > 0.5
    parts, pairs, sends, came, crossed = {}, {}, {}, {}, {}
    backs, branches, kept = {}, {}, {}
    state = {"squares": squares, "squares_rec": squares_rec, "token": up_own}

    def do_read(u, token):
        first, count = read_units[u]
        own, rec = windows_of(cot_own, cot_rec, cot_units, first, count)
        outs = unit_call(
            read_kernel, read_units[u], [], [own, (after(rec[0], token), rec[1])],
            [up_own, up_rec, *legendre], [(rows, ORDER)] * count, 15, weight=WEIGHT[0][u],
        )
        for k in range(count):
            parts[first + k] = outs[k]
        return outs[0]

    def do_rank(u, token):
        first, count = rank_units[u]
        own, rec = windows_of(ser_own, ser_rec, ser_units, first, count)
        outs = unit_call(
            functools.partial(rank_kernel, first, full_width), rank_units[u], [], [own, (after(rec[0], token), rec[1])],
            [state["squares"], down_own, down_rec, *legendre, phase], [(rows, ORDER)] * count, 21, weight=WEIGHT[1][u],
        )
        for k in range(count):
            parts[half + first + k] = outs[k]
        return outs[0]

    def do_swap(k, token):
        if not chained:
            if k < windows:
                came[k + LAG] = sends[k + LAG] = line_sum(after(parts[k], token))
            return token
        done = k - LAG
        if done < 0:
            out = after(parts[k], token)
        else:
            out = pairs[done] + after(crossed[done], token)
            if k < windows:
                out = jnp.where(at_end, parts[k], out)
        with jax.named_scope(f"e{k}"):
            sends[k], came[k] = out, swap(out, "order", 2)
        return out

    def do_cross(k, token):
        if not chained:
            return token
        out = pairs[k] = parts[k] + after(came[k], token)
        with jax.named_scope(f"m{k}"):
            crossed[k] = cross(out)
        return out

    def sums_of(first, count, token):
        at = range(first + LAG, first + LAG + count)
        return [sends[k] for k in at] + [after(came[k], token) for k in at]

    def do_back(u, token):
        first, count = back_units[u]
        previous = [state["grad_in"]] if "grad_in" in state else []
        mine, theirs, state["grad_in"], dots = unit_call(
            functools.partial(back_kernel, first, full_width, line_length), back_units[u], [lengths],
            windows_of(ser_own, ser_rec, ser_units, first, count),
            [*sums_of(first, count, token), state["squares"], down_both, *legendre, phase, *previous],
            [(count, channels, LANES)] * 2 + [(2 * channels, rows), (count, STATS, 256)], 24, weight=WEIGHT[2][u],
        )
        with jax.named_scope("scaled_x"):
            backs[u] = (mine, swap(theirs, "order", 1), dots)
        return state["grad_in"]

    def do_mix(u, token):
        first, count = mix_units[u]
        previous = [state["grad_mix"]] if "grad_mix" in state else []
        mine, theirs, state["grad_mix"] = unit_call(
            functools.partial(branch_kernel, first, line_length), mix_units[u], [lengths],
            [*windows_of(ser_own, ser_rec, ser_units, first, count), *windows_of(cot_own, cot_rec, cot_units, first, count)],
            [*sums_of(half + first, count, token), up_both, *legendre, *previous],
            [(count, channels, LANES)] * 2 + [(2 * channels + STATS, rows)], 18, weight=WEIGHT[3][u],
        )
        branches[u] = mine
        with jax.named_scope("branch_x"):
            kept[u] = swap(theirs, "order", 1)
        return state["grad_mix"]

    def do_grads(token):
        grad_in, grad_mix, small = state["grad_in"], state["grad_mix"], state["small"]
        state["own"] = jnp.concatenate([grad_in[:channels], grad_mix[:channels], small], axis=0)
        rec = jnp.concatenate([grad_in[channels:], grad_mix[channels : 2 * channels], small], axis=0)
        with jax.named_scope("grads_x"):
            state["rec"] = swap(after(rec, token), "order", 1)
        return rec

    def do_series(token):
        count = len(back_units)
        return one_call(
            functools.partial(series_grad_kernel, back_units, full_width), struct(series.shape),
            [grad_out, series, state["squares"], state["small"], after(state["small_rec"], token)]
            + [backs[u][0] for u in range(count)] + [backs[u][1] for u in range(count)],
        )

    def do_layer(token):
        count = len(mix_units)
        return one_call(
            functools.partial(layer_kernel, mix_units), struct(series.shape),
            [after(series, token)] + [branches[u] for u in range(count)] + [kept[u] for u in range(count)],
        )

    for step in PLAN:
        name, token = step.rstrip("0123456789"), state["token"]
        u = int(step[len(name) :] or 0)
        if name == "q":
            with jax.named_scope("squares_z2"):
                out = state["squares"] + after(state["squares_rec"], token)
                state["squares"] = add_over(out, "order", bits_of(order_devices, 4))
        elif name == "s":
            out = after(backs[u][1], token)
            backs[u] = (backs[u][0], out, backs[u][2])
        elif name == "b":
            out = kept[u] = after(kept[u], token)
        elif name == "Q":
            out = state["squares"] = after(state["squares"], token)
        elif name == "R":
            out = do_read(u, token)
        elif name == "K":
            out = do_rank(u, token)
        elif name == "e":
            out = do_swap(u, token)
        elif name == "m":
            out = do_cross(u, token)
        elif name == "B":
            out = do_back(u, token)
        elif name == "M":
            out = do_mix(u, token)
        elif name == "st":
            with jax.named_scope("stats_z"):
                if u == 1:
                    out = jnp.concatenate([state["grad_mix"][2 * channels :]] + [backs[k][2].reshape(-1, 256) for k in range(len(back_units))], axis=0)
                else:
                    out = state["small"] + after(state["small_rec"], token)
                state["small"], state["small_rec"] = out, swap(out, "order", 1 << u)
        elif name == "se":
            with jax.named_scope("stats_z"):
                out = state["small"] + after(state["small_rec"], token)
                state["small"] = out = add_over(out, "order", bits_of(order_devices, 8))
        elif name == "G":
            out = do_grads(token)
        elif name == "gc":
            with jax.named_scope("grads_core"):
                rec = after(state["rec"], token)
                state["small_rec"] = rec[2 * channels :]
                out = state["own"] + rec
                state["own"], state["rec"] = out, swap(out, "batch", 1)
        elif name == "gy":
            with jax.named_scope("grads_y"):
                out = state["own"] + after(state["rec"], token)
                out = add_over(out, "batch", bits_of(lax.axis_size("batch") // 2, 2))
                state["own"], state["rec"] = out, swap(out, "batch", lax.axis_size("batch") // 2)
        elif name == "F":
            out = state[step] = do_layer(token) if u == 1 else do_series(token)
        state["token"] = out
    grad_mode_in, grad_mode_out, grad_gain, stream_rms = one_call(
        functools.partial(close_kernel, order_devices / full_width),
        [struct(mode_in.shape), struct(mode_out.shape), struct((1, channels)), struct((3,))],
        [state["own"], after(state["rec"], state["token"]), mode_in, gain], scalars_out=1,
    )
    return state["F1"], state["F2"], grad_gain.reshape(channels), grad_mode_in, grad_mode_out, stream_rms


def solution(mesh):
    wide = P("order", "batch")
    weight = P(None, None, None, "order")
    in_specs = (wide, P("order"), weight, weight, P("batch"), wide)
    out_specs = (wide, wide, P("order"), weight, weight, P())
    return jax.shard_map(local, mesh=mesh, in_specs=in_specs, out_specs=out_specs, check_vma=False)
```

```python
import functools
import math

import jax
import jax.numpy as jnp
import numpy as np
from jax import lax
from jax.experimental import pallas as pl
from jax.experimental.pallas import tpu as pltpu
from jax.sharding import PartitionSpec as P

ORDER = 256
LEN = 720
LANES = 768
BLOCK = 256
epsilon = 1e-06
f32 = jnp.float32
bf16 = jnp.bfloat16


def legendre_rows():
    coords = 1.0 - (2.0 * np.arange(LEN) + 1.0) / LEN
    rows = [np.ones(LEN), coords]
    for k in range(1, ORDER - 1):
        rows.append(((2.0 * k + 1.0) * coords * rows[k] - k * rows[k - 1]) / (k + 1.0))
    table = np.stack(rows) * np.sqrt((2.0 * np.arange(ORDER) + 1.0) / LEN)[:, None]
    out = np.zeros((ORDER, LANES))
    out[:, :LEN] = table[:, ::-1]
    return out


def phase_rows(mode_count):
    modes = np.arange(mode_count)[:, None]
    steps = np.arange(LANES)[None, :]
    now = 2.0 * np.pi * ((modes * steps) % LEN) / LEN
    nxt = 2.0 * np.pi * ((modes * (steps + 1)) % LEN) / LEN
    root = 1.0 / math.sqrt(LEN)
    rows = np.stack([np.cos(now), np.sin(now), np.cos(nxt) * root, np.sin(nxt) * root])
    return rows.astype(np.float32)


def halves(table):
    high = table.astype(np.float32).astype(jnp.bfloat16)
    low = (table - high.astype(np.float64)).astype(np.float32).astype(jnp.bfloat16)
    return high, low


def split(x):
    high = x.astype(bf16)
    return high, (x - high.astype(f32)).astype(bf16)


def nn(a, b):
    return lax.dot_general(a, b, (((1,), (0,)), ((), ())), preferred_element_type=f32)


def nt(a, b):
    return lax.dot_general(a, b, (((1,), (1,)), ((), ())), preferred_element_type=f32)


def three(dot, pairs, table):
    rows = pairs[0][0].shape[0]
    high = dot(jnp.concatenate([half for pair in pairs for half in pair], axis=0), table[0])
    low = dot(jnp.concatenate([pair[0] for pair in pairs], axis=0), table[1])
    out = []
    for k in range(len(pairs)):
        at = 2 * k * rows
        out.append(high[at : at + rows] + high[at + rows : at + 2 * rows] + low[k * rows : (k + 1) * rows])
    return out


def deep(x):
    high, low = split(x)
    return jnp.concatenate([high, low, high], axis=0)


def stacked(weights, pair, rows):
    first = nn(weights, pair[0])
    return first[:rows] + first[rows:] + nn(weights[:rows], pair[1])


def stacked_nt(left, pair, rows):
    first = nt(left, pair[0])
    return first[:rows] + first[rows:] + nt(left[:rows], pair[1])


def rotate(real, imag, cos, sin):
    modes = cos.shape[0]
    shape = (real.shape[0] // modes, modes, real.shape[1])
    real, imag = real.reshape(shape), imag.reshape(shape)
    cos, sin = cos[None], sin[None]
    flat = (shape[0] * modes, shape[2])
    return (real * cos + imag * sin).reshape(flat), (imag * cos - real * sin).reshape(flat)


def triangle():
    row = lax.broadcasted_iota(jnp.int32, (BLOCK, BLOCK), 0)
    col = lax.broadcasted_iota(jnp.int32, (BLOCK, BLOCK), 1)
    return jnp.where(row <= col, 1.0, 0.0).astype(bf16)


def block_sums(dot, x):
    rows, blocks = x.shape[0], LANES // BLOCK
    halves_of = split(x)
    stack = [half[:, b * BLOCK : (b + 1) * BLOCK] for half in halves_of for b in range(blocks)]
    sums = dot(jnp.concatenate(stack, axis=0), triangle())
    return [sums[b * rows : (b + 1) * rows] + sums[(blocks + b) * rows : (blocks + b + 1) * rows] for b in range(blocks)]


def running_sum(x):
    blocks = block_sums(nn, x)
    for b in range(1, len(blocks)):
        blocks[b] = blocks[b] + blocks[b - 1][:, BLOCK - 1 : BLOCK]
    return jnp.concatenate(blocks, axis=1)


def running_sum_back(x):
    blocks = block_sums(nt, x)
    for b in reversed(range(len(blocks) - 1)):
        blocks[b] = blocks[b] + blocks[b + 1][:, 0:1]
    return jnp.concatenate(blocks, axis=1)


def side_of():
    return lax.rem(lax.axis_index("order"), 2)


def at_line_end(line_length):
    line = lax.div(lax.axis_index("order"), 2)
    return jnp.logical_or(line == 0, line == line_length - 1)


def locate(units, j):
    u = max(k for k in range(len(units)) if units[k][0] <= j)
    return u, j - units[u][0]


def chunk_ends(windows):
    return [-(-LEN * min(w + 2, windows) // 128) * 128 for w in range(0, windows, 2)]


def deal_windows(split_at, len_hbm, hbm_ref, len_ref, buffer, sems, out_refs, use):
    lengths_copy = pltpu.make_async_copy(len_hbm, len_ref, sems.at[0])
    lengths_copy.start()
    own_ref, send_refs = out_refs[0], out_refs[1:]
    channels = hbm_ref.shape[0]
    windows = hbm_ref.shape[1] // LEN
    half = windows // 2
    ends = chunk_ends(windows)
    copies = []
    for c, end in enumerate(ends):
        at = slice(ends[c - 1] if c else 0, end)
        copies.append(pltpu.make_async_copy(hbm_ref.at[:, at], buffer.at[:, at], sems.at[1 + c]))
        copies[-1].start()
    lane = lax.broadcasted_iota(jnp.int32, (channels, LEN), 1)
    side = side_of()
    for ref in out_refs:
        ref[:, :, LANES - 128 :] = jnp.zeros((ref.shape[0], channels, 128), f32)
    lengths_copy.wait()
    for w in range(windows):
        if w % 2 == 0:
            copies[w // 2].wait()
        value = buffer[:, w * LEN : (w + 1) * LEN]
        value = jnp.where(lane < len_ref[w], value, 0.0)
        use(w, value)
        unit, at = locate(split_at, w % half)
        send_ref = send_refs[unit]
        mine = side == (0 if w < half else 1)

        @pl.when(mine)
        def _():
            own_ref[w % half, :, :LEN] = value

        @pl.when(jnp.logical_not(mine))
        def _():
            send_ref[at, :, :LEN] = value


PACK = 48
STATS = 8


def readout_columns(modes, channels):
    mode = lax.broadcasted_iota(jnp.int32, (modes, channels), 0)
    angle = mode.astype(f32) * (2.0 * math.pi / LEN)
    factor = jnp.where(mode == 0, 1.0, 2.0) * (1.0 / math.sqrt(LEN))
    return factor * jnp.cos(angle), factor * jnp.sin(angle)


def front_kernel(units, line_length, len_hbm, in_hbm, out_hbm, gain_hbm, x_hbm, message_ref, end_ref, *refs):
    out_refs, (len_ref, in_ref, out_ref, gain_ref, buffer, packed, sems, weight_sems) = refs[:-8], refs[-8:]
    windows = x_hbm.shape[1] // LEN
    end_ref[...] = jnp.where(at_line_end(line_length), jnp.ones(end_ref.shape, f32), 0.0)
    weights = [(in_hbm, in_ref), (out_hbm, out_ref), (gain_hbm, gain_ref)]
    weights = [pltpu.make_async_copy(a, b, weight_sems.at[k]) for k, (a, b) in enumerate(weights)]
    for copy in weights:
        copy.start()
    message_ref[...] = jnp.zeros(message_ref.shape, f32)

    def use(w, value):
        message_ref[w : w + 1, :LEN] = jnp.sum(value * value, axis=0, keepdims=True)

    deal_windows(units, len_hbm, x_hbm, len_ref, buffer, sems, out_refs, use)
    for copy in weights:
        copy.wait()
    modes, ranks, channels = in_ref.shape[1:]
    packed[...] = jnp.zeros(packed.shape, f32)
    read_real, read_imag = readout_columns(modes, channels)
    for r in range(ranks):
        real, imag = out_ref[0, :, r, :], out_ref[1, :, r, :]
        second = (read_real * real + read_imag * imag, read_imag * real - read_real * imag)
        for part in range(2):
            at = slice((part * ranks + r) * modes, (part * ranks + r + 1) * modes)
            packed[at, :channels] = in_ref[part, :, r, :] * gain_ref[...]
            packed[at, channels : 2 * channels] = second[part]
    rows = packed.shape[0]
    for k in range(-(-rows // PACK)):
        count = min(PACK, rows - k * PACK)
        message_ref[windows : windows + count, k * 128 : (k + 1) * 128] = packed[k * PACK : k * PACK + count]


def unpack(message_ref, windows, rows):
    pieces = []
    for k in range(-(-rows // PACK)):
        count = min(PACK, rows - k * PACK)
        pieces.append(message_ref[windows : windows + count, k * 128 : (k + 1) * 128])
    return jnp.concatenate(pieces, axis=0)


def cot_kernel(units, len_hbm, x_hbm, *refs):
    deal_windows(units, len_hbm, x_hbm, *refs[-3:], refs[:-3], lambda w, value: None)


def weights_kernel(windows, own_ref, rec_ref, down_own, down_rec, up_own, up_rec, down_both, up_both):
    rows, channels = down_own.shape[0], down_own.shape[1] // 3
    pieces = []
    for ref, down, up in ((own_ref, down_own, up_own), (rec_ref, down_rec, up_rec)):
        packed = unpack(ref, windows, rows)
        high, low = split(packed)
        down[...] = jnp.concatenate([high[:, :channels], high[:, :channels], low[:, :channels]], axis=1)
        upper = slice(channels, 2 * channels)
        up[...] = jnp.concatenate([high[:, upper], high[:, upper], low[:, upper]], axis=1)
        pieces.append(packed.T)
    for k, ref in ((0, down_both), (1, up_both)):
        at = slice(k * channels, (k + 1) * channels)
        both = jnp.concatenate([pieces[0][at], pieces[1][at]], axis=0)
        high, low = split(both)
        ref[...] = jnp.concatenate([high, low], axis=0)


def read_kernel(own_ref, rec_ref, up_own, up_rec, leg_high, leg_low, *out_refs):
    pairs = []
    for k in range(len(out_refs)):
        pairs.append(split(nn(up_own[...], deep(own_ref[k])) + nn(up_rec[...], deep(rec_ref[k]))))
    for ref, value in zip(out_refs, three(nt, pairs, (leg_high[...], leg_low[...]))):
        ref[...] = value


def inverse_rms(ss_ref, row, full_width):
    return lax.rsqrt(ss_ref[pl.ds(row, 1), :] * (1.0 / full_width) + epsilon)


def rank_kernel(first, full_width, own_ref, rec_ref, ss_ref, down_own, down_rec, leg_high, leg_low, phase_ref, *out_refs):
    row = side_of() * (ss_ref.shape[0] // 2) + first
    pairs = []
    for k in range(len(out_refs)):
        inv = inverse_rms(ss_ref, row + k, full_width)
        mixed = nn(down_own[...], deep(own_ref[k] * inv)) + nn(down_rec[...], deep(rec_ref[k] * inv))
        part = mixed.shape[0] // 2
        real, imag = rotate(mixed[:part], mixed[part:], phase_ref[0], phase_ref[1])
        total = running_sum(jnp.concatenate([real, imag], axis=0))
        real, imag = rotate(total[:part], total[part:], phase_ref[2], -phase_ref[3])
        pairs.append(split(jnp.concatenate([real, imag], axis=0)))
    for ref, value in zip(out_refs, three(nt, pairs, (leg_high[...], leg_low[...]))):
        ref[...] = value


def totals(line_length, refs):
    count, at_end = len(refs) // 2, at_line_end(line_length)
    return [split(jnp.where(at_end, refs[count + k][...], refs[k][...])) for k in range(count)]


def masked(value, length):
    lane = lax.broadcasted_iota(jnp.int32, value.shape, 1)
    return jnp.where(lane < length, value, 0.0)


def opening(refs, outs):
    return 0.0 if len(refs) == outs else refs[0][...], refs[-outs:]


def back_kernel(first, full_width, line_length, len_ref, own_ref, rec_ref, *refs):
    sums, refs = refs[: 2 * own_ref.shape[0]], refs[2 * own_ref.shape[0] :]
    ss_ref, down_both, leg_high, leg_low, phase_ref, *refs = refs
    grads, (own_out, rec_out, grad_out, inner_out) = opening(refs, 4)
    row = side_of() * (ss_ref.shape[0] // 2) + first
    channels = own_ref.shape[1]
    for k, total in enumerate(totals(line_length, sums)):
        (memory,) = three(nn, [total], (leg_high[...], leg_low[...]))
        part = memory.shape[0] // 2
        real, imag = rotate(memory[:part], memory[part:], phase_ref[2], phase_ref[3])
        back = running_sum_back(jnp.concatenate([real, imag], axis=0))
        real, imag = rotate(back[:part], back[part:], phase_ref[0], -phase_ref[1])
        pair = split(jnp.concatenate([real, imag], axis=0))
        scaled = masked(stacked(down_both[...], pair, 2 * channels), len_ref[row + k])
        own_out[k] = scaled[:channels]
        rec_out[k] = scaled[channels:]
        both = jnp.concatenate([own_ref[k], rec_ref[k]], axis=0)
        inner = jnp.sum(scaled * both, axis=0, keepdims=True)
        pieces = [inner[:, p * 256 : (p + 1) * 256] for p in range(LANES // 256)]
        inner_out[k] = jnp.concatenate(pieces + [jnp.zeros((STATS - len(pieces), 256), f32)], axis=0)
        high, low = split(both * inverse_rms(ss_ref, row + k, full_width))
        grads = grads + stacked_nt(jnp.concatenate([high, low], axis=0), pair, 2 * channels)
    grad_out[...] = grads


def branch_kernel(first, line_length, len_ref, ser_own, ser_rec, cot_own, cot_rec, *refs):
    sums, refs = refs[: 2 * ser_own.shape[0]], refs[2 * ser_own.shape[0] :]
    up_both, leg_high, leg_low, *refs = refs
    before, (own_out, rec_out, grad_out) = opening(refs, 3)
    channels = ser_own.shape[1]
    rows = 2 * channels
    windows = len_ref.shape[0]
    row = side_of() * (windows // 2) + first
    grads, stats = 0.0, [0.0, 0.0, 0.0]
    for k, total in enumerate(totals(line_length, sums)):
        pair = split(three(nn, [total], (leg_high[...], leg_low[...]))[0])
        branch = masked(stacked(up_both[...], pair, rows), len_ref[row + k])
        own_out[k] = branch[:channels]
        rec_out[k] = branch[channels:]
        high, low = split(jnp.concatenate([cot_own[k], cot_rec[k]], axis=0))
        grads = grads + stacked_nt(jnp.concatenate([high, low], axis=0), pair, rows)
        series = jnp.concatenate([ser_own[k], ser_rec[k]], axis=0)
        for i, v in enumerate((series, branch, series + branch)):
            stats[i] = stats[i] + jnp.sum(v * v, axis=0, keepdims=True)
    width = grads.shape[1]
    stats = [jnp.broadcast_to(jnp.sum(v, axis=1, keepdims=True), (1, width)) for v in stats]
    steps = functools.reduce(lambda a, b: a + b, [len_ref[w] for w in range(windows)]) if first == 0 else 0
    stats.append(jnp.full((1, width), steps, jnp.int32).astype(f32))
    stats = jnp.concatenate(stats + [jnp.zeros((STATS - 4, width), f32)], axis=0)
    grad_out[...] = before + jnp.concatenate([grads, stats], axis=0)


def layer_kernel(units, x_ref, *refs):
    own_refs, rec_refs, out_ref = refs[: len(units)], refs[len(units) : 2 * len(units)], refs[-1]
    windows = x_ref.shape[1] // LEN
    half = windows // 2
    first_side = side_of() == 0
    for w in range(windows):
        u, j = locate(units, w % half)
        value = jnp.where(first_side == (w < half), own_refs[u][j], rec_refs[u][j])
        at = slice(w * LEN, (w + 1) * LEN)
        out_ref[:, at] = x_ref[:, at] + value[:, :LEN]


def inner_row(small_ref, j):
    row = STATS * j
    return jnp.concatenate([small_ref[row + p : row + p + 1, :] for p in range(LANES // 256)], axis=1)


def series_grad_kernel(units, full_width, cot_ref, x_ref, ss_ref, in_own, in_rec, *refs):
    own_refs, rec_refs, out_ref = refs[: len(units)], refs[len(units) : 2 * len(units)], refs[-1]
    windows = x_ref.shape[1] // LEN
    half = windows // 2
    first_side = side_of() == 0
    for w in range(windows):
        u, j = locate(units, w % half)
        keep = first_side == (w < half)
        scaled = jnp.where(keep, own_refs[u][j], rec_refs[u][j])[:, :LEN]
        inner = jnp.where(keep, inner_row(in_own, w % half), inner_row(in_rec, w % half))[:, :LEN]
        inv = inverse_rms(ss_ref, w, full_width)[:, :LEN]
        at = slice(w * LEN, (w + 1) * LEN)
        shift = inv * inv * inner * (1.0 / full_width)
        out_ref[:, at] = cot_ref[:, at] + inv * (scaled - x_ref[:, at] * shift)


def close_kernel(sums_ref, in_ref, gain_ref, grad_in_ref, grad_out_ref, grad_gain_ref):
    modes, ranks, channels = in_ref.shape[1:]
    into, mix = sums_ref[:channels].T, sums_ref[channels : 2 * channels].T
    total = jnp.zeros((modes, channels), f32)
    read_real, read_imag = readout_columns(modes, channels)
    for r in range(ranks):
        pieces = []
        for part in range(2):
            at = slice((part * ranks + r) * modes, (part * ranks + r + 1) * modes)
            grad = into[at]
            total = total + grad * in_ref[part, :, r, :]
            grad_in_ref[part, :, r, :] = grad * gain_ref[...]
            pieces.append(mix[at])
        grad_out_ref[0, :, r, :] = read_real * pieces[0] + read_imag * pieces[1]
        grad_out_ref[1, :, r, :] = read_imag * pieces[0] - read_real * pieces[1]
    grad_gain_ref[...] = jnp.sum(total, axis=0, keepdims=True)


def rms_kernel(share, own_ref, rec_ref, rms_ref):
    stats = own_ref[...] + rec_ref[...]
    rms = jnp.sqrt(stats * share / stats[3:4])
    for k in range(3):
        rms_ref[k] = rms[k, 0]


def whole(shape):
    return pl.BlockSpec(shape, lambda *_: (0,) * len(shape))


SMEM = pl.BlockSpec(memory_space=pltpu.SMEM)
PARAMS = pltpu.CompilerParams(vmem_limit_bytes=8 * 1024 * 1024)


def cost(flops, byte_count, weight=1):
    return pl.CostEstimate(flops=int(flops * weight), bytes_accessed=int(byte_count * weight), transcendentals=0)


def struct(shape, dtype=f32):
    return jax.ShapeDtypeStruct(shape, dtype)


def one_call(kernel, outs, args, smem=0, scalars_out=0, weight=1):
    single = not isinstance(outs, list)
    shapes = [outs] if single else outs
    specs = [SMEM] * smem + [whole(a.shape) for a in args[smem:]]
    moved = sum(a.size * a.dtype.itemsize for a in args) + sum(math.prod(o.shape) * 4 for o in shapes)
    result = pl.pallas_call(
        kernel,
        out_shape=shapes,
        in_specs=specs,
        out_specs=[whole(o.shape) for o in shapes[: len(shapes) - scalars_out]] + [SMEM] * scalars_out,
        grid=(1,),
        compiler_params=PARAMS,
        cost_estimate=cost(moved, moved, weight),
    )(*args)
    return result[0] if single else result


HBM = pl.BlockSpec(memory_space=pltpu.MemorySpace.HBM)


def in_hbm(arrays):
    return [pltpu.with_memory_space_constraint(a, pltpu.MemorySpace.HBM) for a in arrays]


def deal_scratch(array, lengths):
    windows = array.shape[1] // LEN
    return [pltpu.SMEM(lengths.shape, jnp.int32)], [
        pltpu.VMEM(array.shape, f32),
        pltpu.SemaphoreType.DMA((1 + len(chunk_ends(windows)),)),
    ]


def front(series, lengths, weights, units, rows, line_length):
    channels, windows = series.shape[0], series.shape[1] // LEN
    shapes = [struct((windows + PACK, LANES)), struct((8, ORDER)), struct((windows // 2, channels, LANES))]
    shapes += [struct((n, channels, LANES)) for _, n in units]
    first, (buffer, sems) = deal_scratch(series, lengths)
    scratch = first + [pltpu.VMEM(a.shape, f32) for a in weights] + [buffer, pltpu.VMEM((rows, 128), f32), sems]
    return pl.pallas_call(
        functools.partial(front_kernel, units, line_length),
        out_shape=shapes,
        in_specs=[HBM] * (2 + len(weights)),
        out_specs=[whole(o.shape) for o in shapes],
        grid=(1,),
        scratch_shapes=scratch + [pltpu.SemaphoreType.DMA((len(weights),))],
        compiler_params=PARAMS,
        cost_estimate=cost(series.size * 4, series.size * 8),
    )(*in_hbm([lengths, *weights, series]))


def deal(array, lengths, units):
    channels, windows = array.shape[0], array.shape[1] // LEN
    shapes = [struct((windows // 2, channels, LANES))] + [struct((n, channels, LANES)) for _, n in units]
    first, rest = deal_scratch(array, lengths)
    return pl.pallas_call(
        functools.partial(cot_kernel, units),
        out_shape=shapes,
        in_specs=[HBM] * 2,
        out_specs=[whole(o.shape) for o in shapes],
        grid=(1,),
        scratch_shapes=first + rest,
        compiler_params=PARAMS,
        cost_estimate=cost(array.size * 4, array.size * 8),
    )(*in_hbm([lengths, array]))


def prepare_weights(own, rec, windows, rows, channels):
    shapes = [struct((rows, 3 * channels), bf16)] * 4 + [struct((4 * channels, rows), bf16)] * 2
    return one_call(functools.partial(weights_kernel, windows), shapes, [own, rec])


MATMUL = 2 * 256 * 256 * 256


def unit_call(kernel, unit, smem, arrays, consts, outs, units_of_work, weight=1):
    count = unit[1]
    specs = [SMEM] * len(smem)
    assert all(o % count == 0 for _, o in arrays)
    specs += [pl.BlockSpec((count,) + a.shape[1:], lambda i, o=o // count, r=a.ndim - 1: (o,) + (0,) * r) for a, o in arrays]
    specs += [whole(c.shape) for c in consts]
    moved = sum(a.size * 4 * count // a.shape[0] for a, _ in arrays) + sum(c.size * c.dtype.itemsize for c in consts)
    return pl.pallas_call(
        kernel,
        out_shape=[struct(shape) for shape in outs],
        in_specs=specs,
        out_specs=[whole(shape) for shape in outs],
        grid=(1,),
        compiler_params=PARAMS,
        cost_estimate=cost(units_of_work * MATMUL * count, moved, weight),
    )(*smem, *[a for a, _ in arrays], *consts)


def swap(x, axis, bit):
    size = lax.axis_size(axis)
    return lax.ppermute(x, axis, [(i, i ^ bit) for i in range(size)])


def add_over(x, axis, bits):
    for bit in bits:
        x = x + swap(x, axis, bit)
    return x


def bits_of(size, start=1):
    bits, bit = [], start
    while bit < size:
        bits.append(bit)
        bit *= 2
    return bits


def cross(x):
    batch, order = lax.axis_size("batch"), lax.axis_size("order")
    pairs = []
    for b in range(batch):
        for o in range(order):
            inner = o // 2 in (1, 2)
            pairs.append((b * order + o, b * order + (o ^ 6) if inner else (b ^ 1) * order + o))
    return lax.ppermute(x, ("batch", "order"), pairs)


def line_sum(x):
    size = lax.axis_size("order")
    return lax.psum(x, "order", axis_index_groups=[list(range(side, size, 2)) for side in (0, 1)])


def after(x, tokens):
    tokens = tokens if isinstance(tokens, tuple) else (tokens,)
    return lax.optimization_barrier((x, *tokens))[0]


WEIGHT = ((10,10,10,10),(10,10),(10,10),(10,10,10))
COT = (1, 1, 1, 1)
SER = (2, 2)
READ = (1, 1, 1, 1)
RANK = (2, 2)
BACK = (2, 2)
MIX = (2, 1, 1)
LAG = 3
EARLY = 2
PLAN = (
    "R0", "e0", "c2", "R1", "q", "e1", "c3", "x0", "m0", "R2", "e2", "Q", "m1", "R3", "x1", "e3",
    "m2", "K0", "e4", "m3", "e5", "K1", "m4", "e6", "m5", "B0", "g0", "e7", "m6", "B1", "e8", "m7",
    "i1", "g1", "e9", "s0", "M0", "y0", "e10", "i2", "s1", "M1", "ix", "y1", "M2", "G", "y2", "iy",
    "b0", "gc", "b1", "gy", "F2", "ge", "st1", "b2", "CL", "st2", "F1",
)


def units_of(half, counts):
    counts = counts if sum(counts) == half else (1,) * half
    return [(sum(counts[:u]), counts[u]) for u in range(len(counts))]


def local(series, norm_gain, mode_in, mode_out, lengths, grad_out):
    channels = series.shape[0]
    windows = series.shape[1] // LEN
    half = windows // 2
    order_devices = lax.axis_size("order")
    line_length = order_devices // 2
    mode_count, rank_count = mode_in.shape[1], mode_in.shape[2]
    full_width = channels * order_devices
    rows = 2 * rank_count * mode_count
    cot_units, ser_units = units_of(half, COT), units_of(half, SER)
    read_units, rank_units = units_of(half, READ), units_of(half, RANK)
    back_units, mix_units = units_of(half, BACK), units_of(half, MIX)

    legendre = [jnp.asarray(h) for h in halves(legendre_rows())]
    phase = jnp.asarray(phase_rows(mode_count))
    gain = norm_gain.reshape(1, channels)

    message, end_mask, ser_own, *ser_rec = front(series, lengths, [mode_in, mode_out, gain], ser_units, rows, line_length)
    with jax.named_scope("message_x"):
        message_rec = swap(message, "order", 1)
    cot_own, *cot_rec = deal(after(grad_out, message), lengths, cot_units)
    message_rec = after(message_rec, cot_own)
    with jax.named_scope("cot_x"):
        for u in range(EARLY):
            cot_rec[u] = swap(cot_rec[u] if u == 0 else after(cot_rec[u], message_rec), "order", 1)
    down_own, down_rec, up_own, up_rec, down_both, up_both = prepare_weights(message, message_rec, windows, rows, channels)
    with jax.named_scope("squares_z1"):
        squares = message[:windows] + message_rec[:windows]
        squares_rec = swap(squares, "order", 2)
    def windows_of(own, received, units, first, count):
        u, offset = locate(units, first)
        v, _ = locate(units, first + count - 1)
        if u < v:
            return [(own, first), (jnp.concatenate(received[u : v + 1], axis=0), offset)]
        return [(own, first), (received[u], offset)]

    chained = order_devices == 8
    at_end = end_mask[:1] > 0.5
    parts, pairs, sends, came, crossed = {}, {}, {}, {}, {}
    backs, branches, kept = {}, {}, {}
    state = {"squares": squares, "squares_rec": squares_rec, "token": up_own}

    def do_read(u, token):
        first, count = read_units[u]
        own, rec = windows_of(cot_own, cot_rec, cot_units, first, count)
        outs = unit_call(
            read_kernel, read_units[u], [], [own, (after(rec[0], token), rec[1])],
            [up_own, up_rec, *legendre], [(rows, ORDER)] * count, 15, weight=WEIGHT[0][u],
        )
        for k in range(count):
            parts[first + k] = outs[k]
        return outs[0]

    def do_rank(u, token):
        first, count = rank_units[u]
        own, rec = windows_of(ser_own, ser_rec, ser_units, first, count)
        outs = unit_call(
            functools.partial(rank_kernel, first, full_width), rank_units[u], [], [own, (after(rec[0], token), rec[1])],
            [state["squares"], down_own, down_rec, *legendre, phase], [(rows, ORDER)] * count, 21, weight=WEIGHT[1][u],
        )
        for k in range(count):
            parts[half + first + k] = outs[k]
        return outs[0]

    def do_swap(k, token):
        if not chained:
            if k < windows:
                came[k + LAG] = sends[k + LAG] = line_sum(after(parts[k], token))
            return token
        done = k - LAG
        if done < 0:
            out = after(parts[k], token)
        else:
            out = pairs[done] + after(crossed[done], token)
            if k < windows:
                out = jnp.where(at_end, parts[k], out)
        with jax.named_scope(f"e{k}"):
            sends[k], came[k] = out, swap(out, "order", 2)
        return out

    def do_cross(k, token):
        if not chained:
            return token
        out = pairs[k] = parts[k] + after(came[k], token)
        with jax.named_scope(f"m{k}"):
            crossed[k] = cross(out)
        return out

    def sums_of(first, count, token):
        at = range(first + LAG, first + LAG + count)
        return [sends[k] for k in at] + [after(came[k], token) for k in at]

    def do_back(u, token):
        first, count = back_units[u]
        previous = [state["grad_in"]] if "grad_in" in state else []
        mine, theirs, state["grad_in"], dots = unit_call(
            functools.partial(back_kernel, first, full_width, line_length), back_units[u], [lengths],
            windows_of(ser_own, ser_rec, ser_units, first, count),
            [*sums_of(first, count, token), state["squares"], down_both, *legendre, phase, *previous],
            [(count, channels, LANES)] * 2 + [(2 * channels, rows), (count, STATS, 256)], 24, weight=WEIGHT[2][u],
        )
        backs[u] = (mine, theirs, dots)
        return state["grad_in"]

    def do_mix(u, token):
        first, count = mix_units[u]
        previous = [state["grad_mix"]] if "grad_mix" in state else []
        mine, theirs, state["grad_mix"] = unit_call(
            functools.partial(branch_kernel, first, line_length), mix_units[u], [lengths],
            [*windows_of(ser_own, ser_rec, ser_units, first, count), *windows_of(cot_own, cot_rec, cot_units, first, count)],
            [*sums_of(half + first, count, token), up_both, *legendre, *previous],
            [(count, channels, LANES)] * 2 + [(2 * channels + STATS, rows)], 18, weight=WEIGHT[3][u],
        )
        branches[u], kept[u] = mine, theirs
        return state["grad_mix"]

    def do_grads(token):
        grad_in, grad_mix = state["grad_in"], state["grad_mix"]
        stats = grad_mix[2 * channels :]
        state["own"] = jnp.concatenate([grad_in[:channels], grad_mix[:channels], stats], axis=0)
        rec = jnp.concatenate([grad_in[channels:], grad_mix[channels : 2 * channels], stats], axis=0)
        with jax.named_scope("grads_x"):
            state["rec"] = swap(after(rec, token), "order", 1)
        return rec

    def do_series(token):
        count = len(back_units)
        return one_call(
            functools.partial(series_grad_kernel, back_units, full_width), struct(series.shape),
            [grad_out, series, state["squares"], state["inner"], after(state["inner_rec"], token)]
            + [backs[u][0] for u in range(count)] + [backs[u][1] for u in range(count)], weight=0.01,
        )

    def do_layer(token):
        count = len(mix_units)
        return one_call(
            functools.partial(layer_kernel, mix_units), struct(series.shape),
            [after(series, token)] + [branches[u] for u in range(count)] + [kept[u] for u in range(count)],
        )

    for step in PLAN:
        name, token = step.rstrip("0123456789"), state["token"]
        u = int(step[len(name) :] or 0)
        if name == "q":
            with jax.named_scope("squares_z2"):
                out = state["squares"] + after(state["squares_rec"], token)
                state["squares"] = add_over(out, "order", bits_of(order_devices, 4))
        elif name == "g":
            out = token
            with jax.named_scope(f"scaled{u}"):
                backs[u] = (backs[u][0], swap(after(backs[u][1], token), "order", 1), backs[u][2])
        elif name == "y":
            out = token
            with jax.named_scope(f"branch{u}"):
                kept[u] = swap(after(kept[u], token), "order", 1)
        elif name == "s":
            out = after(backs[u][1], token)
            backs[u] = (backs[u][0], out, backs[u][2])
        elif name == "b":
            out = kept[u] = after(kept[u], token)
        elif name == "Q":
            out = state["squares"] = after(state["squares"], token)
        elif name == "R":
            out = do_read(u, token)
        elif name == "K":
            out = do_rank(u, token)
        elif name in ("c", "x"):
            out, sent = token, cot_rec if name == "c" else ser_rec
            if u < len(sent):
                with jax.named_scope("cot_x" if name == "c" else "ser_x"):
                    sent[u] = swap(after(sent[u], token), "order", 1)
        elif name == "e":
            out = do_swap(u, token)
        elif name == "m":
            out = do_cross(u, token)
        elif name == "B":
            out = do_back(u, token)
        elif name == "M":
            out = do_mix(u, token)
        elif name == "i":
            with jax.named_scope(f"inner_z{u}"):
                if u == 1:
                    out = [after(backs[k][2], token).reshape(-1, 256) for k in range(len(back_units))]
                    out = jnp.concatenate(out, axis=0)
                else:
                    out = state["inner"] + after(state["inner_rec"], token)
                state["inner"], state["inner_rec"] = out, swap(out, "order", 1 << u)
        elif name == "ix":
            with jax.named_scope("inner_x"):
                out = state["inner"] + after(state["inner_rec"], token)
                out = add_over(out, "order", bits_of(order_devices, 8))
                state["inner"], state["inner_rec"] = out, swap(out, "order", 1)
        elif name == "iy":
            out = state["inner_rec"] = after(state["inner_rec"], token)
        elif name == "st":
            with jax.named_scope(f"stats_z{u}"):
                if u == 1:
                    out = state["own"][2 * channels :]
                else:
                    out = state["stats"] + after(state["stats_rec"], token)
                    out = add_over(out, "order", bits_of(order_devices // 2, 4))
                step_bit = 2 if u == 1 else order_devices // 2
                state["stats"], state["stats_rec"] = out, swap(out, "order", step_bit)
        elif name == "CL":
            state["close"] = one_call(
                close_kernel, [struct(mode_in.shape), struct(mode_out.shape), struct((1, channels))],
                [after(state["own"], token), mode_in, gain],
            )
            out = state["close"][0]
        elif name == "G":
            out = do_grads(token)
        elif name == "gc":
            with jax.named_scope("grads_core"):
                out = state["own"] + after(state["rec"], token)
                state["own"], state["rec"] = out, swap(out, "batch", 1)
        elif name == "gy":
            with jax.named_scope("grads_y"):
                out = state["own"] + after(state["rec"], token)
                out = add_over(out, "batch", bits_of(lax.axis_size("batch") // 2, 2))
                state["own"], state["rec"] = out, swap(out, "batch", lax.axis_size("batch") // 2)
        elif name == "ge":
            state["own"] = out = state["own"] + after(state["rec"], token)
        elif name == "F":
            out = state[step] = do_layer(token) if u == 1 else do_series(token)
        state["token"] = out
    stream_rms = one_call(
        functools.partial(rms_kernel, order_devices / full_width), [struct((3,))],
        [state["stats"], after(state["stats_rec"], state["token"])], scalars_out=1,
    )[0]
    grad_mode_in, grad_mode_out, grad_gain = state["close"]
    return state["F1"], state["F2"], grad_gain.reshape(channels), grad_mode_in, grad_mode_out, stream_rms


def solution(mesh):
    wide = P("order", "batch")
    weight = P(None, None, None, "order")
    in_specs = (wide, P("order"), weight, weight, P("batch"), wide)
    out_specs = (wide, wide, P("order"), weight, weight, P())
    return jax.shard_map(local, mesh=mesh, in_specs=in_specs, out_specs=out_specs, check_vma=False)
```

```python
import functools
import math

import jax
import jax.numpy as jnp
import numpy as np
from jax import lax
from jax.experimental import pallas as pl
from jax.experimental.pallas import tpu as pltpu
from jax.sharding import PartitionSpec as P

ORDER = 256
LEN = 720
LANES = 768
BLOCK = 256
epsilon = 1e-06
f32 = jnp.float32
bf16 = jnp.bfloat16


def legendre_rows():
    coords = 1.0 - (2.0 * np.arange(LEN) + 1.0) / LEN
    rows = [np.ones(LEN), coords]
    for k in range(1, ORDER - 1):
        rows.append(((2.0 * k + 1.0) * coords * rows[k] - k * rows[k - 1]) / (k + 1.0))
    table = np.stack(rows) * np.sqrt((2.0 * np.arange(ORDER) + 1.0) / LEN)[:, None]
    out = np.zeros((ORDER, LANES))
    out[:, :LEN] = table[:, ::-1]
    return out


def phase_rows(mode_count):
    modes = np.arange(mode_count)[:, None]
    steps = np.arange(LANES)[None, :]
    now = 2.0 * np.pi * ((modes * steps) % LEN) / LEN
    nxt = 2.0 * np.pi * ((modes * (steps + 1)) % LEN) / LEN
    root = 1.0 / math.sqrt(LEN)
    rows = np.stack([np.cos(now), np.sin(now), np.cos(nxt) * root, np.sin(nxt) * root])
    return rows.astype(np.float32)


def halves(table):
    high = table.astype(np.float32).astype(jnp.bfloat16)
    low = (table - high.astype(np.float64)).astype(np.float32).astype(jnp.bfloat16)
    return high, low


def split(x):
    high = x.astype(bf16)
    return high, (x - high.astype(f32)).astype(bf16)


def nn(a, b):
    return lax.dot_general(a, b, (((1,), (0,)), ((), ())), preferred_element_type=f32)


def nt(a, b):
    return lax.dot_general(a, b, (((1,), (1,)), ((), ())), preferred_element_type=f32)


def three(dot, pairs, table):
    rows = pairs[0][0].shape[0]
    high = dot(jnp.concatenate([half for pair in pairs for half in pair], axis=0), table[0])
    low = dot(jnp.concatenate([pair[0] for pair in pairs], axis=0), table[1])
    out = []
    for k in range(len(pairs)):
        at = 2 * k * rows
        out.append(high[at : at + rows] + high[at + rows : at + 2 * rows] + low[k * rows : (k + 1) * rows])
    return out


def deep(x):
    high, low = split(x)
    return jnp.concatenate([high, low, high], axis=0)


def stacked(weights, pair, rows):
    first = nn(weights, pair[0])
    return first[:rows] + first[rows:] + nn(weights[:rows], pair[1])


def stacked_nt(left, pair, rows):
    first = nt(left, pair[0])
    return first[:rows] + first[rows:] + nt(left[:rows], pair[1])


def rotate(real, imag, cos, sin):
    modes = cos.shape[0]
    shape = (real.shape[0] // modes, modes, real.shape[1])
    real, imag = real.reshape(shape), imag.reshape(shape)
    cos, sin = cos[None], sin[None]
    flat = (shape[0] * modes, shape[2])
    return (real * cos + imag * sin).reshape(flat), (imag * cos - real * sin).reshape(flat)


def triangle():
    row = lax.broadcasted_iota(jnp.int32, (BLOCK, BLOCK), 0)
    col = lax.broadcasted_iota(jnp.int32, (BLOCK, BLOCK), 1)
    return jnp.where(row <= col, 1.0, 0.0).astype(bf16)


def block_sums(dot, x):
    rows, blocks = x.shape[0], LANES // BLOCK
    halves_of = split(x)
    stack = [half[:, b * BLOCK : (b + 1) * BLOCK] for half in halves_of for b in range(blocks)]
    sums = dot(jnp.concatenate(stack, axis=0), triangle())
    return [sums[b * rows : (b + 1) * rows] + sums[(blocks + b) * rows : (blocks + b + 1) * rows] for b in range(blocks)]


def running_sum(x):
    blocks = block_sums(nn, x)
    for b in range(1, len(blocks)):
        blocks[b] = blocks[b] + blocks[b - 1][:, BLOCK - 1 : BLOCK]
    return jnp.concatenate(blocks, axis=1)


def running_sum_back(x):
    blocks = block_sums(nt, x)
    for b in reversed(range(len(blocks) - 1)):
        blocks[b] = blocks[b] + blocks[b + 1][:, 0:1]
    return jnp.concatenate(blocks, axis=1)


def side_of():
    return lax.rem(lax.axis_index("order"), 2)


def at_line_end(line_length):
    line = lax.div(lax.axis_index("order"), 2)
    return jnp.logical_or(line == 0, line == line_length - 1)


def locate(units, j):
    u = max(k for k in range(len(units)) if units[k][0] <= j)
    return u, j - units[u][0]


def chunk_ends(windows):
    return [-(-LEN * min(w + 2, windows) // 128) * 128 for w in range(0, windows, 2)]


def deal_windows(split_at, len_hbm, hbm_ref, len_ref, buffer, sems, out_refs, use):
    lengths_copy = pltpu.make_async_copy(len_hbm, len_ref, sems.at[0])
    lengths_copy.start()
    own_ref, send_refs = out_refs[0], out_refs[1:]
    channels = hbm_ref.shape[0]
    windows = hbm_ref.shape[1] // LEN
    half = windows // 2
    ends = chunk_ends(windows)
    copies = []
    for c, end in enumerate(ends):
        at = slice(ends[c - 1] if c else 0, end)
        copies.append(pltpu.make_async_copy(hbm_ref.at[:, at], buffer.at[:, at], sems.at[1 + c]))
        copies[-1].start()
    lane = lax.broadcasted_iota(jnp.int32, (channels, LEN), 1)
    side = side_of()
    for ref in out_refs:
        ref[:, :, LANES - 128 :] = jnp.zeros((ref.shape[0], channels, 128), f32)
    lengths_copy.wait()
    for w in range(windows):
        if w % 2 == 0:
            copies[w // 2].wait()
        value = buffer[:, w * LEN : (w + 1) * LEN]
        value = jnp.where(lane < len_ref[w], value, 0.0)
        use(w, value)
        unit, at = locate(split_at, w % half)
        send_ref = send_refs[unit]
        mine = side == (0 if w < half else 1)

        @pl.when(mine)
        def _():
            own_ref[w % half, :, :LEN] = value

        @pl.when(jnp.logical_not(mine))
        def _():
            send_ref[at, :, :LEN] = value


PACK = 48
STATS = 8


def readout_columns(modes, channels):
    mode = lax.broadcasted_iota(jnp.int32, (modes, channels), 0)
    angle = mode.astype(f32) * (2.0 * math.pi / LEN)
    factor = jnp.where(mode == 0, 1.0, 2.0) * (1.0 / math.sqrt(LEN))
    return factor * jnp.cos(angle), factor * jnp.sin(angle)


def front_kernel(units, line_length, len_hbm, in_hbm, out_hbm, gain_hbm, x_hbm, message_ref, end_ref, *refs):
    out_refs, (len_ref, in_ref, out_ref, gain_ref, buffer, packed, sems, weight_sems) = refs[:-8], refs[-8:]
    windows = x_hbm.shape[1] // LEN
    end_ref[...] = jnp.where(at_line_end(line_length), jnp.ones(end_ref.shape, f32), 0.0)
    weights = [(in_hbm, in_ref), (out_hbm, out_ref), (gain_hbm, gain_ref)]
    weights = [pltpu.make_async_copy(a, b, weight_sems.at[k]) for k, (a, b) in enumerate(weights)]
    for copy in weights:
        copy.start()
    message_ref[...] = jnp.zeros(message_ref.shape, f32)

    def use(w, value):
        message_ref[w : w + 1, :LEN] = jnp.sum(value * value, axis=0, keepdims=True)

    deal_windows(units, len_hbm, x_hbm, len_ref, buffer, sems, out_refs, use)
    for copy in weights:
        copy.wait()
    modes, ranks, channels = in_ref.shape[1:]
    packed[...] = jnp.zeros(packed.shape, f32)
    read_real, read_imag = readout_columns(modes, channels)
    for r in range(ranks):
        real, imag = out_ref[0, :, r, :], out_ref[1, :, r, :]
        second = (read_real * real + read_imag * imag, read_imag * real - read_real * imag)
        for part in range(2):
            at = slice((part * ranks + r) * modes, (part * ranks + r + 1) * modes)
            packed[at, :channels] = in_ref[part, :, r, :] * gain_ref[...]
            packed[at, channels : 2 * channels] = second[part]
    rows = packed.shape[0]
    for k in range(-(-rows // PACK)):
        count = min(PACK, rows - k * PACK)
        message_ref[windows : windows + count, k * 128 : (k + 1) * 128] = packed[k * PACK : k * PACK + count]


def unpack(message_ref, windows, rows):
    pieces = []
    for k in range(-(-rows // PACK)):
        count = min(PACK, rows - k * PACK)
        pieces.append(message_ref[windows : windows + count, k * 128 : (k + 1) * 128])
    return jnp.concatenate(pieces, axis=0)


def cot_kernel(units, len_hbm, x_hbm, *refs):
    deal_windows(units, len_hbm, x_hbm, *refs[-3:], refs[:-3], lambda w, value: None)


def weights_kernel(windows, own_ref, rec_ref, down_own, down_rec, up_own, up_rec, down_both, up_both):
    rows, channels = down_own.shape[0], down_own.shape[1] // 3
    pieces = []
    for ref, down, up in ((own_ref, down_own, up_own), (rec_ref, down_rec, up_rec)):
        packed = unpack(ref, windows, rows)
        high, low = split(packed)
        down[...] = jnp.concatenate([high[:, :channels], high[:, :channels], low[:, :channels]], axis=1)
        upper = slice(channels, 2 * channels)
        up[...] = jnp.concatenate([high[:, upper], high[:, upper], low[:, upper]], axis=1)
        pieces.append(packed.T)
    for k, ref in ((0, down_both), (1, up_both)):
        at = slice(k * channels, (k + 1) * channels)
        both = jnp.concatenate([pieces[0][at], pieces[1][at]], axis=0)
        high, low = split(both)
        ref[...] = jnp.concatenate([high, low], axis=0)


def read_kernel(own_ref, rec_ref, up_own, up_rec, leg_high, leg_low, *out_refs):
    pairs = []
    for k in range(len(out_refs)):
        pairs.append(split(nn(up_own[...], deep(own_ref[k])) + nn(up_rec[...], deep(rec_ref[k]))))
    for ref, value in zip(out_refs, three(nt, pairs, (leg_high[...], leg_low[...]))):
        ref[...] = value


def inverse_rms(ss_ref, row, full_width):
    return lax.rsqrt(ss_ref[pl.ds(row, 1), :] * (1.0 / full_width) + epsilon)


def rank_kernel(first, full_width, own_ref, rec_ref, ss_ref, down_own, down_rec, leg_high, leg_low, phase_ref, *out_refs):
    row = side_of() * (ss_ref.shape[0] // 2) + first
    pairs = []
    for k in range(len(out_refs)):
        inv = inverse_rms(ss_ref, row + k, full_width)
        mixed = nn(down_own[...], deep(own_ref[k] * inv)) + nn(down_rec[...], deep(rec_ref[k] * inv))
        part = mixed.shape[0] // 2
        real, imag = rotate(mixed[:part], mixed[part:], phase_ref[0], phase_ref[1])
        total = running_sum(jnp.concatenate([real, imag], axis=0))
        real, imag = rotate(total[:part], total[part:], phase_ref[2], -phase_ref[3])
        pairs.append(split(jnp.concatenate([real, imag], axis=0)))
    for ref, value in zip(out_refs, three(nt, pairs, (leg_high[...], leg_low[...]))):
        ref[...] = value


def totals(line_length, refs):
    count, at_end = len(refs) // 2, at_line_end(line_length)
    return [split(jnp.where(at_end, refs[count + k][...], refs[k][...])) for k in range(count)]


def masked(value, length):
    lane = lax.broadcasted_iota(jnp.int32, value.shape, 1)
    return jnp.where(lane < length, value, 0.0)


def opening(refs, outs, sums):
    return [ref[...] for ref in refs[:-outs]] or [0.0] * sums, refs[-outs:]


def back_kernel(first, full_width, line_length, len_ref, own_ref, rec_ref, *refs):
    sums, refs = refs[: 2 * own_ref.shape[0]], refs[2 * own_ref.shape[0] :]
    ss_ref, down_both, leg_high, leg_low, phase_ref, *refs = refs
    before, (own_out, rec_out, grad_own, grad_rec, inner_out) = opening(refs, 5, 2)
    grads = 0.0
    row = side_of() * (ss_ref.shape[0] // 2) + first
    channels = own_ref.shape[1]
    for k, total in enumerate(totals(line_length, sums)):
        (memory,) = three(nn, [total], (leg_high[...], leg_low[...]))
        part = memory.shape[0] // 2
        real, imag = rotate(memory[:part], memory[part:], phase_ref[2], phase_ref[3])
        back = running_sum_back(jnp.concatenate([real, imag], axis=0))
        real, imag = rotate(back[:part], back[part:], phase_ref[0], -phase_ref[1])
        pair = split(jnp.concatenate([real, imag], axis=0))
        scaled = masked(stacked(down_both[...], pair, 2 * channels), len_ref[row + k])
        own_out[k] = scaled[:channels]
        rec_out[k] = scaled[channels:]
        both = jnp.concatenate([own_ref[k], rec_ref[k]], axis=0)
        inner = jnp.sum(scaled * both, axis=0, keepdims=True)
        pieces = [inner[:, p * 256 : (p + 1) * 256] for p in range(LANES // 256)]
        inner_out[k] = jnp.concatenate(pieces + [jnp.zeros((STATS - len(pieces), 256), f32)], axis=0)
        high, low = split(both * inverse_rms(ss_ref, row + k, full_width))
        grads = grads + stacked_nt(jnp.concatenate([high, low], axis=0), pair, 2 * channels)
    grad_own[...] = before[0] + grads[:channels]
    grad_rec[...] = before[1] + grads[channels:]


def branch_kernel(first, line_length, len_ref, ser_own, ser_rec, cot_own, cot_rec, *refs):
    sums, refs = refs[: 2 * ser_own.shape[0]], refs[2 * ser_own.shape[0] :]
    up_both, leg_high, leg_low, *refs = refs
    before, (own_out, rec_out, grad_own, grad_rec, stats_out) = opening(refs, 5, 3)
    channels = ser_own.shape[1]
    rows = 2 * channels
    windows = len_ref.shape[0]
    row = side_of() * (windows // 2) + first
    grads, stats = 0.0, [0.0, 0.0, 0.0]
    for k, total in enumerate(totals(line_length, sums)):
        pair = split(three(nn, [total], (leg_high[...], leg_low[...]))[0])
        branch = masked(stacked(up_both[...], pair, rows), len_ref[row + k])
        own_out[k] = branch[:channels]
        rec_out[k] = branch[channels:]
        high, low = split(jnp.concatenate([cot_own[k], cot_rec[k]], axis=0))
        grads = grads + stacked_nt(jnp.concatenate([high, low], axis=0), pair, rows)
        series = jnp.concatenate([ser_own[k], ser_rec[k]], axis=0)
        for i, v in enumerate((series, branch, series + branch)):
            stats[i] = stats[i] + jnp.sum(v * v, axis=0, keepdims=True)
    width = grads.shape[1]
    stats = [jnp.broadcast_to(jnp.sum(v, axis=1, keepdims=True), (1, width)) for v in stats]
    steps = functools.reduce(lambda a, b: a + b, [len_ref[w] for w in range(windows)]) if first == 0 else 0
    stats.append(jnp.full((1, width), steps, jnp.int32).astype(f32))
    stats = jnp.concatenate(stats + [jnp.zeros((STATS - 4, width), f32)], axis=0)
    grad_own[...] = before[0] + grads[:channels]
    grad_rec[...] = before[1] + grads[channels:]
    stats_out[...] = before[2] + stats


def own_or_theirs(units, own_refs, rec_refs, w, half):
    u, j = locate(units, w % half)
    return jnp.where((side_of() == 0) == (w < half), own_refs[u][j], rec_refs[u][j])


def layer_kernel(units, x_ref, *refs):
    own_refs, rec_refs, out_ref = refs[: len(units)], refs[len(units) : 2 * len(units)], refs[-1]
    windows = x_ref.shape[1] // LEN
    branches = [own_or_theirs(units, own_refs, rec_refs, w, windows // 2)[:, :LEN] for w in range(windows)]
    out_ref[...] = x_ref[...] + jnp.concatenate(branches, axis=1)


def inner_row(small_ref, j):
    row = STATS * j
    return jnp.concatenate([small_ref[row + p : row + p + 1, :] for p in range(LANES // 256)], axis=1)


def series_grad_kernel(units, full_width, cot_ref, x_own, ss_ref, in_own, in_rec, *refs):
    count = len(units)
    own_refs, rec_refs, sent_refs, out_ref = refs[:count], refs[count : 2 * count], refs[2 * count : -1], refs[-1]
    windows = cot_ref.shape[1] // LEN
    half = windows // 2
    first_side = side_of() == 0
    sent = [(ref, k) for ref in sent_refs for k in range(ref.shape[0])]
    shifts = []
    for w in range(windows):
        keep = first_side == (w < half)
        scaled = own_or_theirs(units, own_refs, rec_refs, w, half)
        ref, k = sent[w % half]
        series = jnp.where(keep, x_own[w % half], ref[k])
        inner = jnp.where(keep, inner_row(in_own, w % half), inner_row(in_rec, w % half))
        inv = inverse_rms(ss_ref, w, full_width)
        shifts.append((inv * (scaled - series * (inv * inv * inner * (1.0 / full_width))))[:, :LEN])
    out_ref[...] = cot_ref[...] + jnp.concatenate(shifts, axis=1)


def close_kernel(into_ref, mix_ref, in_ref, gain_ref, grad_in_ref, grad_out_ref, grad_gain_ref):
    modes, ranks, channels = in_ref.shape[1:]
    into, mix = into_ref[...].T, mix_ref[:channels].T
    total = jnp.zeros((modes, channels), f32)
    read_real, read_imag = readout_columns(modes, channels)
    for r in range(ranks):
        pieces = []
        for part in range(2):
            at = slice((part * ranks + r) * modes, (part * ranks + r + 1) * modes)
            grad = into[at]
            total = total + grad * in_ref[part, :, r, :]
            grad_in_ref[part, :, r, :] = grad * gain_ref[...]
            pieces.append(mix[at])
        grad_out_ref[0, :, r, :] = read_real * pieces[0] + read_imag * pieces[1]
        grad_out_ref[1, :, r, :] = read_imag * pieces[0] - read_real * pieces[1]
    grad_gain_ref[...] = jnp.sum(total, axis=0, keepdims=True)


def rms_kernel(share, own_ref, rec_ref, rms_ref):
    stats = own_ref[...] + rec_ref[...]
    rms = jnp.sqrt(stats * share / stats[3:4])
    for k in range(3):
        rms_ref[k] = rms[k, 0]


def whole(shape):
    return pl.BlockSpec(shape, lambda *_: (0,) * len(shape))


SMEM = pl.BlockSpec(memory_space=pltpu.SMEM)
PARAMS = pltpu.CompilerParams(vmem_limit_bytes=8 * 1024 * 1024)


def cost(flops, byte_count, weight=1):
    return pl.CostEstimate(flops=int(flops * weight), bytes_accessed=int(byte_count * weight), transcendentals=0)


def struct(shape, dtype=f32):
    return jax.ShapeDtypeStruct(shape, dtype)


def one_call(kernel, outs, args, smem=0, scalars_out=0, weight=1):
    single = not isinstance(outs, list)
    shapes = [outs] if single else outs
    specs = [SMEM] * smem + [whole(a.shape) for a in args[smem:]]
    moved = sum(a.size * a.dtype.itemsize for a in args) + sum(math.prod(o.shape) * 4 for o in shapes)
    result = pl.pallas_call(
        kernel,
        out_shape=shapes,
        in_specs=specs,
        out_specs=[whole(o.shape) for o in shapes[: len(shapes) - scalars_out]] + [SMEM] * scalars_out,
        grid=(1,),
        compiler_params=PARAMS,
        cost_estimate=cost(moved, moved, weight),
    )(*args)
    return result[0] if single else result


HBM = pl.BlockSpec(memory_space=pltpu.MemorySpace.HBM)


def in_hbm(arrays):
    return [pltpu.with_memory_space_constraint(a, pltpu.MemorySpace.HBM) for a in arrays]


def deal_scratch(array, lengths):
    windows = array.shape[1] // LEN
    return [pltpu.SMEM(lengths.shape, jnp.int32)], [
        pltpu.VMEM(array.shape, f32),
        pltpu.SemaphoreType.DMA((1 + len(chunk_ends(windows)),)),
    ]


def front(series, lengths, weights, units, rows, line_length):
    channels, windows = series.shape[0], series.shape[1] // LEN
    shapes = [struct((windows + PACK, LANES)), struct((8, ORDER)), struct((windows // 2, channels, LANES))]
    shapes += [struct((n, channels, LANES)) for _, n in units]
    first, (buffer, sems) = deal_scratch(series, lengths)
    scratch = first + [pltpu.VMEM(a.shape, f32) for a in weights] + [buffer, pltpu.VMEM((rows, 128), f32), sems]
    return pl.pallas_call(
        functools.partial(front_kernel, units, line_length),
        out_shape=shapes,
        in_specs=[HBM] * (2 + len(weights)),
        out_specs=[whole(o.shape) for o in shapes],
        grid=(1,),
        scratch_shapes=scratch + [pltpu.SemaphoreType.DMA((len(weights),))],
        compiler_params=PARAMS,
        cost_estimate=cost(series.size * 4, series.size * 8),
    )(*in_hbm([lengths, *weights, series]))


def deal(array, lengths, units):
    channels, windows = array.shape[0], array.shape[1] // LEN
    shapes = [struct((windows // 2, channels, LANES))] + [struct((n, channels, LANES)) for _, n in units]
    first, rest = deal_scratch(array, lengths)
    return pl.pallas_call(
        functools.partial(cot_kernel, units),
        out_shape=shapes,
        in_specs=[HBM] * 2,
        out_specs=[whole(o.shape) for o in shapes],
        grid=(1,),
        scratch_shapes=first + rest,
        compiler_params=PARAMS,
        cost_estimate=cost(array.size * 4, array.size * 8),
    )(*in_hbm([lengths, array]))


def prepare_weights(own, rec, windows, rows, channels):
    shapes = [struct((rows, 3 * channels), bf16)] * 4 + [struct((4 * channels, rows), bf16)] * 2
    return one_call(functools.partial(weights_kernel, windows), shapes, [own, rec])


MATMUL = 2 * 256 * 256 * 256


def unit_call(kernel, unit, smem, arrays, consts, outs, units_of_work, weight=1):
    count = unit[1]
    specs = [SMEM] * len(smem)
    assert all(o % count == 0 for _, o in arrays)
    specs += [pl.BlockSpec((count,) + a.shape[1:], lambda i, o=o // count, r=a.ndim - 1: (o,) + (0,) * r) for a, o in arrays]
    specs += [whole(c.shape) for c in consts]
    moved = sum(a.size * 4 * count // a.shape[0] for a, _ in arrays) + sum(c.size * c.dtype.itemsize for c in consts)
    return pl.pallas_call(
        kernel,
        out_shape=[struct(shape) for shape in outs],
        in_specs=specs,
        out_specs=[whole(shape) for shape in outs],
        grid=(1,),
        compiler_params=PARAMS,
        cost_estimate=cost(units_of_work * MATMUL * count, moved, weight),
    )(*smem, *[a for a, _ in arrays], *consts)


def swap(x, axis, bit):
    size = lax.axis_size(axis)
    return lax.ppermute(x, axis, [(i, i ^ bit) for i in range(size)])


def add_over(x, axis, bits):
    for bit in bits:
        x = x + swap(x, axis, bit)
    return x


def bits_of(size, start=1):
    bits, bit = [], start
    while bit < size:
        bits.append(bit)
        bit *= 2
    return bits


def cross(x):
    batch, order = lax.axis_size("batch"), lax.axis_size("order")
    pairs = []
    for b in range(batch):
        for o in range(order):
            inner = o // 2 in (1, 2)
            pairs.append((b * order + o, b * order + (o ^ 6) if inner else (b ^ 1) * order + o))
    return lax.ppermute(x, ("batch", "order"), pairs)


def line_sum(x):
    size = lax.axis_size("order")
    return lax.psum(x, "order", axis_index_groups=[list(range(side, size, 2)) for side in (0, 1)])


def after(x, tokens):
    tokens = tokens if isinstance(tokens, tuple) else (tokens,)
    return lax.optimization_barrier((x, *tokens))[0]


WEIGHT = ((10,10,10,10),(10,10),(10,10),(10,10,10))
COT = (1, 1, 1, 1)
SER = (2, 2)
READ = (1, 1, 1, 1)
RANK = (2, 2)
BACK = (2, 2)
MIX = (2, 1, 1)
LAG = 3
EARLY = 2
PLAN = (
    "R0", "e0", "c2", "R1", "q", "e1", "c3", "x0", "m0", "R2", "e2", "Q", "m1", "R3", "x1", "e3",
    "m2", "K0", "e4", "m3", "e5", "K1", "m4", "e6", "m5", "B0", "g0", "e7", "m6", "B1", "e8", "m7",
    "r", "e9", "g1", "i1", "rc", "s0", "M0", "y0", "e10", "i2", "M1", "s1", "ry", "ix", "y1", "M2",
    "re", "G", "y2", "iy", "b0", "gc", "gy", "F2", "b1", "ge", "t1", "b2", "CL", "t2", "F1",
)


def units_of(half, counts):
    counts = counts if sum(counts) == half else (1,) * half
    return [(sum(counts[:u]), counts[u]) for u in range(len(counts))]


def local(series, norm_gain, mode_in, mode_out, lengths, grad_out):
    channels = series.shape[0]
    windows = series.shape[1] // LEN
    half = windows // 2
    order_devices = lax.axis_size("order")
    line_length = order_devices // 2
    mode_count, rank_count = mode_in.shape[1], mode_in.shape[2]
    full_width = channels * order_devices
    rows = 2 * rank_count * mode_count
    cot_units, ser_units = units_of(half, COT), units_of(half, SER)
    read_units, rank_units = units_of(half, READ), units_of(half, RANK)
    back_units, mix_units = units_of(half, BACK), units_of(half, MIX)

    legendre = [jnp.asarray(h) for h in halves(legendre_rows())]
    phase = jnp.asarray(phase_rows(mode_count))
    gain = norm_gain.reshape(1, channels)

    message, end_mask, ser_own, *ser_sent = front(series, lengths, [mode_in, mode_out, gain], ser_units, rows, line_length)
    ser_rec = list(ser_sent)
    with jax.named_scope("message_x"):
        message_rec = swap(message, "order", 1)
    cot_own, *cot_rec = deal(after(grad_out, message), lengths, cot_units)
    message_rec = after(message_rec, cot_own)
    with jax.named_scope("cot_x"):
        for u in range(EARLY):
            cot_rec[u] = swap(cot_rec[u] if u == 0 else after(cot_rec[u], message_rec), "order", 1)
    down_own, down_rec, up_own, up_rec, down_both, up_both = prepare_weights(message, message_rec, windows, rows, channels)
    with jax.named_scope("squares_z1"):
        squares = message[:windows] + message_rec[:windows]
        squares_rec = swap(squares, "order", 2)
    def windows_of(own, received, units, first, count):
        u, offset = locate(units, first)
        v, _ = locate(units, first + count - 1)
        if u < v:
            return [(own, first), (jnp.concatenate(received[u : v + 1], axis=0), offset)]
        return [(own, first), (received[u], offset)]

    chained = order_devices == 8
    at_end = end_mask[:1] > 0.5
    parts, pairs, sends, came, crossed = {}, {}, {}, {}, {}
    backs, branches, kept = {}, {}, {}
    state = {"squares": squares, "squares_rec": squares_rec, "token": up_own}

    def do_read(u, token):
        first, count = read_units[u]
        own, rec = windows_of(cot_own, cot_rec, cot_units, first, count)
        outs = unit_call(
            read_kernel, read_units[u], [], [own, (after(rec[0], token), rec[1])],
            [up_own, up_rec, *legendre], [(rows, ORDER)] * count, 15, weight=WEIGHT[0][u],
        )
        for k in range(count):
            parts[first + k] = outs[k]
        return outs[0]

    def do_rank(u, token):
        first, count = rank_units[u]
        own, rec = windows_of(ser_own, ser_rec, ser_units, first, count)
        outs = unit_call(
            functools.partial(rank_kernel, first, full_width), rank_units[u], [], [own, (after(rec[0], token), rec[1])],
            [state["squares"], down_own, down_rec, *legendre, phase], [(rows, ORDER)] * count, 21, weight=WEIGHT[1][u],
        )
        for k in range(count):
            parts[half + first + k] = outs[k]
        return outs[0]

    def do_swap(k, token):
        if not chained:
            if k < windows:
                came[k + LAG] = sends[k + LAG] = line_sum(after(parts[k], token))
            return token
        done = k - LAG
        if done < 0:
            out = after(parts[k], token)
        else:
            out = pairs[done] + after(crossed[done], token)
            if k < windows:
                out = jnp.where(at_end, parts[k], out)
        with jax.named_scope(f"e{k}"):
            sends[k], came[k] = out, swap(out, "order", 2)
        return out

    def do_cross(k, token):
        if not chained:
            return token
        out = pairs[k] = parts[k] + after(came[k], token)
        with jax.named_scope(f"m{k}"):
            crossed[k] = cross(out)
        return out

    def sums_of(first, count, token):
        at = range(first + LAG, first + LAG + count)
        return [sends[k] for k in at] + [after(came[k], token) for k in at]

    def do_back(u, token):
        first, count = back_units[u]
        mine, theirs, *sums, dots = unit_call(
            functools.partial(back_kernel, first, full_width, line_length), back_units[u], [lengths],
            windows_of(ser_own, ser_rec, ser_units, first, count),
            [*sums_of(first, count, token), state["squares"], down_both, *legendre, phase, *state.get("into", [])],
            [(count, channels, LANES)] * 2 + [(channels, rows)] * 2 + [(count, STATS, 256)], 24, weight=WEIGHT[2][u],
        )
        backs[u], state["into"] = (mine, theirs, dots), sums
        return dots

    def do_mix(u, token):
        first, count = mix_units[u]
        branches[u], kept[u], *state["mix"] = unit_call(
            functools.partial(branch_kernel, first, line_length), mix_units[u], [lengths],
            [*windows_of(ser_own, ser_rec, ser_units, first, count), *windows_of(cot_own, cot_rec, cot_units, first, count)],
            [*sums_of(half + first, count, token), up_both, *legendre, *state.get("mix", [])],
            [(count, channels, LANES)] * 2 + [(channels, rows)] * 2 + [(STATS, rows)], 18, weight=WEIGHT[3][u],
        )
        return state["mix"][2]

    def reduce_step(key, letter, token):
        kept_part, came_part = state[key]
        out = kept_part if came_part is None else kept_part + after(came_part, token)
        if came_part is None:
            out = after(out, token)
        order, batch = order_devices, lax.axis_size("batch")
        axis, early, bit = {
            "x": ("order", [], 1), "1": ("order", [], 2), "2": ("order", bits_of(order // 2, 4), order // 2),
            "c": ("batch", [], 1), "y": ("batch", bits_of(batch // 2, 2), batch // 2), "e": ("", [], 0),
        }[letter]
        with jax.named_scope(f"{key}_{letter}"):
            if axis:
                out = add_over(out, axis, early)
            state[key] = (out, swap(out, axis, bit) if axis else None)
        return out

    def start_sums(key, sums, token):
        with jax.named_scope(f"{key}_x"):
            state[key] = (sums[0], swap(after(sums[1], token), "order", 1))
        return token

    def do_series(token):
        count = len(back_units)
        return one_call(
            functools.partial(series_grad_kernel, back_units, full_width), struct(series.shape),
            [grad_out, ser_own, state["squares"], state["inner"], after(state["inner_rec"], token)]
            + [backs[u][0] for u in range(count)] + [backs[u][1] for u in range(count)] + ser_sent, weight=0.01,
        )

    def do_layer(token):
        count = len(mix_units)
        return one_call(
            functools.partial(layer_kernel, mix_units), struct(series.shape),
            [after(series, token)] + [branches[u] for u in range(count)] + [kept[u] for u in range(count)],
        )

    for step in PLAN:
        name, token = step.rstrip("0123456789"), state["token"]
        u = int(step[len(name) :] or 0)
        if name == "q":
            with jax.named_scope("squares_z2"):
                out = state["squares"] + after(state["squares_rec"], token)
                state["squares"] = add_over(out, "order", bits_of(order_devices, 4))
        elif name == "g":
            out = token
            with jax.named_scope(f"scaled{u}"):
                backs[u] = (backs[u][0], swap(after(backs[u][1], token), "order", 1), backs[u][2])
        elif name == "y":
            out = token
            with jax.named_scope(f"branch{u}"):
                kept[u] = swap(after(kept[u], token), "order", 1)
        elif name == "s":
            out = after(backs[u][1], token)
            backs[u] = (backs[u][0], out, backs[u][2])
        elif name == "b":
            out = kept[u] = after(kept[u], token)
        elif name == "Q":
            out = state["squares"] = after(state["squares"], token)
        elif name == "R":
            out = do_read(u, token)
        elif name == "K":
            out = do_rank(u, token)
        elif name in ("c", "x"):
            out, sent = token, cot_rec if name == "c" else ser_rec
            if u < len(sent):
                with jax.named_scope("cot_x" if name == "c" else "ser_x"):
                    sent[u] = swap(after(sent[u], token), "order", 1)
        elif name == "e":
            out = do_swap(u, token)
        elif name == "m":
            out = do_cross(u, token)
        elif name == "B":
            out = do_back(u, token)
        elif name == "M":
            out = do_mix(u, token)
        elif name == "i":
            with jax.named_scope(f"inner_z{u}"):
                if u == 1:
                    out = [after(backs[k][2], token).reshape(-1, 256) for k in range(len(back_units))]
                    out = jnp.concatenate(out, axis=0)
                else:
                    out = state["inner"] + after(state["inner_rec"], token)
                state["inner"], state["inner_rec"] = out, swap(out, "order", 1 << u)
        elif name == "ix":
            with jax.named_scope("inner_x"):
                out = state["inner"] + after(state["inner_rec"], token)
                out = add_over(out, "order", bits_of(order_devices, 8))
                state["inner"], state["inner_rec"] = out, swap(out, "order", 1)
        elif name == "iy":
            out = state["inner_rec"] = after(state["inner_rec"], token)
        elif name == "t":
            if "stats" not in state:
                state["stats"] = (state["w"][0][channels:], None)
            out = reduce_step("stats", str(u), token)
        elif name in ("tx", "tc", "ty", "gc", "gy", "ge", "rc", "ry", "re"):
            out = reduce_step({"t": "stats", "g": "w", "r": "r"}[name[0]], name[1], token)
        elif name == "r":
            out = start_sums("r", state["into"], token)
        elif name == "G":
            out = start_sums("w", [jnp.concatenate([part, state["mix"][2]], axis=0) for part in state["mix"][:2]], token)
        elif name == "CL":
            state["close"] = one_call(
                close_kernel, [struct(mode_in.shape), struct(mode_out.shape), struct((1, channels))],
                [state["r"][0], after(state["w"][0], token), mode_in, gain],
            )
            out = state["close"][0]
        elif name == "F":
            out = state[step] = do_layer(token) if u == 1 else do_series(token)
        state["token"] = out
    stream_rms = one_call(
        functools.partial(rms_kernel, order_devices / full_width), [struct((3,))],
        [state["stats"][0], after(state["stats"][1], state["token"])], scalars_out=1,
    )[0]
    grad_mode_in, grad_mode_out, grad_gain = state["close"]
    return state["F1"], state["F2"], grad_gain.reshape(channels), grad_mode_in, grad_mode_out, stream_rms


def solution(mesh):
    wide = P("order", "batch")
    weight = P(None, None, None, "order")
    in_specs = (wide, P("order"), weight, weight, P("batch"), wide)
    out_specs = (wide, wide, P("order"), weight, weight, P())
    return jax.shard_map(local, mesh=mesh, in_specs=in_specs, out_specs=out_specs, check_vma=False)
```

```python
import functools
import math

import jax
import jax.numpy as jnp
import numpy as np
from jax import lax
from jax.experimental import pallas as pl
from jax.experimental.pallas import tpu as pltpu
from jax.sharding import PartitionSpec as P

ORDER = 256
LEN = 720
LANES = 768
BLOCK = 256
epsilon = 1e-06
f32 = jnp.float32
bf16 = jnp.bfloat16


def legendre_rows():
    coords = 1.0 - (2.0 * np.arange(LEN) + 1.0) / LEN
    rows = [np.ones(LEN), coords]
    for k in range(1, ORDER - 1):
        rows.append(((2.0 * k + 1.0) * coords * rows[k] - k * rows[k - 1]) / (k + 1.0))
    table = np.stack(rows) * np.sqrt((2.0 * np.arange(ORDER) + 1.0) / LEN)[:, None]
    out = np.zeros((ORDER, LANES))
    out[:, :LEN] = table[:, ::-1]
    return out


def phase_rows(mode_count):
    modes = np.arange(mode_count)[:, None]
    steps = np.arange(LANES)[None, :]
    now = 2.0 * np.pi * ((modes * steps) % LEN) / LEN
    nxt = 2.0 * np.pi * ((modes * (steps + 1)) % LEN) / LEN
    root = 1.0 / math.sqrt(LEN)
    rows = np.stack([np.cos(now), np.sin(now), np.cos(nxt) * root, np.sin(nxt) * root])
    return rows.astype(np.float32)


def halves(table):
    high = table.astype(np.float32).astype(jnp.bfloat16)
    low = (table - high.astype(np.float64)).astype(np.float32).astype(jnp.bfloat16)
    return high, low


def split(x):
    high = x.astype(bf16)
    return high, (x - high.astype(f32)).astype(bf16)


def nn(a, b):
    return lax.dot_general(a, b, (((1,), (0,)), ((), ())), preferred_element_type=f32)


def nt(a, b):
    return lax.dot_general(a, b, (((1,), (1,)), ((), ())), preferred_element_type=f32)


def three(dot, pairs, table):
    rows = pairs[0][0].shape[0]
    high = dot(jnp.concatenate([half for pair in pairs for half in pair], axis=0), table[0])
    low = dot(jnp.concatenate([pair[0] for pair in pairs], axis=0), table[1])
    out = []
    for k in range(len(pairs)):
        at = 2 * k * rows
        out.append(high[at : at + rows] + high[at + rows : at + 2 * rows] + low[k * rows : (k + 1) * rows])
    return out


def deep(x):
    high, low = split(x)
    return jnp.concatenate([high, low, high], axis=0)


def stacked(weights, pair, rows):
    first = nn(weights, pair[0])
    return first[:rows] + first[rows:] + nn(weights[:rows], pair[1])


def stacked_nt(left, pair, rows):
    first = nt(left, pair[0])
    return first[:rows] + first[rows:] + nt(left[:rows], pair[1])


def rotate(real, imag, cos, sin):
    modes = cos.shape[0]
    shape = (real.shape[0] // modes, modes, real.shape[1])
    real, imag = real.reshape(shape), imag.reshape(shape)
    cos, sin = cos[None], sin[None]
    flat = (shape[0] * modes, shape[2])
    return (real * cos + imag * sin).reshape(flat), (imag * cos - real * sin).reshape(flat)


def triangle():
    row = lax.broadcasted_iota(jnp.int32, (BLOCK, BLOCK), 0)
    col = lax.broadcasted_iota(jnp.int32, (BLOCK, BLOCK), 1)
    return jnp.where(row <= col, 1.0, 0.0).astype(bf16)


def block_sums(dot, x):
    rows, blocks = x.shape[0], LANES // BLOCK
    halves_of = split(x)
    stack = [half[:, b * BLOCK : (b + 1) * BLOCK] for half in halves_of for b in range(blocks)]
    sums = dot(jnp.concatenate(stack, axis=0), triangle())
    return [sums[b * rows : (b + 1) * rows] + sums[(blocks + b) * rows : (blocks + b + 1) * rows] for b in range(blocks)]


def running_sum(x):
    blocks = block_sums(nn, x)
    for b in range(1, len(blocks)):
        blocks[b] = blocks[b] + blocks[b - 1][:, BLOCK - 1 : BLOCK]
    return jnp.concatenate(blocks, axis=1)


def running_sum_back(x):
    blocks = block_sums(nt, x)
    for b in reversed(range(len(blocks) - 1)):
        blocks[b] = blocks[b] + blocks[b + 1][:, 0:1]
    return jnp.concatenate(blocks, axis=1)


def side_of():
    return lax.rem(lax.axis_index("order"), 2)


def at_line_end(line_length):
    line = lax.div(lax.axis_index("order"), 2)
    return jnp.logical_or(line == 0, line == line_length - 1)


def locate(units, j):
    u = max(k for k in range(len(units)) if units[k][0] <= j)
    return u, j - units[u][0]


def chunk_ends(windows):
    return [-(-LEN * min(w + 2, windows) // 128) * 128 for w in range(0, windows, 2)]


def deal_windows(split_at, len_hbm, hbm_ref, len_ref, buffer, sems, out_refs, use):
    lengths_copy = pltpu.make_async_copy(len_hbm, len_ref, sems.at[0])
    lengths_copy.start()
    own_ref, send_refs = out_refs[0], out_refs[1:]
    channels = hbm_ref.shape[0]
    windows = hbm_ref.shape[1] // LEN
    half = windows // 2
    ends = chunk_ends(windows)
    copies = []
    for c, end in enumerate(ends):
        at = slice(ends[c - 1] if c else 0, end)
        copies.append(pltpu.make_async_copy(hbm_ref.at[:, at], buffer.at[:, at], sems.at[1 + c]))
        copies[-1].start()
    lane = lax.broadcasted_iota(jnp.int32, (channels, LEN), 1)
    side = side_of()
    for ref in out_refs:
        ref[:, :, LANES - 128 :] = jnp.zeros((ref.shape[0], channels, 128), f32)
    lengths_copy.wait()
    for w in range(windows):
        if w % 2 == 0:
            copies[w // 2].wait()
        value = buffer[:, w * LEN : (w + 1) * LEN]
        value = jnp.where(lane < len_ref[w], value, 0.0)
        use(w, value)
        unit, at = locate(split_at, w % half)
        send_ref = send_refs[unit]
        mine = side == (0 if w < half else 1)

        @pl.when(mine)
        def _():
            own_ref[w % half, :, :LEN] = value

        @pl.when(jnp.logical_not(mine))
        def _():
            send_ref[at, :, :LEN] = value


PACK = 48
STATS = 8


def readout_columns(modes, channels):
    mode = lax.broadcasted_iota(jnp.int32, (modes, channels), 0)
    angle = mode.astype(f32) * (2.0 * math.pi / LEN)
    factor = jnp.where(mode == 0, 1.0, 2.0) * (1.0 / math.sqrt(LEN))
    return factor * jnp.cos(angle), factor * jnp.sin(angle)


def pack_kernel(line_length, in_hbm, out_hbm, gain_hbm, message_ref, end_ref, in_ref, out_ref, gain_ref, packed, sems):
    copies = [(in_hbm, in_ref), (out_hbm, out_ref), (gain_hbm, gain_ref)]
    copies = [pltpu.make_async_copy(a, b, sems.at[k]) for k, (a, b) in enumerate(copies)]
    for copy in copies:
        copy.start()
    end_ref[...] = jnp.where(at_line_end(line_length), jnp.ones(end_ref.shape, f32), 0.0)
    message_ref[...] = jnp.zeros(message_ref.shape, f32)
    packed[...] = jnp.zeros(packed.shape, f32)
    for copy in copies:
        copy.wait()
    modes, ranks, channels = in_ref.shape[1:]
    read_real, read_imag = readout_columns(modes, channels)
    for r in range(ranks):
        real, imag = out_ref[0, :, r, :], out_ref[1, :, r, :]
        second = (read_real * real + read_imag * imag, read_imag * real - read_real * imag)
        for part in range(2):
            at = slice((part * ranks + r) * modes, (part * ranks + r + 1) * modes)
            packed[at, :channels] = in_ref[part, :, r, :] * gain_ref[...]
            packed[at, channels : 2 * channels] = second[part]
    rows = packed.shape[0]
    for k in range(-(-rows // PACK)):
        count = min(PACK, rows - k * PACK)
        message_ref[:count, k * 128 : (k + 1) * 128] = packed[k * PACK : k * PACK + count]


def series_kernel(units, len_hbm, x_hbm, squares_ref, *refs):
    squares_ref[...] = jnp.zeros(squares_ref.shape, f32)

    def use(w, value):
        squares_ref[w : w + 1, :LEN] = jnp.sum(value * value, axis=0, keepdims=True)

    deal_windows(units, len_hbm, x_hbm, *refs[-3:], refs[:-3], use)


def unpack(message_ref, rows):
    pieces = []
    for k in range(-(-rows // PACK)):
        count = min(PACK, rows - k * PACK)
        pieces.append(message_ref[:count, k * 128 : (k + 1) * 128])
    return jnp.concatenate(pieces, axis=0)


def cot_kernel(units, len_hbm, x_hbm, *refs):
    deal_windows(units, len_hbm, x_hbm, *refs[-3:], refs[:-3], lambda w, value: None)


def weights_kernel(own_ref, rec_ref, down_own, down_rec, up_own, up_rec, down_both, up_both):
    rows, channels = down_own.shape[0], down_own.shape[1] // 3
    pieces = []
    for ref, down, up in ((own_ref, down_own, up_own), (rec_ref, down_rec, up_rec)):
        packed = unpack(ref, rows)
        high, low = split(packed)
        down[...] = jnp.concatenate([high[:, :channels], high[:, :channels], low[:, :channels]], axis=1)
        upper = slice(channels, 2 * channels)
        up[...] = jnp.concatenate([high[:, upper], high[:, upper], low[:, upper]], axis=1)
        pieces.append(packed.T)
    for k, ref in ((0, down_both), (1, up_both)):
        at = slice(k * channels, (k + 1) * channels)
        both = jnp.concatenate([pieces[0][at], pieces[1][at]], axis=0)
        high, low = split(both)
        ref[...] = jnp.concatenate([high, low], axis=0)


def read_kernel(own_ref, rec_ref, up_own, up_rec, leg_high, leg_low, *out_refs):
    pairs = []
    for k in range(len(out_refs)):
        pairs.append(split(nn(up_own[...], deep(own_ref[k])) + nn(up_rec[...], deep(rec_ref[k]))))
    for ref, value in zip(out_refs, three(nt, pairs, (leg_high[...], leg_low[...]))):
        ref[...] = value


def inverse_rms(ss_ref, row, full_width):
    return lax.rsqrt(ss_ref[pl.ds(row, 1), :] * (1.0 / full_width) + epsilon)


def rank_kernel(first, full_width, own_ref, rec_ref, ss_ref, down_own, down_rec, leg_high, leg_low, phase_ref, *out_refs):
    row = side_of() * (ss_ref.shape[0] // 2) + first
    pairs = []
    for k in range(len(out_refs)):
        inv = inverse_rms(ss_ref, row + k, full_width)
        mixed = nn(down_own[...], deep(own_ref[k] * inv)) + nn(down_rec[...], deep(rec_ref[k] * inv))
        part = mixed.shape[0] // 2
        real, imag = rotate(mixed[:part], mixed[part:], phase_ref[0], phase_ref[1])
        total = running_sum(jnp.concatenate([real, imag], axis=0))
        real, imag = rotate(total[:part], total[part:], phase_ref[2], -phase_ref[3])
        pairs.append(split(jnp.concatenate([real, imag], axis=0)))
    for ref, value in zip(out_refs, three(nt, pairs, (leg_high[...], leg_low[...]))):
        ref[...] = value


def totals(line_length, refs):
    count, at_end = len(refs) // 2, at_line_end(line_length)
    return [split(jnp.where(at_end, refs[count + k][...], refs[k][...])) for k in range(count)]


def masked(value, length):
    lane = lax.broadcasted_iota(jnp.int32, value.shape, 1)
    return jnp.where(lane < length, value, 0.0)


def opening(refs, outs, sums):
    return [ref[...] for ref in refs[:-outs]] or [0.0] * sums, refs[-outs:]


def back_kernel(first, full_width, line_length, len_ref, own_ref, rec_ref, *refs):
    sums, refs = refs[: 2 * own_ref.shape[0]], refs[2 * own_ref.shape[0] :]
    ss_ref, down_both, leg_high, leg_low, phase_ref, *refs = refs
    before, (own_out, rec_out, grad_own, grad_rec, inner_out) = opening(refs, 5, 2)
    grads = 0.0
    row = side_of() * (ss_ref.shape[0] // 2) + first
    channels = own_ref.shape[1]
    for k, total in enumerate(totals(line_length, sums)):
        (memory,) = three(nn, [total], (leg_high[...], leg_low[...]))
        part = memory.shape[0] // 2
        real, imag = rotate(memory[:part], memory[part:], phase_ref[2], phase_ref[3])
        back = running_sum_back(jnp.concatenate([real, imag], axis=0))
        real, imag = rotate(back[:part], back[part:], phase_ref[0], -phase_ref[1])
        pair = split(jnp.concatenate([real, imag], axis=0))
        scaled = masked(stacked(down_both[...], pair, 2 * channels), len_ref[row + k])
        own_out[k] = scaled[:channels]
        rec_out[k] = scaled[channels:]
        both = jnp.concatenate([own_ref[k], rec_ref[k]], axis=0)
        inner = jnp.sum(scaled * both, axis=0, keepdims=True)
        pieces = [inner[:, p * 256 : (p + 1) * 256] for p in range(LANES // 256)]
        inner_out[k] = jnp.concatenate(pieces + [jnp.zeros((STATS - len(pieces), 256), f32)], axis=0)
        high, low = split(both * inverse_rms(ss_ref, row + k, full_width))
        grads = grads + stacked_nt(jnp.concatenate([high, low], axis=0), pair, 2 * channels)
    grad_own[...] = before[0] + grads[:channels]
    grad_rec[...] = before[1] + grads[channels:]


def branch_kernel(first, line_length, len_ref, ser_own, ser_rec, cot_own, cot_rec, *refs):
    sums, refs = refs[: 2 * ser_own.shape[0]], refs[2 * ser_own.shape[0] :]
    up_both, leg_high, leg_low, *refs = refs
    before, (own_out, rec_out, grad_own, grad_rec, stats_out) = opening(refs, 5, 3)
    channels = ser_own.shape[1]
    rows = 2 * channels
    windows = len_ref.shape[0]
    row = side_of() * (windows // 2) + first
    grads, stats = 0.0, [0.0, 0.0, 0.0]
    for k, total in enumerate(totals(line_length, sums)):
        pair = split(three(nn, [total], (leg_high[...], leg_low[...]))[0])
        branch = masked(stacked(up_both[...], pair, rows), len_ref[row + k])
        own_out[k] = branch[:channels]
        rec_out[k] = branch[channels:]
        high, low = split(jnp.concatenate([cot_own[k], cot_rec[k]], axis=0))
        grads = grads + stacked_nt(jnp.concatenate([high, low], axis=0), pair, rows)
        series = jnp.concatenate([ser_own[k], ser_rec[k]], axis=0)
        for i, v in enumerate((series, branch, series + branch)):
            stats[i] = stats[i] + jnp.sum(v * v, axis=0, keepdims=True)
    width = grads.shape[1]
    stats = [jnp.broadcast_to(jnp.sum(v, axis=1, keepdims=True), (1, width)) for v in stats]
    steps = functools.reduce(lambda a, b: a + b, [len_ref[w] for w in range(windows)]) if first == 0 else 0
    stats.append(jnp.full((1, width), steps, jnp.int32).astype(f32))
    stats = jnp.concatenate(stats + [jnp.zeros((STATS - 4, width), f32)], axis=0)
    grad_own[...] = before[0] + grads[:channels]
    grad_rec[...] = before[1] + grads[channels:]
    stats_out[...] = before[2] + stats


def own_or_theirs(units, own_refs, rec_refs, w, half):
    u, j = locate(units, w % half)
    return jnp.where((side_of() == 0) == (w < half), own_refs[u][j], rec_refs[u][j])


def layer_kernel(units, x_ref, *refs):
    own_refs, rec_refs, out_ref = refs[: len(units)], refs[len(units) : 2 * len(units)], refs[-1]
    windows = x_ref.shape[1] // LEN
    branches = [own_or_theirs(units, own_refs, rec_refs, w, windows // 2)[:, :LEN] for w in range(windows)]
    out_ref[...] = x_ref[...] + jnp.concatenate(branches, axis=1)


def inner_row(small_ref, j):
    row = STATS * j
    return jnp.concatenate([small_ref[row + p : row + p + 1, :] for p in range(LANES // 256)], axis=1)


def series_grad_kernel(units, full_width, cot_ref, x_own, ss_ref, in_own, in_rec, *refs):
    count = len(units)
    own_refs, rec_refs, sent_refs, out_ref = refs[:count], refs[count : 2 * count], refs[2 * count : -1], refs[-1]
    windows = cot_ref.shape[1] // LEN
    half = windows // 2
    first_side = side_of() == 0
    sent = [(ref, k) for ref in sent_refs for k in range(ref.shape[0])]
    shifts = []
    for w in range(windows):
        keep = first_side == (w < half)
        scaled = own_or_theirs(units, own_refs, rec_refs, w, half)
        ref, k = sent[w % half]
        series = jnp.where(keep, x_own[w % half], ref[k])
        inner = jnp.where(keep, inner_row(in_own, w % half), inner_row(in_rec, w % half))
        inv = inverse_rms(ss_ref, w, full_width)
        shifts.append((inv * (scaled - series * (inv * inv * inner * (1.0 / full_width))))[:, :LEN])
    out_ref[...] = cot_ref[...] + jnp.concatenate(shifts, axis=1)


def close_kernel(into_ref, mix_ref, in_ref, gain_ref, grad_in_ref, grad_out_ref, grad_gain_ref):
    modes, ranks, channels = in_ref.shape[1:]
    into, mix = into_ref[...].T, mix_ref[:channels].T
    total = jnp.zeros((modes, channels), f32)
    read_real, read_imag = readout_columns(modes, channels)
    for r in range(ranks):
        pieces = []
        for part in range(2):
            at = slice((part * ranks + r) * modes, (part * ranks + r + 1) * modes)
            grad = into[at]
            total = total + grad * in_ref[part, :, r, :]
            grad_in_ref[part, :, r, :] = grad * gain_ref[...]
            pieces.append(mix[at])
        grad_out_ref[0, :, r, :] = read_real * pieces[0] + read_imag * pieces[1]
        grad_out_ref[1, :, r, :] = read_imag * pieces[0] - read_real * pieces[1]
    grad_gain_ref[...] = jnp.sum(total, axis=0, keepdims=True)


def rms_kernel(share, own_ref, rec_ref, rms_ref):
    stats = own_ref[...] + rec_ref[...]
    rms = jnp.sqrt(stats * share / stats[3:4])
    for k in range(3):
        rms_ref[k] = rms[k, 0]


def whole(shape):
    return pl.BlockSpec(shape, lambda *_: (0,) * len(shape))


SMEM = pl.BlockSpec(memory_space=pltpu.SMEM)
PARAMS = pltpu.CompilerParams(vmem_limit_bytes=8 * 1024 * 1024)


def cost(flops, byte_count, weight=1):
    return pl.CostEstimate(flops=int(flops * weight), bytes_accessed=int(byte_count * weight), transcendentals=0)


def struct(shape, dtype=f32):
    return jax.ShapeDtypeStruct(shape, dtype)


def one_call(kernel, outs, args, smem=0, scalars_out=0, weight=1):
    single = not isinstance(outs, list)
    shapes = [outs] if single else outs
    specs = [SMEM] * smem + [whole(a.shape) for a in args[smem:]]
    moved = sum(a.size * a.dtype.itemsize for a in args) + sum(math.prod(o.shape) * 4 for o in shapes)
    result = pl.pallas_call(
        kernel,
        out_shape=shapes,
        in_specs=specs,
        out_specs=[whole(o.shape) for o in shapes[: len(shapes) - scalars_out]] + [SMEM] * scalars_out,
        grid=(1,),
        compiler_params=PARAMS,
        cost_estimate=cost(moved, moved, weight),
    )(*args)
    return result[0] if single else result


HBM = pl.BlockSpec(memory_space=pltpu.MemorySpace.HBM)


def in_hbm(arrays):
    return [pltpu.with_memory_space_constraint(a, pltpu.MemorySpace.HBM) for a in arrays]


def deal_scratch(array, lengths):
    windows = array.shape[1] // LEN
    return [pltpu.SMEM(lengths.shape, jnp.int32)], [
        pltpu.VMEM(array.shape, f32),
        pltpu.SemaphoreType.DMA((1 + len(chunk_ends(windows)),)),
    ]


def pack(weights, rows, line_length):
    shapes = [struct((PACK, LANES)), struct((8, ORDER))]
    return pl.pallas_call(
        functools.partial(pack_kernel, line_length),
        out_shape=shapes,
        in_specs=[HBM] * len(weights),
        out_specs=[whole(o.shape) for o in shapes],
        grid=(1,),
        scratch_shapes=[pltpu.VMEM(a.shape, f32) for a in weights]
        + [pltpu.VMEM((rows, 128), f32), pltpu.SemaphoreType.DMA((len(weights),))],
        compiler_params=PARAMS,
        cost_estimate=cost(rows * 1024, rows * 2048),
    )(*in_hbm(weights))


def deal(kernel, array, lengths, units, extra=()):
    channels, windows = array.shape[0], array.shape[1] // LEN
    shapes = [struct(shape) for shape in extra] + [struct((windows // 2, channels, LANES))] + [struct((n, channels, LANES)) for _, n in units]
    first, rest = deal_scratch(array, lengths)
    return pl.pallas_call(
        functools.partial(kernel, units),
        out_shape=shapes,
        in_specs=[HBM] * 2,
        out_specs=[whole(o.shape) for o in shapes],
        grid=(1,),
        scratch_shapes=first + rest,
        compiler_params=PARAMS,
        cost_estimate=cost(array.size * 4, array.size * 8, DEAL),
    )(*in_hbm([lengths, array]))


def prepare_weights(own, rec, rows, channels):
    shapes = [struct((rows, 3 * channels), bf16)] * 4 + [struct((4 * channels, rows), bf16)] * 2
    return one_call(weights_kernel, shapes, [own, rec])


MATMUL = 2 * 256 * 256 * 256


def unit_call(kernel, unit, smem, arrays, consts, outs, units_of_work, weight=1):
    count = unit[1]
    specs = [SMEM] * len(smem)
    assert all(o % count == 0 for _, o in arrays)
    specs += [pl.BlockSpec((count,) + a.shape[1:], lambda i, o=o // count, r=a.ndim - 1: (o,) + (0,) * r) for a, o in arrays]
    specs += [whole(c.shape) for c in consts]
    moved = sum(a.size * 4 * count // a.shape[0] for a, _ in arrays) + sum(c.size * c.dtype.itemsize for c in consts)
    return pl.pallas_call(
        kernel,
        out_shape=[struct(shape) for shape in outs],
        in_specs=specs,
        out_specs=[whole(shape) for shape in outs],
        grid=(1,),
        compiler_params=PARAMS,
        cost_estimate=cost(units_of_work * MATMUL * count, moved, weight),
    )(*smem, *[a for a, _ in arrays], *consts)


def swap(x, axis, bit):
    size = lax.axis_size(axis)
    return lax.ppermute(x, axis, [(i, i ^ bit) for i in range(size)])


def add_over(x, axis, bits):
    for bit in bits:
        x = x + swap(x, axis, bit)
    return x


def bits_of(size, start=1):
    bits, bit = [], start
    while bit < size:
        bits.append(bit)
        bit *= 2
    return bits


def cross(x):
    batch, order = lax.axis_size("batch"), lax.axis_size("order")
    pairs = []
    for b in range(batch):
        for o in range(order):
            inner = o // 2 in (1, 2)
            pairs.append((b * order + o, b * order + (o ^ 6) if inner else (b ^ 1) * order + o))
    return lax.ppermute(x, ("batch", "order"), pairs)


def line_sum(x):
    size = lax.axis_size("order")
    return lax.psum(x, "order", axis_index_groups=[list(range(side, size, 2)) for side in (0, 1)])


def after(x, tokens):
    tokens = tokens if isinstance(tokens, tuple) else (tokens,)
    return lax.optimization_barrier((x, *tokens))[0]


DEAL = 1000
WEIGHT = ((10,10,10,10),(10,10),(10,10),(10,10,10))
COT = (1, 1, 1, 1)
SER = (2, 2)
READ = (1, 1, 1, 1)
RANK = (2, 2)
BACK = (2, 2)
MIX = (2, 1, 1)
LAG = 3
EARLY = 2
PLAN = (
    "R0", "e0", "c2", "R1", "q", "e1", "c3", "x0", "m0", "R2", "e2", "Q", "m1", "R3", "x1", "e3",
    "m2", "K0", "e4", "m3", "e5", "K1", "m4", "e6", "m5", "B0", "g0", "e7", "m6", "B1", "e8", "m7",
    "r", "e9", "g1", "i1", "rc", "s0", "M0", "y0", "e10", "i2", "M1", "s1", "ry", "ix", "y1", "M2",
    "re", "G", "y2", "iy", "b0", "gc", "gy", "F2", "b1", "ge", "t1", "b2", "CL", "t2", "F1",
)


def units_of(half, counts):
    counts = counts if sum(counts) == half else (1,) * half
    return [(sum(counts[:u]), counts[u]) for u in range(len(counts))]


def local(series, norm_gain, mode_in, mode_out, lengths, grad_out):
    channels = series.shape[0]
    windows = series.shape[1] // LEN
    half = windows // 2
    order_devices = lax.axis_size("order")
    line_length = order_devices // 2
    mode_count, rank_count = mode_in.shape[1], mode_in.shape[2]
    full_width = channels * order_devices
    rows = 2 * rank_count * mode_count
    cot_units, ser_units = units_of(half, COT), units_of(half, SER)
    read_units, rank_units = units_of(half, READ), units_of(half, RANK)
    back_units, mix_units = units_of(half, BACK), units_of(half, MIX)

    legendre = [jnp.asarray(h) for h in halves(legendre_rows())]
    phase = jnp.asarray(phase_rows(mode_count))
    gain = norm_gain.reshape(1, channels)

    message, end_mask = pack([mode_in, mode_out, gain], rows, line_length)
    with jax.named_scope("message_x"):
        message_rec = swap(message, "order", 1)
    cot_own, *cot_rec = deal(cot_kernel, after(grad_out, message), lengths, cot_units)
    with jax.named_scope("cot_x"):
        cot_rec[0] = swap(cot_rec[0], "order", 1)
    squares, ser_own, *ser_sent = deal(series_kernel, after(series, cot_own), lengths, ser_units, [(windows, LANES)])
    ser_rec = list(ser_sent)
    with jax.named_scope("squares_x"):
        squares_rec = swap(squares, "order", 1)
    message_rec = after(message_rec, ser_own)
    with jax.named_scope("cot_x"):
        for u in range(1, EARLY):
            cot_rec[u] = swap(after(cot_rec[u], message_rec), "order", 1)
    down_own, down_rec, up_own, up_rec, down_both, up_both = prepare_weights(message, message_rec, rows, channels)
    with jax.named_scope("squares_z1"):
        squares = squares + after(squares_rec, up_own)
        squares_rec = swap(squares, "order", 2)

    def windows_of(own, received, units, first, count):
        u, offset = locate(units, first)
        v, _ = locate(units, first + count - 1)
        if u < v:
            return [(own, first), (jnp.concatenate(received[u : v + 1], axis=0), offset)]
        return [(own, first), (received[u], offset)]

    chained = order_devices == 8
    at_end = end_mask[:1] > 0.5
    parts, pairs, sends, came, crossed = {}, {}, {}, {}, {}
    backs, branches, kept = {}, {}, {}
    state = {"squares": squares, "squares_rec": squares_rec, "token": up_own}

    def do_read(u, token):
        first, count = read_units[u]
        own, rec = windows_of(cot_own, cot_rec, cot_units, first, count)
        outs = unit_call(
            read_kernel, read_units[u], [], [own, (after(rec[0], token), rec[1])],
            [up_own, up_rec, *legendre], [(rows, ORDER)] * count, 15, weight=WEIGHT[0][u],
        )
        for k in range(count):
            parts[first + k] = outs[k]
        return outs[0]

    def do_rank(u, token):
        first, count = rank_units[u]
        own, rec = windows_of(ser_own, ser_rec, ser_units, first, count)
        outs = unit_call(
            functools.partial(rank_kernel, first, full_width), rank_units[u], [], [own, (after(rec[0], token), rec[1])],
            [state["squares"], down_own, down_rec, *legendre, phase], [(rows, ORDER)] * count, 21, weight=WEIGHT[1][u],
        )
        for k in range(count):
            parts[half + first + k] = outs[k]
        return outs[0]

    def do_swap(k, token):
        if not chained:
            if k < windows:
                came[k + LAG] = sends[k + LAG] = line_sum(after(parts[k], token))
            return token
        done = k - LAG
        if done < 0:
            out = after(parts[k], token)
        else:
            out = pairs[done] + after(crossed[done], token)
            if k < windows:
                out = jnp.where(at_end, parts[k], out)
        with jax.named_scope(f"e{k}"):
            sends[k], came[k] = out, swap(out, "order", 2)
        return out

    def do_cross(k, token):
        if not chained:
            return token
        out = pairs[k] = parts[k] + after(came[k], token)
        with jax.named_scope(f"m{k}"):
            crossed[k] = cross(out)
        return out

    def sums_of(first, count, token):
        at = range(first + LAG, first + LAG + count)
        return [sends[k] for k in at] + [after(came[k], token) for k in at]

    def do_back(u, token):
        first, count = back_units[u]
        mine, theirs, *sums, dots = unit_call(
            functools.partial(back_kernel, first, full_width, line_length), back_units[u], [lengths],
            windows_of(ser_own, ser_rec, ser_units, first, count),
            [*sums_of(first, count, token), state["squares"], down_both, *legendre, phase, *state.get("into", [])],
            [(count, channels, LANES)] * 2 + [(channels, rows)] * 2 + [(count, STATS, 256)], 24, weight=WEIGHT[2][u],
        )
        backs[u], state["into"] = (mine, theirs, dots), sums
        return dots

    def do_mix(u, token):
        first, count = mix_units[u]
        branches[u], kept[u], *state["mix"] = unit_call(
            functools.partial(branch_kernel, first, line_length), mix_units[u], [lengths],
            [*windows_of(ser_own, ser_rec, ser_units, first, count), *windows_of(cot_own, cot_rec, cot_units, first, count)],
            [*sums_of(half + first, count, token), up_both, *legendre, *state.get("mix", [])],
            [(count, channels, LANES)] * 2 + [(channels, rows)] * 2 + [(STATS, rows)], 18, weight=WEIGHT[3][u],
        )
        return state["mix"][2]

    def reduce_step(key, letter, token):
        kept_part, came_part = state[key]
        out = kept_part if came_part is None else kept_part + after(came_part, token)
        if came_part is None:
            out = after(out, token)
        order, batch = order_devices, lax.axis_size("batch")
        axis, early, bit = {
            "x": ("order", [], 1), "1": ("order", [], 2), "2": ("order", bits_of(order // 2, 4), order // 2),
            "c": ("batch", [], 1), "y": ("batch", bits_of(batch // 2, 2), batch // 2), "e": ("", [], 0),
        }[letter]
        with jax.named_scope(f"{key}_{letter}"):
            if axis:
                out = add_over(out, axis, early)
            state[key] = (out, swap(out, axis, bit) if axis else None)
        return out

    def start_sums(key, sums, token):
        with jax.named_scope(f"{key}_x"):
            state[key] = (sums[0], swap(after(sums[1], token), "order", 1))
        return token

    def do_series(token):
        count = len(back_units)
        return one_call(
            functools.partial(series_grad_kernel, back_units, full_width), struct(series.shape),
            [grad_out, ser_own, state["squares"], state["inner"], after(state["inner_rec"], token)]
            + [backs[u][0] for u in range(count)] + [backs[u][1] for u in range(count)] + ser_sent, weight=0.01,
        )

    def do_layer(token):
        count = len(mix_units)
        return one_call(
            functools.partial(layer_kernel, mix_units), struct(series.shape),
            [after(series, token)] + [branches[u] for u in range(count)] + [kept[u] for u in range(count)],
        )

    for step in PLAN:
        name, token = step.rstrip("0123456789"), state["token"]
        u = int(step[len(name) :] or 0)
        if name == "q":
            with jax.named_scope("squares_z2"):
                out = state["squares"] + after(state["squares_rec"], token)
                state["squares"], state["squares_rec"] = out, swap(out, "order", 4)
        elif name == "g":
            out = token
            with jax.named_scope(f"scaled{u}"):
                backs[u] = (backs[u][0], swap(after(backs[u][1], token), "order", 1), backs[u][2])
        elif name == "y":
            out = token
            with jax.named_scope(f"branch{u}"):
                kept[u] = swap(after(kept[u], token), "order", 1)
        elif name == "s":
            out = after(backs[u][1], token)
            backs[u] = (backs[u][0], out, backs[u][2])
        elif name == "b":
            out = kept[u] = after(kept[u], token)
        elif name == "Q":
            out = state["squares"] + after(state["squares_rec"], token)
            state["squares"] = out = add_over(out, "order", bits_of(order_devices, 8))
        elif name == "R":
            out = do_read(u, token)
        elif name == "K":
            out = do_rank(u, token)
        elif name in ("c", "x"):
            out, sent = token, cot_rec if name == "c" else ser_rec
            if u < len(sent):
                with jax.named_scope("cot_x" if name == "c" else "ser_x"):
                    sent[u] = swap(after(sent[u], token), "order", 1)
        elif name == "e":
            out = do_swap(u, token)
        elif name == "m":
            out = do_cross(u, token)
        elif name == "B":
            out = do_back(u, token)
        elif name == "M":
            out = do_mix(u, token)
        elif name == "i":
            with jax.named_scope(f"inner_z{u}"):
                if u == 1:
                    out = [after(backs[k][2], token).reshape(-1, 256) for k in range(len(back_units))]
                    out = jnp.concatenate(out, axis=0)
                else:
                    out = state["inner"] + after(state["inner_rec"], token)
                state["inner"], state["inner_rec"] = out, swap(out, "order", 1 << u)
        elif name == "ix":
            with jax.named_scope("inner_x"):
                out = state["inner"] + after(state["inner_rec"], token)
                out = add_over(out, "order", bits_of(order_devices, 8))
                state["inner"], state["inner_rec"] = out, swap(out, "order", 1)
        elif name == "iy":
            out = state["inner_rec"] = after(state["inner_rec"], token)
        elif name == "t":
            if "stats" not in state:
                state["stats"] = (state["w"][0][channels:], None)
            out = reduce_step("stats", str(u), token)
        elif name in ("tx", "tc", "ty", "gc", "gy", "ge", "rc", "ry", "re"):
            out = reduce_step({"t": "stats", "g": "w", "r": "r"}[name[0]], name[1], token)
        elif name == "r":
            out = start_sums("r", state["into"], token)
        elif name == "G":
            out = start_sums("w", [jnp.concatenate([part, state["mix"][2]], axis=0) for part in state["mix"][:2]], token)
        elif name == "CL":
            state["close"] = one_call(
                close_kernel, [struct(mode_in.shape), struct(mode_out.shape), struct((1, channels))],
                [state["r"][0], after(state["w"][0], token), mode_in, gain],
            )
            out = state["close"][0]
        elif name == "F":
            out = state[step] = do_layer(token) if u == 1 else do_series(token)
        state["token"] = out
    stream_rms = one_call(
        functools.partial(rms_kernel, order_devices / full_width), [struct((3,))],
        [state["stats"][0], after(state["stats"][1], state["token"])], scalars_out=1,
    )[0]
    grad_mode_in, grad_mode_out, grad_gain = state["close"]
    return state["F1"], state["F2"], grad_gain.reshape(channels), grad_mode_in, grad_mode_out, stream_rms


def solution(mesh):
    wide = P("order", "batch")
    weight = P(None, None, None, "order")
    in_specs = (wide, P("order"), weight, weight, P("batch"), wide)
    out_specs = (wide, wide, P("order"), weight, weight, P())
    return jax.shard_map(local, mesh=mesh, in_specs=in_specs, out_specs=out_specs, check_vma=False)
```
